32 devices in a mesh: mem: 4 (over y, core), tile: 8 (over z, x).
Axes of the slice: x: 2, y: 2, z: 4, core: 2. Of those that a mesh axis runs over, the one named last changes fastest.
Arguments:
- ensemble_profiles_before: bfloat16 [64, 40, 4096], P('mem', None, 'tile'), may hold values from -6 to 6
- mixing_coefficient: float32 [4096], P('tile'), may hold values from 0.05 to 0.24
- surface_driver: float32 [64, 4096], P('mem', 'tile'), may hold values from -3 to 3
- terrain_indicator: int32 [4096], P('tile'), may hold values 0 or 1
- measured_profile_position: int32 [32768], P('tile'), may hold values from 0 to 511
- measured_field_index: int32 [32768], P('tile'), may hold values from 0 to 39
- obs_valid: int32 [32768], P('tile'), may hold values 0 or 1
- obs_value: bfloat16 [32768], P('tile'), may hold values from -6 to 6
- obs_error: bfloat16 [32768], P('tile'), may hold values from 0.5 to 4
- local_weight: float32 [4, 8, 20480], P('mem', 'tile'), may hold values from 0.001 to 0.03
Outputs:
- analysis: bfloat16 [64, 40, 4096], P('mem', None, 'tile')
The draws below stay inside these ranges and needn't reach their ends.
All inputs are finite; a program needn't handle non-finite values. No bound on the sum of `terrain_indicator` or of `obs_valid` on one device may be relied on, other than what follows from the above.
Results may differ from the reference program's by a relative error of at most 0.0034.
Values may be sent and summed in bfloat16 or wider, within the bound.
A program may use at most 64 MiB of HBM per device.

```python
import math
import jax
import jax.numpy as jnp
from jax import lax

K = 64
PROFILE_SIZE = 40
BLK = 128
OBS_T = 4096
REACH = 2
NS_ITERS = 3
C_TILE = 512
COLS = 4096
NB_TILE = 4
P_OBS = 20480
N_TILE = 8


def set_ends(values, stream_key, least, largest):
    longest = values.shape.index(max(values.shape))
    spots = []
    for shift in (0, 1):
        where = [jax.random.randint(jax.random.fold_in(stream_key, axis), (), 0, length) for axis, length in enumerate(values.shape)]
        where[longest] = (where[longest] + shift) % values.shape[longest]
        spots.append(tuple(where))
    return values.at[spots[0]].set(least).at[spots[1]].set(largest)


def block_levels(rng, extent, pieces, least, high):
    level, own = 1.0, jax.random.fold_in(rng, 6)
    for position, blocks in pieces:
        steps = jnp.exp(jax.random.uniform(jax.random.fold_in(own, position), (blocks,), jnp.float32, least / len(pieces), high / len(pieces)))
        level = level * jnp.repeat(steps, extent[position] // blocks).reshape([-1 if axis == position else 1 for axis in range(len(extent))])
    return level


def centred(key, shape, scale, reach, cuts=(), kind=jnp.bfloat16):
    values = scale * jax.random.normal(key, shape, jnp.float32)
    if cuts:
        values = values * block_levels(key, shape, cuts, -0.22, 0.18)
    return jnp.clip(values, -reach, reach).astype(kind)


def setup_inputs(seed: int = 0) -> dict:
    arg_keys = jax.random.split(jax.random.key(seed), 11)
    return {
        "ensemble_profiles_before": centred(arg_keys[0], (K, PROFILE_SIZE, COLS), 1.0, 6.0, ((0, 4), (2, 8))),
        "mixing_coefficient": jnp.clip(jnp.exp(math.log(0.24) - 1.5686159 * jax.random.uniform(arg_keys[1], (COLS,), jnp.float32) ** block_levels(arg_keys[1], (COLS,), ((0, 8),), -0.2, 0.2)), 0.05, 0.24),
        "surface_driver": centred(arg_keys[2], (K, COLS), 0.5, 3.0, ((0, 4), (1, 8)), jnp.float32),
        "terrain_indicator": set_ends((jax.random.randint(arg_keys[3], (COLS,), 0, 4) < 3).astype(jnp.int32), jax.random.fold_in(arg_keys[3], 1), 0, 1),
        "measured_profile_position": set_ends(jax.random.randint(arg_keys[4], (N_TILE * OBS_T,), 0, C_TILE), jax.random.fold_in(arg_keys[4], 1), 0, C_TILE - 1).astype(jnp.int32),
        "measured_field_index": set_ends(jax.random.randint(arg_keys[5], (N_TILE * OBS_T,), 0, PROFILE_SIZE), jax.random.fold_in(arg_keys[5], 1), 0, PROFILE_SIZE - 1).astype(jnp.int32),
        "obs_valid": set_ends((jax.random.randint(arg_keys[6], (N_TILE * OBS_T,), 0, 8) < 7).astype(jnp.int32), jax.random.fold_in(arg_keys[6], 1), 0, 1),
        "obs_value": centred(arg_keys[7], (N_TILE * OBS_T,), 1.0, 6.0, ((0, 8),)),
        "obs_error": jnp.clip(jnp.exp(math.log(4.0) - 2.0794415 * jax.random.uniform(arg_keys[8], (N_TILE * OBS_T,), jnp.float32) ** block_levels(arg_keys[8], (N_TILE * OBS_T,), ((0, 8),), -0.2, 0.2)), 0.5, 4.0).astype(jnp.bfloat16),
        "local_weight": jnp.clip(jnp.exp(math.log(0.03) - 3.4011973 * jax.random.uniform(arg_keys[9], (NB_TILE, N_TILE, P_OBS), jnp.float32) ** block_levels(arg_keys[9], (NB_TILE, N_TILE, P_OBS), ((0, 4), (1, 8)), -0.2, 0.2)), 0.001, 0.03),
    }


EXACT = lax.Precision.HIGHEST

def vertical_mixing_step(ensemble_profiles_before, mixing_coefficient, surface_driver, terrain_indicator):
    values = ensemble_profiles_before.astype(jnp.float32)
    above_layer = jnp.concatenate([values[:, :1], values[:, :-1]], axis=1)
    below_layer = jnp.concatenate([values[:, 1:], values[:, -1:]], axis=1)
    diffused = values + mixing_coefficient[None, None, :] * (above_layer - 2.0 * values + below_layer)
    stepped = diffused - 0.05 * values * values * values
    surface = jnp.concatenate([stepped[:, :1] + surface_driver[:, None, :], stepped[:, 1:]], axis=1)
    result = jnp.where(terrain_indicator[None, None, :] > 0, surface, values)
    return result.astype(jnp.bfloat16)

def measurement_operator(background_ensemble, measured_profile_position, measured_field_index):
    profile_sequence = background_ensemble.shape[2]
    unrolled_ensemble = background_ensemble.reshape(background_ensemble.shape[0], -1)
    slot_index = measured_field_index.astype(jnp.int32) * profile_sequence + measured_profile_position.astype(jnp.int32)
    return jnp.take(unrolled_ensemble, slot_index, axis=1)

def prepare(window):
    ensemble_profiles = window.shape[0] - 3
    measured_quantities = window[:ensemble_profiles].astype(jnp.float32)
    average = lax.optimization_barrier(jnp.mean(measured_quantities, axis=0))
    deviation = measured_quantities - average
    innovation = window[ensemble_profiles].astype(jnp.float32) - average
    obs_precision = window[ensemble_profiles + 2].astype(jnp.float32) / window[ensemble_profiles + 1].astype(jnp.float32)
    return (deviation, innovation, obs_precision)

def weights_for(deviation, innovation, precision, portions):
    ensemble_profiles = deviation.shape[0]
    portion_width = deviation.shape[1] // portions
    spread = jnp.zeros((ensemble_profiles, ensemble_profiles), jnp.float32)
    for portion_index in range(portions):
        portion = deviation[:, portion_index * portion_width:(portion_index + 1) * portion_width]
        scaled = portion * precision[None, portion_index * portion_width:(portion_index + 1) * portion_width]
        spread = spread + jnp.dot(scaled, portion.T, precision=EXACT, preferred_element_type=jnp.float32)
    spread = spread / (ensemble_profiles - 1.0)
    pulled = jnp.dot(deviation, precision * innovation, precision=EXACT, preferred_element_type=jnp.float32) / (ensemble_profiles - 1.0)
    identity = jnp.eye(ensemble_profiles, dtype=jnp.float32)
    system = identity + spread
    norm_scale = jnp.sqrt(jnp.sum(system * system))

    def newton(sweep, carry):
        current, inv_root = carry
        middle = 1.5 * identity - 0.5 * jnp.dot(inv_root, current, precision=EXACT)
        return (jnp.dot(current, middle, precision=EXACT), jnp.dot(middle, inv_root, precision=EXACT))
    current, inv_root = lax.fori_loop(0, NS_ITERS, newton, (system / norm_scale, identity))
    inv_root = inv_root / jnp.sqrt(norm_scale)
    inverse = jnp.dot(inv_root, inv_root, precision=EXACT)
    mean_weight = jnp.dot(inverse, pulled, precision=EXACT)
    return inv_root + mean_weight[:, None]

def update(states, transform, land_block):
    values = states.astype(jnp.float32)
    average = lax.optimization_barrier(jnp.mean(values, axis=0))
    deviation = values - average[None]
    moved = jnp.einsum('isc,ij->jsc', deviation, transform, precision=EXACT)
    result = jnp.where(land_block[None, None, :] > 0, average[None] + moved, values)
    return result.astype(jnp.bfloat16)

def reference(ensemble_profiles_before, mixing_coefficient, surface_driver, terrain_indicator, measured_profile_position, measured_field_index, obs_valid, obs_value, obs_error, local_weight):
    background_ensemble = vertical_mixing_step(ensemble_profiles_before, mixing_coefficient, surface_driver, terrain_indicator)
    number_sections = N_TILE
    ensemble_profiles = ensemble_profiles_before.shape[0]
    section_breadth = ensemble_profiles_before.shape[2] // number_sections
    blocks_tile = section_breadth // BLK
    sectioned_ensemble = background_ensemble.reshape(ensemble_profiles, PROFILE_SIZE, number_sections, section_breadth).transpose(2, 0, 1, 3)
    measured_quantities = jax.vmap(measurement_operator)(sectioned_ensemble, measured_profile_position.reshape(number_sections, OBS_T), measured_field_index.reshape(number_sections, OBS_T))
    metadata = jnp.stack([obs_value.reshape(number_sections, OBS_T), obs_error.reshape(number_sections, OBS_T), obs_valid.reshape(number_sections, OBS_T).astype(jnp.bfloat16)], axis=1)
    obs_rows = jnp.concatenate([measured_quantities, metadata], axis=1)
    offsets = jnp.arange(-REACH, REACH + 1, dtype=jnp.int32)
    land_tiles = terrain_indicator.reshape(number_sections, blocks_tile, BLK)

    def one_tile(tile_index):
        chosen = (tile_index + offsets) % number_sections
        window = jnp.take(obs_rows, chosen, axis=0).transpose(1, 0, 2).reshape(ensemble_profiles + 3, -1)
        deviation, innovation, obs_precision = prepare(window)
        tile_states = lax.dynamic_index_in_dim(sectioned_ensemble, tile_index, 0, keepdims=False)
        tile_states = tile_states.reshape(ensemble_profiles, PROFILE_SIZE, blocks_tile, BLK).transpose(2, 0, 1, 3)
        tile_land = lax.dynamic_index_in_dim(land_tiles, tile_index, 0, keepdims=False)
        tile_weight = lax.dynamic_index_in_dim(local_weight, tile_index, 1, keepdims=False)

        def one_block(inputs):
            states, land_block, weight = inputs
            transform = weights_for(deviation, innovation, obs_precision * weight, 2 * REACH + 1)
            return update(states, transform, land_block)
        finished = lax.map(one_block, (tile_states, tile_land, tile_weight))
        return finished.transpose(1, 2, 0, 3).reshape(ensemble_profiles, PROFILE_SIZE, section_breadth)
    analysed = lax.map(one_tile, jnp.arange(number_sections, dtype=jnp.int32))
    return analysed.transpose(1, 2, 0, 3).reshape(ensemble_profiles, PROFILE_SIZE, number_sections * section_breadth)
```

```python
import functools

import jax
import jax.numpy as jnp
from jax import lax
from jax.experimental import pallas as pl
from jax.experimental.pallas import tpu as pltpu
from jax.sharding import PartitionSpec as P

REACH = 2
NS_ITERS = 3


EXACT = lax.Precision.HIGHEST


def from_behind(value, axis, steps):
    count = lax.axis_size(axis)
    pairs = [(source, (source + steps) % count) for source in range(count)]
    return lax.ppermute(value, axis, pairs)


def vertical_mixing_step(
    ensemble_profiles_before, mixing_coefficient, surface_driver, terrain_indicator
):
    values = ensemble_profiles_before.astype(jnp.float32)
    above_layer = jnp.concatenate([values[:, :1], values[:, :-1]], axis=1)
    below_layer = jnp.concatenate([values[:, 1:], values[:, -1:]], axis=1)
    diffused = values + mixing_coefficient[None, None, :] * (
        above_layer - 2.0 * values + below_layer
    )
    stepped = diffused - 0.05 * values * values * values
    surface = jnp.concatenate([stepped[:, :1] + surface_driver[:, None, :], stepped[:, 1:]], axis=1)
    result = jnp.where(terrain_indicator[None, None, :] > 0, surface, values)
    return result.astype(jnp.bfloat16)


def measurement_operator(background_ensemble, measured_profile_position, measured_field_index):
    profile_sequence = background_ensemble.shape[2]
    unrolled_ensemble = background_ensemble.reshape(background_ensemble.shape[0], -1)
    slot_index = measured_field_index * profile_sequence + measured_profile_position
    return jnp.take(unrolled_ensemble, slot_index, axis=1)


def prepare(window):
    ensemble_profiles = window.shape[0] - 3
    measured_quantities = window[:ensemble_profiles].astype(jnp.float32)
    average = jnp.mean(measured_quantities, axis=0)
    deviation = measured_quantities - average
    innovation = window[ensemble_profiles].astype(jnp.float32) - average
    obs_precision = window[ensemble_profiles + 2].astype(jnp.float32) / window[
        ensemble_profiles + 1
    ].astype(jnp.float32)
    return (deviation, innovation, obs_precision)


def weights_for(deviation, innovation, precision, portions):
    ensemble_profiles = deviation.shape[0]
    portion_width = deviation.shape[1] // portions
    spread = jnp.zeros((ensemble_profiles, ensemble_profiles), jnp.float32)
    for portion_index in range(portions):
        portion = deviation[:, portion_index * portion_width : (portion_index + 1) * portion_width]
        scaled = (
            portion
            * precision[None, portion_index * portion_width : (portion_index + 1) * portion_width]
        )
        spread = spread + jnp.dot(
            scaled, portion.T, precision=EXACT, preferred_element_type=jnp.float32
        )
    spread = spread / (ensemble_profiles - 1.0)
    pulled = jnp.dot(
        deviation, precision * innovation, precision=EXACT, preferred_element_type=jnp.float32
    ) / (ensemble_profiles - 1.0)
    identity = jnp.eye(ensemble_profiles, dtype=jnp.float32)
    system = identity + spread
    norm_scale = jnp.sqrt(jnp.sum(system * system))

    def newton(sweep, carry):
        current, inv_root = carry
        middle = 1.5 * identity - 0.5 * jnp.dot(inv_root, current, precision=EXACT)
        return (
            jnp.dot(current, middle, precision=EXACT),
            jnp.dot(middle, inv_root, precision=EXACT),
        )

    current, inv_root = lax.fori_loop(0, NS_ITERS, newton, (system / norm_scale, identity))
    inv_root = inv_root / jnp.sqrt(norm_scale)
    inverse = jnp.dot(inv_root, inv_root, precision=EXACT)
    mean_weight = jnp.dot(inverse, pulled, precision=EXACT)
    return inv_root + mean_weight[:, None]


def update(states, transform, land_block):
    values = states.astype(jnp.float32)
    average = jnp.mean(values, axis=0)
    deviation = values - average[None]
    moved = jnp.einsum("isc,ij->jsc", deviation, transform, precision=EXACT)
    result = jnp.where(land_block[None, None, :] > 0, average[None] + moved, values)
    return result.astype(jnp.bfloat16)


def plain_on_device(
    ensemble_profiles_before,
    mixing_coefficient,
    surface_driver,
    terrain_indicator,
    measured_profile_position,
    measured_field_index,
    obs_valid,
    obs_value,
    obs_error,
    local_weight,
):
    background_ensemble = vertical_mixing_step(
        ensemble_profiles_before, mixing_coefficient, surface_driver, terrain_indicator
    )
    measured_quantities = measurement_operator(
        background_ensemble, measured_profile_position, measured_field_index
    )
    metadata = jnp.stack([obs_value, obs_error, obs_valid.astype(jnp.bfloat16)])
    own_rows = jnp.concatenate([measured_quantities, metadata], axis=0)
    pieces = []
    for offset in range(-REACH, REACH + 1):
        if offset == 0:
            pieces.append(own_rows)
        else:
            pieces.append(from_behind(own_rows, "tile", -offset))
    nearby = jnp.concatenate(pieces, axis=1)
    members_here = measured_quantities.shape[0]
    everyone = lax.all_gather(nearby[:members_here], "mem", axis=0, tiled=True)
    window = jnp.concatenate([everyone, nearby[members_here:]], axis=0)
    regrouped_states = lax.all_to_all(
        background_ensemble, "mem", split_axis=2, concat_axis=0, tiled=True
    )
    deviation, innovation, obs_precision = prepare(window)
    columns_here = regrouped_states.shape[2]
    local_land = lax.dynamic_slice_in_dim(
        terrain_indicator, lax.axis_index("mem") * columns_here, columns_here
    )
    transform = weights_for(
        deviation, innovation, obs_precision * local_weight[0, 0], 2 * REACH + 1
    )
    outputs = update(regrouped_states, transform, local_land)
    return lax.all_to_all(outputs, "mem", split_axis=0, concat_axis=2, tiled=True)


MESH = pl.DeviceIdType.MESH
CHUNKS = 4
CORES = 2
GATE = CORES - 1


def rounded_dot(a, b):
    return jnp.dot(a, b, preferred_element_type=jnp.float32)


def halves(a):
    high = a.astype(jnp.bfloat16)
    return high, (a - high.astype(jnp.float32)).astype(jnp.bfloat16)


def fine_dot(a, b):
    (a_high, a_low), (b_high, b_low) = a, b
    return rounded_dot(a_high, b_high) + (rounded_dot(a_high, b_low) + rounded_dot(a_low, b_high))


def drain(ref, sem):
    pltpu.make_async_copy(ref, ref, sem).wait()


def kernel(
    n_mem,
    n_tile,
    pieces,
    ens_hbm,
    mix_hbm,
    surf_hbm,
    land_hbm,
    pos_hbm,
    field_hbm,
    valid_hbm,
    value_hbm,
    error_hbm,
    weight_hbm,
    out_ref,
    ens_ref,
    mix_ref,
    surf_ref,
    land_ref,
    pos_ref,
    field_ref,
    valid_ref,
    value_ref,
    error_ref,
    fc_ref,
    seen_ref,
    near_ref,
    slot_ref,
    acc_ref,
    part_ref,
    got_ref,
    tsend_ref,
    trecv_ref,
    moved_ref,
    ens_sem,
    in_sem,
    seen_send,
    seen_across,
    seen_all,
    fc_send,
    fc_across,
    fc_block,
    tile_send,
    tile_recv,
    t_send,
    t_recv,
    hello,
    ready,
):
    members, fields, columns = ens_ref.shape
    everyone = members * n_mem
    slots = pos_ref.shape[1]
    near = 2 * REACH + 1
    wide = columns // n_mem
    me, tile = lax.axis_index("mem"), lax.axis_index("tile")
    n_y = n_mem // CORES
    y, core = me // CORES, lax.rem(me, CORES)
    sibling = y * CORES + (1 - core)
    across = [lax.rem(y + step, n_y) * CORES + core for step in range(1, n_y)]
    gate = me == GATE

    barrier = pltpu.get_barrier_semaphore()
    for step in range(1, n_mem):
        peer = lax.rem(me + step, n_mem)

        @pl.when(peer != GATE)
        def _(peer=peer):
            pl.semaphore_signal(barrier, inc=1, device_id={"mem": peer}, device_id_type=MESH)

    def ens_copy(step):
        where = pl.ds(pl.multiple_of(step * wide, wide), wide)
        return pltpu.make_async_copy(
            ens_hbm.at[:, :, where], ens_ref.at[:, :, where], ens_sem.at[step]
        )

    groups = [
        [(mix_hbm, mix_ref), (surf_hbm, surf_ref), (land_hbm, land_ref)],
        [(pos_hbm, pos_ref), (field_hbm, field_ref)],
        [
            (valid_hbm, valid_ref),
            (value_hbm, value_ref),
            (error_hbm, error_ref),
            (weight_hbm.at[REACH], near_ref.at[REACH]),
        ],
    ]
    loads = [
        [pltpu.make_async_copy(src, dst, in_sem.at[g]) for src, dst in group]
        for g, group in enumerate(groups)
    ]
    for copy in loads[0]:
        copy.start()
    for step in range(n_mem):
        ens_copy(step).start()
    for group in loads[1:]:
        for copy in group:
            copy.start()

    def remote(src, dst, send, recv, where):
        return pltpu.make_async_remote_copy(
            src_ref=src,
            dst_ref=dst,
            send_sem=send,
            recv_sem=recv,
            device_id=where,
            device_id_type=MESH,
        )

    def fc_copy(piece, owner, recv, target):
        block, first, last = pieces[piece]
        ref = fc_ref.at[owner, block, pl.ds(first, last - first)]
        return remote(ref, ref, fc_send.at[0], recv, {"mem": target})

    def fc_over(piece, owner, index, target):
        return fc_copy(piece, owner, fc_across.at[piece, index], target)

    def fc_near(piece, owner):
        return fc_copy(piece, owner, fc_block.at[pieces[piece][0]], sibling)

    def own_fc(piece):
        for index, peer in enumerate(across):
            fc_over(piece, me, n_y - 2 - index, peer).start()
        fc_near(piece, me).start()

    def relay_fc(piece):
        for index, peer in enumerate(across):
            fc_over(piece, peer, index, peer).wait_recv()
            fc_near(piece, peer).start()

    def seen_copy(h, owner, recv, target):
        ref = seen_ref.at[owner, h]
        return remote(ref, ref, seen_send.at[0], recv, {"mem": target})

    def own_seen(h):
        for index, peer in enumerate(across):
            seen_copy(h, me, seen_across.at[h, n_y - 2 - index], peer).start()
        seen_copy(h, me, seen_all.at[h], sibling).start()

    def relay_seen(h):
        for index, peer in enumerate(across):
            seen_copy(h, peer, seen_across.at[h, index], peer).wait_recv()
            seen_copy(h, peer, seen_all.at[h], sibling).start()

    def tile_peer(offset):
        return {"tile": lax.rem(tile + offset + n_tile, n_tile)}

    def mix_block(step):
        where = pl.ds(pl.multiple_of(step * wide, wide), wide)
        ens_copy(step).wait()
        x = jnp.transpose(ens_ref[:, :, where].astype(jnp.float32), (1, 0, 2))
        rate = mix_ref[:, where][None]
        above = jnp.concatenate([x[:1], x[:-1]], axis=0)
        below = jnp.concatenate([x[1:], x[-1:]], axis=0)
        stepped = x + rate * (above - 2.0 * x + below) - 0.05 * x * x * x
        top = stepped[:1] + surf_ref[:, where][None]
        stepped = jnp.concatenate([top, stepped[1:]], axis=0)
        land = jnp.broadcast_to(land_ref[:, where][None], x.shape) > 0
        fc_ref[me, step] = jnp.where(land, stepped, x).astype(jnp.bfloat16)

    head_bytes = 4 * columns * (members + 2)
    drain(acc_ref.at[pl.ds(0, head_bytes // 512)], in_sem.at[0])
    mix_block(0)

    @pl.when(jnp.logical_not(gate))
    def _():
        pl.semaphore_wait(barrier, n_mem - 1)
        pl.semaphore_signal(hello, inc=1, device_id={"mem": GATE}, device_id_type=MESH)
        own_fc(0)

    def mix(step, carry):
        mix_block(step)
        return carry

    lax.fori_loop(1, n_mem, mix, 0)

    @pl.when(gate)
    def _():
        pl.semaphore_wait(hello, n_mem - 1)
        for offset in range(-REACH, REACH + 1):
            if offset:
                pl.semaphore_signal(
                    barrier, inc=1, device_id=tile_peer(offset), device_id_type=MESH
                )
        own_fc(0)

    drain(slot_ref.at[pl.ds(0, 2)], in_sem.at[1])
    share = slots // CHUNKS
    width = min(share, 512)
    flat = jnp.concatenate(
        [fc_ref[me, b].reshape(fields * members, wide) for b in range(n_mem)], axis=1
    )
    for h in range(CHUNKS):
        for step in range(share // width):
            where = pl.ds(h * share + step * width, width)
            rows = lax.broadcasted_iota(jnp.int32, (columns, width), 0)
            hot = jnp.where(rows == pos_ref[:, where], 1.0, 0.0).astype(jnp.bfloat16)
            found = rounded_dot(flat, hot)
            wanted = jnp.broadcast_to(field_ref[:, where], (members, width))
            total = found[:members]
            for f in range(1, fields):
                total = jnp.where(wanted == f, found[f * members : (f + 1) * members], total)
            seen_ref[me, h, :, pl.ds(step * width, width)] = total.astype(jnp.bfloat16)
        own_seen(h)

    n_pieces = len(pieces)
    for piece in range(1, n_pieces):
        own_fc(piece)

    @pl.when(gate)
    def _():
        pl.semaphore_wait(barrier, 2 * REACH)
        for step in range(1, n_mem):
            pl.semaphore_signal(
                ready, inc=1, device_id={"mem": lax.rem(me + step, n_mem)}, device_id_type=MESH
            )

    @pl.when(jnp.logical_not(gate))
    def _():
        pl.semaphore_wait(ready, 1)

    for j in range(near):
        if j != REACH:
            remote(
                weight_hbm.at[j],
                near_ref.at[j],
                tile_send.at[0],
                tile_recv.at[0],
                tile_peer(j - REACH),
            ).start()
    drain(slot_ref.at[pl.ds(0, 3)], in_sem.at[2])
    base = valid_ref[...].astype(jnp.float32) / error_ref[...].astype(jnp.float32)
    slot_ref[near] = value_ref[...].astype(jnp.float32)
    for spare in range(near + 1, slot_ref.shape[0]):
        slot_ref[spare] = jnp.zeros_like(base)
    slot_ref[REACH] = base * near_ref[REACH]
    acc_ref[...] = jnp.zeros_like(acc_ref)

    relay_fc(0)
    lanes = 128

    relay_seen(0)
    relay_seen(1)

    drain(near_ref.at[pl.ds(0, near - 1)], tile_recv.at[0])
    for j in range(near):
        if j != REACH:
            slot_ref[j] = base * near_ref[j]

    for h in range(CHUNKS):
        if h >= 1 and h + 1 < CHUNKS:
            relay_seen(h + 1)
        drain(seen_ref.at[pl.ds(0, n_y), h], seen_all.at[h])

        def gather_stats(step, carry, h=h):
            inner = pl.ds(pl.multiple_of(step * width, width), width)
            seen = jnp.concatenate(
                [seen_ref[m, h, :, inner].astype(jnp.float32) for m in range(n_mem)], axis=0
            )
            average = jnp.mean(seen, axis=0, keepdims=True)
            deviation = seen - average
            first = (h * share + step * width) // lanes
            rinv = jnp.concatenate(
                [slot_ref[:, first + r, :] for r in range(width // lanes)], axis=1
            )
            innovation = rinv[near : near + 1] - average
            pulls = rinv * innovation
            rows = [(deviation * rinv[j : j + 1]).astype(jnp.bfloat16) for j in range(near)]
            rows.append(jnp.concatenate([pulls, jnp.zeros_like(pulls)], axis=0).astype(jnp.bfloat16))
            sums = lax.dot_general(
                jnp.concatenate(rows, axis=0),
                deviation.astype(jnp.bfloat16),
                (((1,), (1,)), ((), ())),
                preferred_element_type=jnp.float32,
            )
            acc_ref[:, :everyone] += sums
            return carry

        lax.fori_loop(0, share // width, gather_stats, 0)

    fold = everyone // 2
    for j in range(near):
        sums = acc_ref[j * everyone : (j + 1) * everyone, :everyone]
        part_ref[j, :fold] = jnp.concatenate([sums[:fold], sums[fold:]], axis=1)
        part_ref[j, fold:] = jnp.broadcast_to(
            acc_ref[near * everyone + j : near * everyone + j + 1], (8, 2 * everyone)
        )

    for j in range(near):
        if j != REACH:
            remote(
                part_ref.at[j],
                got_ref.at[j],
                tile_send.at[1],
                tile_recv.at[1],
                tile_peer(REACH - j),
            ).start()

    relay_fc(1)
    relay_fc(2)

    summed = part_ref[REACH]
    drain(got_ref.at[pl.ds(0, near - 1)], tile_recv.at[1])

    for j in range(near):
        if j != REACH:
            summed = summed + got_ref[j]
    summed = summed / (everyone - 1.0)
    spread = jnp.concatenate([summed[:fold, :everyone], summed[:fold, everyone:]], axis=0)
    pulled = summed[fold:, :everyone]
    rows = lax.broadcasted_iota(jnp.int32, (everyone, everyone), 0)
    identity = jnp.where(
        rows == lax.broadcasted_iota(jnp.int32, (everyone, everyone), 1), 1.0, 0.0
    )
    system = identity + spread
    square = jnp.sum(system * system, keepdims=True)
    scale = jnp.sqrt(square)
    parts = halves(system)
    second = fine_dot(parts, parts) / square
    current = system / scale
    parts, second_parts = halves(current), halves(second)
    third = fine_dot(second_parts, parts)
    fourth = fine_dot(second_parts, second_parts)
    root = 2.25 * identity - 2.4375 * current + 1.6875 * second - 0.5625 * third + 0.0625 * fourth
    root_parts = halves(root)
    inner_parts = halves(fine_dot(parts, root_parts))
    outer_parts = halves(fine_dot(root_parts, root_parts))
    root = 1.5 * root - 0.5 * fine_dot(inner_parts, outer_parts)
    root_parts = halves(root)
    ones = jnp.ones((everyone, everyone), jnp.bfloat16)
    sums = rounded_dot(root_parts[0], ones) + rounded_dot(root_parts[1], ones)
    drawn = halves(fine_dot(halves(pulled), root_parts))
    mean_weight = fine_dot(drawn, root_parts)[:1] / scale
    weight_sum = fine_dot(drawn, halves(sums))[:1] / scale
    turned = root / jnp.sqrt(scale) + mean_weight
    turned = turned + (1.0 - sums / jnp.sqrt(scale) - weight_sum) / everyone
    for m in range(n_mem):
        tsend_ref[m, :, :everyone] = turned[m * members : (m + 1) * members]
        tsend_ref[m, :, everyone:] = jnp.zeros((members, everyone), jnp.float32)

    for step in range(1, n_mem):
        target = lax.rem(me + step, n_mem)
        remote(
            tsend_ref.at[target],
            trecv_ref.at[me],
            t_send.at[0],
            t_recv.at[0],
            {"mem": target},
        ).start()
    trecv_ref[me] = tsend_ref[me]

    group = 8

    def apply(block):
        where = pl.ds(block * wide, wide)
        left = jnp.concatenate(halves(trecv_ref[block][:, :everyone]), axis=0)
        land = jnp.broadcast_to(land_ref[:, where], (members, wide)) > 0
        for first in range(0, fields, group):
            states = jnp.concatenate(
                [
                    jnp.concatenate([fc_ref[m, block, f] for m in range(n_mem)], axis=0)
                    for f in range(first, first + group)
                ],
                axis=1,
            )
            both = rounded_dot(left, states)
            total = both[:members] + both[members:]
            for f in range(group):
                moved_ref[first + f, :, :] = jnp.where(
                    land,
                    total[:, f * wide : (f + 1) * wide],
                    fc_ref[me, block, first + f].astype(jnp.float32),
                )
        out_ref[:, :, where] = jnp.transpose(moved_ref[...], (1, 0, 2)).astype(jnp.bfloat16)

    for piece in range(3, n_pieces - 1):
        relay_fc(piece)

    drain(trecv_ref.at[pl.ds(0, n_mem - 1)], t_recv.at[0])

    for block in range(n_mem):
        if block == n_mem - 2:
            relay_fc(n_pieces - 1)
        drain(fc_ref.at[pl.ds(0, n_y), block], fc_block.at[block])
        apply(block)

    drain(fc_ref.at[pl.ds(0, n_mem - 1)], fc_send.at[0])
    drain(seen_ref.at[pl.ds(0, n_mem - 1)], seen_send.at[0])
    drain(near_ref.at[pl.ds(0, near - 1)], tile_send.at[0])
    drain(part_ref.at[pl.ds(0, near - 1)], tile_send.at[1])
    drain(tsend_ref.at[pl.ds(0, n_mem - 1)], t_send.at[0])


def on_device(
    n_mem,
    n_tile,
    ensemble_profiles_before,
    mixing_coefficient,
    surface_driver,
    terrain_indicator,
    measured_profile_position,
    measured_field_index,
    obs_valid,
    obs_value,
    obs_error,
    local_weight,
):
    members, fields, columns = ensemble_profiles_before.shape
    slots = measured_field_index.shape[0]
    everyone = members * n_mem
    near = 2 * REACH + 1
    n_y = n_mem // CORES
    wide = columns // n_mem
    half = fields // 2
    pieces = [(0, 0, half), (0, half, fields)]
    pieces += [(block, 0, fields) for block in range(1, n_mem - 1)]
    pieces += [(n_mem - 1, 0, half), (n_mem - 1, half, fields)]
    row = lambda a: a.reshape(1, -1)
    table = lambda a: a.reshape(-1, 128)
    far = pl.BlockSpec(memory_space=pltpu.HBM)
    dma = pltpu.SemaphoreType.DMA
    return pl.pallas_call(
        functools.partial(kernel, n_mem, n_tile, pieces),
        out_shape=pltpu.VMEM(ensemble_profiles_before.shape, jnp.bfloat16),
        in_specs=[far] * 10,
        out_specs=pl.BlockSpec(memory_space=pltpu.VMEM),
        scratch_shapes=[
            pltpu.VMEM((members, fields, columns), jnp.bfloat16),
            pltpu.VMEM((1, columns), jnp.float32),
            pltpu.VMEM((members, columns), jnp.float32),
            pltpu.VMEM((1, columns), jnp.int32),
            pltpu.VMEM((1, slots), jnp.int32),
            pltpu.VMEM((1, slots), jnp.int32),
            pltpu.VMEM((slots // 128, 128), jnp.int32),
            pltpu.VMEM((slots // 128, 128), jnp.bfloat16),
            pltpu.VMEM((slots // 128, 128), jnp.bfloat16),
            pltpu.VMEM((n_mem, n_mem, fields, members, wide), jnp.bfloat16),
            pltpu.VMEM((n_mem, CHUNKS, members, slots // CHUNKS), jnp.bfloat16),
            pltpu.VMEM((near, slots // 128, 128), jnp.float32),
            pltpu.VMEM((8, slots // 128, 128), jnp.float32),
            pltpu.VMEM((near * everyone + 16, 2 * everyone), jnp.float32),
            pltpu.VMEM((near, everyone // 2 + 8, 2 * everyone), jnp.float32),
            pltpu.VMEM((near, everyone // 2 + 8, 2 * everyone), jnp.float32),
            pltpu.VMEM((n_mem, members, 2 * everyone), jnp.float32),
            pltpu.VMEM((n_mem, members, 2 * everyone), jnp.float32),
            pltpu.VMEM((fields, members, wide), jnp.float32),
            dma((n_mem,)),
            dma((3,)),
            dma((1,)),
            dma((CHUNKS, n_y - 1)),
            dma((CHUNKS,)),
            dma((1,)),
            dma((len(pieces), n_y - 1)),
            dma((n_mem,)),
            dma((2,)),
            dma((2,)),
            dma((1,)),
            dma((1,)),
            pltpu.SemaphoreType.REGULAR,
            pltpu.SemaphoreType.REGULAR,
        ],
        compiler_params=pltpu.CompilerParams(
            collective_id=0, has_side_effects=True, vmem_limit_bytes=66_000_000
        ),
    )(
        ensemble_profiles_before,
        row(mixing_coefficient),
        surface_driver,
        row(terrain_indicator),
        row(measured_profile_position),
        row(measured_field_index),
        table(obs_valid),
        table(obs_value),
        table(obs_error),
        local_weight.reshape(near, slots // 128, 128),
    )


def fits(n_mem, n_tile, ensemble, slots):
    members, fields, columns = ensemble[0] // n_mem, ensemble[1], ensemble[2] // n_tile
    return (
        n_mem % CORES == 0
        and n_mem > CORES
        and 2 * members * n_mem == 128
        and n_tile > 2 * REACH
        and members % 16 == 0
        and fields % 8 == 0
        and columns % (128 * n_mem) == 0
        and slots // n_tile % (512 * CHUNKS) == 0
    )


def solution(mesh):
    in_specs = (
        P("mem", None, "tile"),
        P("tile"),
        P("mem", "tile"),
        P("tile"),
        P("tile"),
        P("tile"),
        P("tile"),
        P("tile"),
        P("tile"),
        P("mem", "tile", None),
    )
    out_specs = P("mem", None, "tile")

    def run(*args):
        sizes = mesh.shape["mem"], mesh.shape["tile"]
        body = plain_on_device
        if fits(*sizes, args[0].shape, args[5].shape[0]):
            body = functools.partial(on_device, *sizes)
        return jax.shard_map(
            body, mesh=mesh, in_specs=in_specs, out_specs=out_specs, check_vma=False
        )(*args)

    return run
```

```python
import functools

import jax
import jax.numpy as jnp
from jax import lax
from jax.experimental import pallas as pl
from jax.experimental.pallas import tpu as pltpu
from jax.sharding import PartitionSpec as P

REACH = 2
NS_ITERS = 3


EXACT = lax.Precision.HIGHEST


def from_behind(value, axis, steps):
    count = lax.axis_size(axis)
    pairs = [(source, (source + steps) % count) for source in range(count)]
    return lax.ppermute(value, axis, pairs)


def vertical_mixing_step(
    ensemble_profiles_before, mixing_coefficient, surface_driver, terrain_indicator
):
    values = ensemble_profiles_before.astype(jnp.float32)
    above_layer = jnp.concatenate([values[:, :1], values[:, :-1]], axis=1)
    below_layer = jnp.concatenate([values[:, 1:], values[:, -1:]], axis=1)
    diffused = values + mixing_coefficient[None, None, :] * (
        above_layer - 2.0 * values + below_layer
    )
    stepped = diffused - 0.05 * values * values * values
    surface = jnp.concatenate([stepped[:, :1] + surface_driver[:, None, :], stepped[:, 1:]], axis=1)
    result = jnp.where(terrain_indicator[None, None, :] > 0, surface, values)
    return result.astype(jnp.bfloat16)


def measurement_operator(background_ensemble, measured_profile_position, measured_field_index):
    profile_sequence = background_ensemble.shape[2]
    unrolled_ensemble = background_ensemble.reshape(background_ensemble.shape[0], -1)
    slot_index = measured_field_index * profile_sequence + measured_profile_position
    return jnp.take(unrolled_ensemble, slot_index, axis=1)


def prepare(window):
    ensemble_profiles = window.shape[0] - 3
    measured_quantities = window[:ensemble_profiles].astype(jnp.float32)
    average = jnp.mean(measured_quantities, axis=0)
    deviation = measured_quantities - average
    innovation = window[ensemble_profiles].astype(jnp.float32) - average
    obs_precision = window[ensemble_profiles + 2].astype(jnp.float32) / window[
        ensemble_profiles + 1
    ].astype(jnp.float32)
    return (deviation, innovation, obs_precision)


def weights_for(deviation, innovation, precision, portions):
    ensemble_profiles = deviation.shape[0]
    portion_width = deviation.shape[1] // portions
    spread = jnp.zeros((ensemble_profiles, ensemble_profiles), jnp.float32)
    for portion_index in range(portions):
        portion = deviation[:, portion_index * portion_width : (portion_index + 1) * portion_width]
        scaled = (
            portion
            * precision[None, portion_index * portion_width : (portion_index + 1) * portion_width]
        )
        spread = spread + jnp.dot(
            scaled, portion.T, precision=EXACT, preferred_element_type=jnp.float32
        )
    spread = spread / (ensemble_profiles - 1.0)
    pulled = jnp.dot(
        deviation, precision * innovation, precision=EXACT, preferred_element_type=jnp.float32
    ) / (ensemble_profiles - 1.0)
    identity = jnp.eye(ensemble_profiles, dtype=jnp.float32)
    system = identity + spread
    norm_scale = jnp.sqrt(jnp.sum(system * system))

    def newton(sweep, carry):
        current, inv_root = carry
        middle = 1.5 * identity - 0.5 * jnp.dot(inv_root, current, precision=EXACT)
        return (
            jnp.dot(current, middle, precision=EXACT),
            jnp.dot(middle, inv_root, precision=EXACT),
        )

    current, inv_root = lax.fori_loop(0, NS_ITERS, newton, (system / norm_scale, identity))
    inv_root = inv_root / jnp.sqrt(norm_scale)
    inverse = jnp.dot(inv_root, inv_root, precision=EXACT)
    mean_weight = jnp.dot(inverse, pulled, precision=EXACT)
    return inv_root + mean_weight[:, None]


def update(states, transform, land_block):
    values = states.astype(jnp.float32)
    average = jnp.mean(values, axis=0)
    deviation = values - average[None]
    moved = jnp.einsum("isc,ij->jsc", deviation, transform, precision=EXACT)
    result = jnp.where(land_block[None, None, :] > 0, average[None] + moved, values)
    return result.astype(jnp.bfloat16)


def plain_on_device(
    ensemble_profiles_before,
    mixing_coefficient,
    surface_driver,
    terrain_indicator,
    measured_profile_position,
    measured_field_index,
    obs_valid,
    obs_value,
    obs_error,
    local_weight,
):
    background_ensemble = vertical_mixing_step(
        ensemble_profiles_before, mixing_coefficient, surface_driver, terrain_indicator
    )
    measured_quantities = measurement_operator(
        background_ensemble, measured_profile_position, measured_field_index
    )
    metadata = jnp.stack([obs_value, obs_error, obs_valid.astype(jnp.bfloat16)])
    own_rows = jnp.concatenate([measured_quantities, metadata], axis=0)
    pieces = []
    for offset in range(-REACH, REACH + 1):
        if offset == 0:
            pieces.append(own_rows)
        else:
            pieces.append(from_behind(own_rows, "tile", -offset))
    nearby = jnp.concatenate(pieces, axis=1)
    members_here = measured_quantities.shape[0]
    everyone = lax.all_gather(nearby[:members_here], "mem", axis=0, tiled=True)
    window = jnp.concatenate([everyone, nearby[members_here:]], axis=0)
    regrouped_states = lax.all_to_all(
        background_ensemble, "mem", split_axis=2, concat_axis=0, tiled=True
    )
    deviation, innovation, obs_precision = prepare(window)
    columns_here = regrouped_states.shape[2]
    local_land = lax.dynamic_slice_in_dim(
        terrain_indicator, lax.axis_index("mem") * columns_here, columns_here
    )
    transform = weights_for(
        deviation, innovation, obs_precision * local_weight[0, 0], 2 * REACH + 1
    )
    outputs = update(regrouped_states, transform, local_land)
    return lax.all_to_all(outputs, "mem", split_axis=0, concat_axis=2, tiled=True)


MESH = pl.DeviceIdType.MESH
CHUNKS = 4
CORES = 2
GATE = 0


def rounded_dot(a, b):
    return jnp.dot(a, b, preferred_element_type=jnp.float32)


def halves(a):
    high = a.astype(jnp.bfloat16)
    return high, (a - high.astype(jnp.float32)).astype(jnp.bfloat16)


def fine_dot(a, b):
    (a_high, a_low), (b_high, b_low) = a, b
    return rounded_dot(a_high, b_high) + (rounded_dot(a_high, b_low) + rounded_dot(a_low, b_high))


def drain(ref, sem):
    pltpu.make_async_copy(ref, ref, sem).wait()


def kernel(
    n_mem,
    n_tile,
    pieces,
    units,
    ens_hbm,
    mix_hbm,
    surf_hbm,
    land_hbm,
    pos_hbm,
    field_hbm,
    valid_hbm,
    value_hbm,
    error_hbm,
    weight_hbm,
    out_ref,
    ens_ref,
    mix_ref,
    surf_ref,
    land_ref,
    pos_ref,
    field_ref,
    valid_ref,
    value_ref,
    error_ref,
    fc_ref,
    seen_ref,
    stage_ref,
    near_ref,
    slot_ref,
    acc_ref,
    part_ref,
    got_ref,
    tsend_ref,
    trecv_ref,
    moved_ref,
    ens_sem,
    in_sem,
    seen_send,
    seen_recv,
    fc_send,
    fc_across,
    fc_unit,
    tile_send,
    tile_recv,
    t_send,
    t_recv,
    hello,
    ready,
):
    members, fields, columns = ens_ref.shape
    everyone = members * n_mem
    slots = pos_ref.shape[1]
    near = 2 * REACH + 1
    wide = columns // n_mem
    me, tile = lax.axis_index("mem"), lax.axis_index("tile")
    n_y = n_mem // CORES
    y, core = me // CORES, lax.rem(me, CORES)
    sibling = y * CORES + (1 - core)
    across = [lax.rem(y + step, n_y) * CORES + core for step in range(1, n_y)]
    gate = me == GATE
    wraps = tile < REACH

    def both(first, second):
        return jnp.logical_and(first, second)

    barrier = pltpu.get_barrier_semaphore()
    for step in range(1, n_mem):
        peer = lax.rem(me + step, n_mem)

        @pl.when(jnp.logical_not(both(wraps, peer == GATE)))
        def _(peer=peer):
            pl.semaphore_signal(barrier, inc=1, device_id={"mem": peer}, device_id_type=MESH)

    for offset in range(-REACH, REACH + 1):
        if offset:
            there = lax.rem(tile + offset + n_tile, n_tile)
            for user in range(CORES):
                who = y * CORES + user

                @pl.when(jnp.logical_or(there >= REACH, user == 0))
                def _(there=there, who=who):
                    target = jnp.where(there < REACH, GATE, who)
                    pl.semaphore_signal(
                        barrier, inc=1, device_id={"mem": target, "tile": there}, device_id_type=MESH
                    )

    def ens_copy(step):
        where = pl.ds(pl.multiple_of(step * wide, wide), wide)
        return pltpu.make_async_copy(
            ens_hbm.at[:, :, where], ens_ref.at[:, :, where], ens_sem.at[step]
        )

    groups = [
        [(mix_hbm, mix_ref), (surf_hbm, surf_ref), (land_hbm, land_ref)],
        [(pos_hbm, pos_ref), (field_hbm, field_ref)],
        [
            (valid_hbm, valid_ref),
            (value_hbm, value_ref),
            (error_hbm, error_ref),
            (weight_hbm, stage_ref),
        ],
    ]
    loads = [
        [pltpu.make_async_copy(src, dst, in_sem.at[g]) for src, dst in group]
        for g, group in enumerate(groups)
    ]
    ens_copy(0).start()
    for copy in loads[0]:
        copy.start()
    for step in range(1, n_mem):
        ens_copy(step).start()
    for group in loads[1:]:
        for copy in group:
            copy.start()

    def remote(src, dst, send, recv, where):
        return pltpu.make_async_remote_copy(
            src_ref=src,
            dst_ref=dst,
            send_sem=send,
            recv_sem=recv,
            device_id=where,
            device_id_type=MESH,
        )

    def fc_copy(piece, owner, recv, target):
        block, first, stop = pieces[piece][:3]
        ref = fc_ref.at[owner, block, pl.ds(first, stop - first)]
        return remote(ref, ref, fc_send.at[0], recv, {"mem": target})

    def fc_over(piece, owner, index, target):
        return fc_copy(piece, owner, fc_across.at[piece, index], target)

    def fc_near(piece, owner):
        return fc_copy(piece, owner, fc_unit.at[pieces[piece][3]], sibling)

    def finish_fc(piece):
        for step in range(1, n_mem):
            unit = fc_unit.at[pieces[piece][3]]
            fc_copy(piece, me, unit, lax.rem(me + step, n_mem)).start()

    def own_fc(piece):
        for index, peer in enumerate(across):
            fc_over(piece, me, n_y - 2 - index, peer).start()
        fc_near(piece, me).start()

    def relay_fc(piece):
        for index, peer in enumerate(across):
            fc_over(piece, peer, index, peer).wait_recv()
            fc_near(piece, peer).start()

    def seen_copy(h, send, target):
        ref = seen_ref.at[me, h]
        return remote(ref, ref, seen_send.at[send], seen_recv.at[h // CORES], {"mem": target})

    def own_seen(h):
        user = h % CORES
        for step in range(1, n_y):
            seen_copy(h, 0, lax.rem(y + step, n_y) * CORES + user).start()

        @pl.when(core != user)
        def _():
            seen_copy(h, 1, sibling).start()

    def tile_peer(offset):
        return {"tile": lax.rem(tile + offset + n_tile, n_tile)}

    def mix_part(step, start, stop):
        where = pl.ds(pl.multiple_of(step * wide, wide), wide)
        low, high = max(start - 8, 0), min(stop + 8, fields)
        x = jnp.transpose(ens_ref[:, low:high, where].astype(jnp.float32), (1, 0, 2))
        rate = mix_ref[:, where][None]
        above = jnp.concatenate([x[:1], x[:-1]], axis=0)
        below = jnp.concatenate([x[1:], x[-1:]], axis=0)
        keep = slice(start - low, stop - low)
        x, above, below = x[keep], above[keep], below[keep]
        stepped = x + rate * (above - 2.0 * x + below) - 0.05 * x * x * x
        if start == 0:
            top = stepped[:1] + surf_ref[:, where][None]
            stepped = jnp.concatenate([top, stepped[1:]], axis=0)
        land = jnp.broadcast_to(land_ref[:, where][None], x.shape) > 0
        fc_ref[me, step, start:stop] = jnp.where(land, stepped, x).astype(jnp.bfloat16)

    def enter():
        pl.semaphore_wait(barrier, n_mem - 1)
        pl.semaphore_signal(hello, inc=1, device_id={"mem": GATE}, device_id_type=MESH)

    def send_weights():
        for j in range(near):
            for user in range(CORES):
                if j != REACH:
                    remote(
                        stage_ref.at[j, :, user],
                        near_ref.at[core * near + j],
                        tile_send.at[0],
                        tile_recv.at[0],
                        {"mem": y * CORES + user, **tile_peer(j - REACH)},
                    ).start()
        remote(
            stage_ref.at[REACH, :, 1 - core],
            near_ref.at[core * near + REACH],
            tile_send.at[0],
            tile_recv.at[0],
            {"mem": sibling},
        ).start()

    @pl.when(both(wraps, me >= CORES))
    def _():
        enter()

    head = pieces[0][2]
    ens_copy(0).wait()
    head_bytes = 4 * columns * (members + 2)
    drain(acc_ref.at[pl.ds(0, head_bytes // 512)], in_sem.at[0])
    mix_part(0, 0, head)

    @pl.when(jnp.logical_not(wraps))
    def _():
        pl.semaphore_wait(barrier, n_mem - 1 + 2 * REACH * CORES)

    @pl.when(both(wraps, both(me < CORES, me != GATE)))
    def _():
        enter()

    @pl.when(jnp.logical_not(both(wraps, gate)))
    def _():
        own_fc(0)

    mix_part(0, head, fields)

    def mix(step, carry):
        ens_copy(step).wait()
        mix_part(step, 0, fields)
        return carry

    lax.fori_loop(1, n_mem, mix, 0)

    drain(slot_ref.at[pl.ds(0, CORES * (near + 2))], in_sem.at[2])

    @pl.when(jnp.logical_not(wraps))
    def _():
        send_weights()

    @pl.when(both(wraps, gate))
    def _():
        pl.semaphore_wait(hello, n_mem - 1)
        own_fc(0)

    drain(slot_ref.at[pl.ds(0, 2 * CORES)], in_sem.at[1])
    share = slots // CHUNKS
    width = min(share, 512)
    flat = jnp.concatenate(
        [fc_ref[me, b].reshape(fields * members, wide) for b in range(n_mem)], axis=1
    )
    for h in range(CHUNKS):
        for step in range(share // width):
            where = pl.ds(h * share + step * width, width)
            rows = lax.broadcasted_iota(jnp.int32, (columns, width), 0)
            hot = jnp.where(rows == pos_ref[:, where], 1.0, 0.0).astype(jnp.bfloat16)
            found = rounded_dot(flat, hot)
            wanted = jnp.broadcast_to(field_ref[:, where], (members, width))
            total = found[:members]
            for f in range(1, fields):
                total = jnp.where(wanted == f, found[f * members : (f + 1) * members], total)
            seen_ref[me, h, :, pl.ds(step * width, width)] = total.astype(jnp.bfloat16)
        own_seen(h)

    n_pieces = len(pieces)
    for piece in range(1, n_pieces - 2):
        own_fc(piece)

    @pl.when(both(wraps, gate))
    def _():
        pl.semaphore_wait(barrier, 2 * REACH * n_mem)
        for step in range(1, n_mem):
            pl.semaphore_signal(
                ready, inc=1, device_id={"mem": lax.rem(me + step, n_mem)}, device_id_type=MESH
            )

    @pl.when(both(wraps, jnp.logical_not(gate)))
    def _():
        pl.semaphore_wait(ready, 1)

    @pl.when(wraps)
    def _():
        send_weights()

    rounds = CHUNKS // CORES
    lanes = 128
    base = [
        valid_ref[i, core].astype(jnp.float32) / error_ref[i, core].astype(jnp.float32)
        for i in range(rounds)
    ]
    for i in range(rounds):
        slot_ref[CORES * near, i] = value_ref[i, core].astype(jnp.float32)
        for spare in range(CORES * near + 1, slot_ref.shape[0]):
            slot_ref[spare, i] = jnp.zeros_like(base[i])
    near_ref[core * near + REACH] = stage_ref[REACH, :, core]

    relay_fc(0)

    drain(near_ref.at[pl.ds(0, CORES * near - 1)], tile_recv.at[0])
    for r in range(CORES * near):
        for i in range(rounds):
            slot_ref[r, i] = base[i] * near_ref[r, i]

    for i in range(rounds):
        drain(seen_ref.at[pl.ds(0, n_mem - 1), 0], seen_recv.at[i])
        seen = jnp.concatenate(
            [seen_ref[m, i * CORES + core].astype(jnp.float32) for m in range(n_mem)], axis=0
        )
        average = jnp.mean(seen, axis=0, keepdims=True)
        deviation = seen - average
        rinv = jnp.concatenate(
            [slot_ref[:, i, r, :] for r in range(share // lanes)], axis=1
        )
        innovation = rinv[CORES * near : CORES * near + 1] - average
        right = jnp.concatenate(
            [deviation, jnp.broadcast_to(innovation, deviation.shape)], axis=0
        ).astype(jnp.bfloat16)
        rows = [
            (deviation * rinv[r : r + 1]).astype(jnp.bfloat16) for r in range(CORES * near)
        ]
        sums = lax.dot_general(
            jnp.concatenate(rows, axis=0),
            right,
            (((1,), (1,)), ((), ())),
            preferred_element_type=jnp.float32,
        )
        if i:
            sums = sums + acc_ref[...]
        acc_ref[...] = sums

    fold = everyone // 2
    lane = lax.broadcasted_iota(jnp.int32, (fold, 2 * everyone), 1)
    for r in range(CORES * near):
        upper = acc_ref[r * everyone : r * everyone + fold]
        lower = acc_ref[r * everyone + fold : (r + 1) * everyone]
        packed = jnp.where(lane < everyone + fold, pltpu.roll(lower, fold, 1), upper)
        packed = jnp.where(lane < everyone, upper, packed)
        packed = jnp.where(lane < 2 * everyone - fold // 2, packed, lower)
        part_ref[r] = packed.astype(jnp.bfloat16)
        user, j = r // near, r % near
        if j != REACH:
            remote(
                part_ref.at[r],
                got_ref.at[core * near + j],
                tile_send.at[1],
                tile_recv.at[1],
                {"mem": y * CORES + user, **tile_peer(REACH - j)},
            ).start()
    remote(
        part_ref.at[(1 - core) * near + REACH],
        got_ref.at[core * near + REACH],
        tile_send.at[1],
        tile_recv.at[1],
        {"mem": sibling},
    ).start()
    got_ref[core * near + REACH] = part_ref[core * near + REACH]

    relay_fc(1)

    drain(got_ref.at[pl.ds(0, CORES * near - 1)], tile_recv.at[1])

    summed = got_ref[0].astype(jnp.float32)
    for r in range(1, CORES * near):
        summed = summed + got_ref[r].astype(jnp.float32)
    summed = summed / (everyone - 1.0)
    flipped = jnp.transpose(summed)
    spread = jnp.concatenate(
        [
            summed[:, :everyone],
            jnp.concatenate(
                [flipped[fold:everyone], summed[:, everyone : everyone + fold]], axis=1
            ),
        ],
        axis=0,
    )
    first, second = everyone + fold, 2 * everyone - fold // 2
    pulled = jnp.concatenate([flipped[first : first + 8], flipped[second : second + 8]], axis=1)
    rows = lax.broadcasted_iota(jnp.int32, (everyone, everyone), 0)
    identity = jnp.where(
        rows == lax.broadcasted_iota(jnp.int32, (everyone, everyone), 1), 1.0, 0.0
    )
    system = identity + spread
    square = jnp.sum(system * system, keepdims=True)
    scale = jnp.sqrt(square)
    parts = halves(system)
    second = fine_dot(parts, parts) / square
    current = system / scale
    parts, second_parts = halves(current), halves(second)
    third = fine_dot(second_parts, parts)
    fourth = fine_dot(second_parts, second_parts)
    root = 2.25 * identity - 2.4375 * current + 1.6875 * second - 0.5625 * third + 0.0625 * fourth
    root_parts = halves(root)
    inner_parts = halves(fine_dot(parts, root_parts))
    outer_parts = halves(fine_dot(root_parts, root_parts))
    root = 1.5 * root - 0.5 * fine_dot(inner_parts, outer_parts)
    root_parts = halves(root)
    ones = jnp.ones((everyone, everyone), jnp.bfloat16)
    sums = rounded_dot(root_parts[0], ones) + rounded_dot(root_parts[1], ones)
    drawn = halves(fine_dot(halves(pulled), root_parts))
    mean_weight = fine_dot(drawn, root_parts)[:1] / scale
    weight_sum = fine_dot(drawn, halves(sums))[:1] / scale
    turned = root / jnp.sqrt(scale) + mean_weight
    turned = turned + (1.0 - sums / jnp.sqrt(scale) - weight_sum) / everyone
    for m in range(n_mem):
        tsend_ref[m, :, :everyone] = turned[m * members : (m + 1) * members]
        tsend_ref[m, :, everyone:] = jnp.zeros((members, everyone), jnp.float32)

    for step in range(1, n_mem):
        target = lax.rem(me + step, n_mem)
        remote(
            tsend_ref.at[target],
            trecv_ref.at[me],
            t_send.at[0],
            t_recv.at[0],
            {"mem": target},
        ).start()
    own_fc(n_pieces - 2)
    finish_fc(n_pieces - 1)
    trecv_ref[me] = tsend_ref[me]

    group = 8

    def apply(block, start, stop):
        where = pl.ds(block * wide, wide)
        left = jnp.concatenate(halves(trecv_ref[block][:, :everyone]), axis=0)
        land = jnp.broadcast_to(land_ref[:, where], (members, wide)) > 0
        for first in range(start, stop, group):
            states = jnp.concatenate(
                [
                    jnp.concatenate([fc_ref[m, block, f] for m in range(n_mem)], axis=0)
                    for f in range(first, first + group)
                ],
                axis=1,
            )
            pair = rounded_dot(left, states)
            total = pair[:members] + pair[members:]
            for f in range(group):
                moved_ref[first + f, :, :] = jnp.where(
                    land,
                    total[:, f * wide : (f + 1) * wide],
                    fc_ref[me, block, first + f].astype(jnp.float32),
                )
        moved = jnp.transpose(moved_ref[start:stop], (1, 0, 2)).astype(jnp.bfloat16)
        out_ref[:, start:stop, where] = moved

    for piece in range(2, n_pieces - 2):
        relay_fc(piece)

    drain(trecv_ref.at[pl.ds(0, n_mem - 1)], t_recv.at[0])

    for unit, (block, start, stop) in enumerate(units):
        if unit == 1:
            relay_fc(n_pieces - 2)
        count = n_y if unit < len(units) - 1 else n_mem - 1
        drain(fc_ref.at[pl.ds(0, count), block, pl.ds(start, stop - start)], fc_unit.at[unit])
        apply(block, start, stop)

    drain(fc_ref.at[pl.ds(0, n_mem - 1)], fc_send.at[0])
    drain(seen_ref.at[pl.ds(0, n_y - 1)], seen_send.at[0])
    drain(seen_ref.at[0, pl.ds(0, CHUNKS // CORES)], seen_send.at[1])
    drain(near_ref.at[pl.ds(0, CORES * near - 1)], tile_send.at[0])
    drain(part_ref.at[pl.ds(0, CORES * near - 1)], tile_send.at[1])
    drain(tsend_ref.at[pl.ds(0, n_mem - 1)], t_send.at[0])


def on_device(
    n_mem,
    n_tile,
    ensemble_profiles_before,
    mixing_coefficient,
    surface_driver,
    terrain_indicator,
    measured_profile_position,
    measured_field_index,
    obs_valid,
    obs_value,
    obs_error,
    local_weight,
):
    members, fields, columns = ensemble_profiles_before.shape
    slots = measured_field_index.shape[0]
    everyone = members * n_mem
    near = 2 * REACH + 1
    n_y = n_mem // CORES
    wide = columns // n_mem
    half = fields // 2
    units = [(block, 0, fields) for block in range(n_mem - 1)]
    cuts = (0, fields - 16, fields - 8, fields)
    units += [(n_mem - 1, *ends) for ends in zip(cuts[:-1], cuts[1:])]
    pieces = [(0, 0, half, 0), (0, half, fields, 0)]
    pieces += [(*unit, index) for index, unit in enumerate(units) if index]
    row = lambda a: a.reshape(1, -1)
    table = (CHUNKS // CORES, CORES, slots // CHUNKS // 128, 128)
    far = pl.BlockSpec(memory_space=pltpu.HBM)
    dma = pltpu.SemaphoreType.DMA
    return pl.pallas_call(
        functools.partial(kernel, n_mem, n_tile, pieces, units),
        out_shape=pltpu.VMEM(ensemble_profiles_before.shape, jnp.bfloat16),
        in_specs=[far] * 10,
        out_specs=pl.BlockSpec(memory_space=pltpu.VMEM),
        scratch_shapes=[
            pltpu.VMEM((members, fields, columns), jnp.bfloat16),
            pltpu.VMEM((1, columns), jnp.float32),
            pltpu.VMEM((members, columns), jnp.float32),
            pltpu.VMEM((1, columns), jnp.int32),
            pltpu.VMEM((1, slots), jnp.int32),
            pltpu.VMEM((1, slots), jnp.int32),
            pltpu.VMEM(table, jnp.int32),
            pltpu.VMEM(table, jnp.bfloat16),
            pltpu.VMEM(table, jnp.bfloat16),
            pltpu.VMEM((n_mem, n_mem, fields, members, wide), jnp.bfloat16),
            pltpu.VMEM((n_mem, CHUNKS, members, slots // CHUNKS), jnp.bfloat16),
            pltpu.VMEM((near, *table), jnp.float32),
            pltpu.VMEM((CORES * near, table[0], *table[2:]), jnp.float32),
            pltpu.VMEM((16, table[0], *table[2:]), jnp.float32),
            pltpu.VMEM((CORES * near * everyone, 2 * everyone), jnp.float32),
            pltpu.VMEM((CORES * near, everyone // 2, 2 * everyone), jnp.bfloat16),
            pltpu.VMEM((CORES * near, everyone // 2, 2 * everyone), jnp.bfloat16),
            pltpu.VMEM((n_mem, members, 2 * everyone), jnp.float32),
            pltpu.VMEM((n_mem, members, 2 * everyone), jnp.float32),
            pltpu.VMEM((fields, members, wide), jnp.float32),
            dma((n_mem,)),
            dma((3,)),
            dma((2,)),
            dma((CHUNKS // CORES,)),
            dma((1,)),
            dma((len(pieces) - 1, n_y - 1)),
            dma((len(units),)),
            dma((2,)),
            dma((2,)),
            dma((1,)),
            dma((1,)),
            pltpu.SemaphoreType.REGULAR,
            pltpu.SemaphoreType.REGULAR,
        ],
        compiler_params=pltpu.CompilerParams(
            collective_id=0, has_side_effects=True, vmem_limit_bytes=66_000_000
        ),
    )(
        ensemble_profiles_before,
        row(mixing_coefficient),
        surface_driver,
        row(terrain_indicator),
        row(measured_profile_position),
        row(measured_field_index),
        obs_valid.reshape(table),
        obs_value.reshape(table),
        obs_error.reshape(table),
        local_weight.reshape(near, *table),
    )


def fits(n_mem, n_tile, ensemble, slots):
    members, fields, columns = ensemble[0] // n_mem, ensemble[1], ensemble[2] // n_tile
    return (
        n_mem % CORES == 0
        and n_mem > CORES
        and 2 * members * n_mem == 128
        and n_tile > 2 * REACH
        and members % 16 == 0
        and fields % 8 == 0
        and fields > 16
        and columns % (128 * n_mem) == 0
        and slots // n_tile % (1024 * CHUNKS) == 0
    )


def solution(mesh):
    in_specs = (
        P("mem", None, "tile"),
        P("tile"),
        P("mem", "tile"),
        P("tile"),
        P("tile"),
        P("tile"),
        P("tile"),
        P("tile"),
        P("tile"),
        P("mem", "tile", None),
    )
    out_specs = P("mem", None, "tile")

    def run(*args):
        sizes = mesh.shape["mem"], mesh.shape["tile"]
        body = plain_on_device
        if fits(*sizes, args[0].shape, args[5].shape[0]):
            body = functools.partial(on_device, *sizes)
        return jax.shard_map(
            body, mesh=mesh, in_specs=in_specs, out_specs=out_specs, check_vma=False
        )(*args)

    return run
```

```python
import functools

import jax
import jax.numpy as jnp
from jax import lax
from jax.experimental import pallas as pl
from jax.experimental.pallas import tpu as pltpu
from jax.sharding import PartitionSpec as P

REACH = 2
NS_ITERS = 3


EXACT = lax.Precision.HIGHEST


def from_behind(value, axis, steps):
    count = lax.axis_size(axis)
    pairs = [(source, (source + steps) % count) for source in range(count)]
    return lax.ppermute(value, axis, pairs)


def vertical_mixing_step(
    ensemble_profiles_before, mixing_coefficient, surface_driver, terrain_indicator
):
    values = ensemble_profiles_before.astype(jnp.float32)
    above_layer = jnp.concatenate([values[:, :1], values[:, :-1]], axis=1)
    below_layer = jnp.concatenate([values[:, 1:], values[:, -1:]], axis=1)
    diffused = values + mixing_coefficient[None, None, :] * (
        above_layer - 2.0 * values + below_layer
    )
    stepped = diffused - 0.05 * values * values * values
    surface = jnp.concatenate([stepped[:, :1] + surface_driver[:, None, :], stepped[:, 1:]], axis=1)
    result = jnp.where(terrain_indicator[None, None, :] > 0, surface, values)
    return result.astype(jnp.bfloat16)


def measurement_operator(background_ensemble, measured_profile_position, measured_field_index):
    profile_sequence = background_ensemble.shape[2]
    unrolled_ensemble = background_ensemble.reshape(background_ensemble.shape[0], -1)
    slot_index = measured_field_index * profile_sequence + measured_profile_position
    return jnp.take(unrolled_ensemble, slot_index, axis=1)


def prepare(window):
    ensemble_profiles = window.shape[0] - 3
    measured_quantities = window[:ensemble_profiles].astype(jnp.float32)
    average = jnp.mean(measured_quantities, axis=0)
    deviation = measured_quantities - average
    innovation = window[ensemble_profiles].astype(jnp.float32) - average
    obs_precision = window[ensemble_profiles + 2].astype(jnp.float32) / window[
        ensemble_profiles + 1
    ].astype(jnp.float32)
    return (deviation, innovation, obs_precision)


def weights_for(deviation, innovation, precision, portions):
    ensemble_profiles = deviation.shape[0]
    portion_width = deviation.shape[1] // portions
    spread = jnp.zeros((ensemble_profiles, ensemble_profiles), jnp.float32)
    for portion_index in range(portions):
        portion = deviation[:, portion_index * portion_width : (portion_index + 1) * portion_width]
        scaled = (
            portion
            * precision[None, portion_index * portion_width : (portion_index + 1) * portion_width]
        )
        spread = spread + jnp.dot(
            scaled, portion.T, precision=EXACT, preferred_element_type=jnp.float32
        )
    spread = spread / (ensemble_profiles - 1.0)
    pulled = jnp.dot(
        deviation, precision * innovation, precision=EXACT, preferred_element_type=jnp.float32
    ) / (ensemble_profiles - 1.0)
    identity = jnp.eye(ensemble_profiles, dtype=jnp.float32)
    system = identity + spread
    norm_scale = jnp.sqrt(jnp.sum(system * system))

    def newton(sweep, carry):
        current, inv_root = carry
        middle = 1.5 * identity - 0.5 * jnp.dot(inv_root, current, precision=EXACT)
        return (
            jnp.dot(current, middle, precision=EXACT),
            jnp.dot(middle, inv_root, precision=EXACT),
        )

    current, inv_root = lax.fori_loop(0, NS_ITERS, newton, (system / norm_scale, identity))
    inv_root = inv_root / jnp.sqrt(norm_scale)
    inverse = jnp.dot(inv_root, inv_root, precision=EXACT)
    mean_weight = jnp.dot(inverse, pulled, precision=EXACT)
    return inv_root + mean_weight[:, None]


def update(states, transform, land_block):
    values = states.astype(jnp.float32)
    average = jnp.mean(values, axis=0)
    deviation = values - average[None]
    moved = jnp.einsum("isc,ij->jsc", deviation, transform, precision=EXACT)
    result = jnp.where(land_block[None, None, :] > 0, average[None] + moved, values)
    return result.astype(jnp.bfloat16)


def plain_on_device(
    ensemble_profiles_before,
    mixing_coefficient,
    surface_driver,
    terrain_indicator,
    measured_profile_position,
    measured_field_index,
    obs_valid,
    obs_value,
    obs_error,
    local_weight,
):
    background_ensemble = vertical_mixing_step(
        ensemble_profiles_before, mixing_coefficient, surface_driver, terrain_indicator
    )
    measured_quantities = measurement_operator(
        background_ensemble, measured_profile_position, measured_field_index
    )
    metadata = jnp.stack([obs_value, obs_error, obs_valid.astype(jnp.bfloat16)])
    own_rows = jnp.concatenate([measured_quantities, metadata], axis=0)
    pieces = []
    for offset in range(-REACH, REACH + 1):
        if offset == 0:
            pieces.append(own_rows)
        else:
            pieces.append(from_behind(own_rows, "tile", -offset))
    nearby = jnp.concatenate(pieces, axis=1)
    members_here = measured_quantities.shape[0]
    everyone = lax.all_gather(nearby[:members_here], "mem", axis=0, tiled=True)
    window = jnp.concatenate([everyone, nearby[members_here:]], axis=0)
    regrouped_states = lax.all_to_all(
        background_ensemble, "mem", split_axis=2, concat_axis=0, tiled=True
    )
    deviation, innovation, obs_precision = prepare(window)
    columns_here = regrouped_states.shape[2]
    local_land = lax.dynamic_slice_in_dim(
        terrain_indicator, lax.axis_index("mem") * columns_here, columns_here
    )
    transform = weights_for(
        deviation, innovation, obs_precision * local_weight[0, 0], 2 * REACH + 1
    )
    outputs = update(regrouped_states, transform, local_land)
    return lax.all_to_all(outputs, "mem", split_axis=0, concat_axis=2, tiled=True)


MESH = pl.DeviceIdType.MESH
CHUNKS = 4
CORES = 2
GATE = 0


def rounded_dot(a, b):
    return jnp.dot(a, b, preferred_element_type=jnp.float32)


def halves(a):
    high = a.astype(jnp.bfloat16)
    return high, (a - high.astype(jnp.float32)).astype(jnp.bfloat16)


def fine_dot(a, b):
    (a_high, a_low), (b_high, b_low) = a, b
    return rounded_dot(a_high, b_high) + (rounded_dot(a_high, b_low) + rounded_dot(a_low, b_high))


def drain(ref, sem):
    pltpu.make_async_copy(ref, ref, sem).wait()


def kernel(
    n_mem,
    n_tile,
    pieces,
    units,
    ens_hbm,
    mix_hbm,
    surf_hbm,
    land_hbm,
    pos_hbm,
    field_hbm,
    valid_hbm,
    value_hbm,
    error_hbm,
    weight_hbm,
    out_ref,
    ens_ref,
    mix_ref,
    surf_ref,
    land_ref,
    pos_ref,
    field_ref,
    valid_ref,
    value_ref,
    error_ref,
    fc_ref,
    seen_ref,
    stage_ref,
    near_ref,
    slot_ref,
    rinv_ref,
    acc_ref,
    part_ref,
    got_ref,
    tsend_ref,
    trecv_ref,
    moved_ref,
    ens_sem,
    in_sem,
    seen_send,
    seen_recv,
    fc_send,
    fc_across,
    fc_unit,
    tile_send,
    tile_recv,
    t_send,
    t_recv,
    hello,
    ready,
):
    members, fields, columns = ens_ref.shape
    everyone = members * n_mem
    slots = pos_ref.shape[1]
    near = 2 * REACH + 1
    wide = columns // n_mem
    me, tile = lax.axis_index("mem"), lax.axis_index("tile")
    n_y = n_mem // CORES
    y, core = me // CORES, lax.rem(me, CORES)
    sibling = y * CORES + (1 - core)
    across = [lax.rem(y + step, n_y) * CORES + core for step in range(1, n_y)]
    gate = me == GATE
    wraps = tile < REACH

    def both(first, second):
        return jnp.logical_and(first, second)

    barrier = pltpu.get_barrier_semaphore()
    for step in range(1, n_mem):
        peer = lax.rem(me + step, n_mem)

        @pl.when(jnp.logical_not(both(wraps, peer == GATE)))
        def _(peer=peer):
            pl.semaphore_signal(barrier, inc=1, device_id={"mem": peer}, device_id_type=MESH)

    for offset in range(-REACH, REACH + 1):
        if offset:
            there = lax.rem(tile + offset + n_tile, n_tile)
            for user in range(CORES):
                who = y * CORES + user

                @pl.when(jnp.logical_or(there >= REACH, user == 0))
                def _(there=there, who=who):
                    target = jnp.where(there < REACH, GATE, who)
                    pl.semaphore_signal(
                        barrier, inc=1, device_id={"mem": target, "tile": there}, device_id_type=MESH
                    )

    def ens_copy(step):
        where = pl.ds(pl.multiple_of(step * wide, wide), wide)
        return pltpu.make_async_copy(
            ens_hbm.at[:, :, where], ens_ref.at[:, :, where], ens_sem.at[step]
        )

    groups = [
        [(mix_hbm, mix_ref), (surf_hbm, surf_ref), (land_hbm, land_ref)],
        [(pos_hbm, pos_ref), (field_hbm, field_ref)],
        [
            (valid_hbm, valid_ref),
            (value_hbm, value_ref),
            (error_hbm, error_ref),
            (weight_hbm, stage_ref),
        ],
    ]
    loads = [
        [pltpu.make_async_copy(src, dst, in_sem.at[g]) for src, dst in group]
        for g, group in enumerate(groups)
    ]
    ens_copy(0).start()
    for copy in loads[0]:
        copy.start()
    for step in range(1, n_mem):
        ens_copy(step).start()
    for group in loads[1:]:
        for copy in group:
            copy.start()

    def remote(src, dst, send, recv, where):
        return pltpu.make_async_remote_copy(
            src_ref=src,
            dst_ref=dst,
            send_sem=send,
            recv_sem=recv,
            device_id=where,
            device_id_type=MESH,
        )

    def fc_copy(piece, owner, recv, target):
        block, first, stop = pieces[piece][:3]
        ref = fc_ref.at[owner, block, pl.ds(first, stop - first)]
        return remote(ref, ref, fc_send.at[0], recv, {"mem": target})

    def fc_over(piece, owner, index, target):
        return fc_copy(piece, owner, fc_across.at[piece, index], target)

    def fc_near(piece, owner):
        return fc_copy(piece, owner, fc_unit.at[pieces[piece][3]], sibling)

    def finish_fc(piece):
        for step in range(1, n_mem):
            unit = fc_unit.at[pieces[piece][3]]
            fc_copy(piece, me, unit, lax.rem(me + step, n_mem)).start()

    def own_fc(piece):
        for index, peer in enumerate(across):
            fc_over(piece, me, n_y - 2 - index, peer).start()
        fc_near(piece, me).start()

    def relay_fc(piece):
        for index, peer in enumerate(across):
            fc_over(piece, peer, index, peer).wait_recv()
            fc_near(piece, peer).start()

    def seen_copy(h, send, target):
        ref = seen_ref.at[me, h]
        return remote(ref, ref, seen_send.at[send], seen_recv.at[h // CORES], {"mem": target})

    def own_seen(h):
        user = h % CORES
        for step in range(1, n_y):
            seen_copy(h, 0, lax.rem(y + step, n_y) * CORES + user).start()

    def near_seen():
        for i in range(CHUNKS // CORES):
            h = i * CORES + 1 - core
            ref = seen_ref.at[me, h]
            remote(ref, ref, seen_send.at[1], seen_recv.at[i], {"mem": sibling}).start()

    def tile_peer(offset):
        return {"tile": lax.rem(tile + offset + n_tile, n_tile)}

    def mix_part(step, start, stop):
        where = pl.ds(pl.multiple_of(step * wide, wide), wide)
        low, high = max(start - 8, 0), min(stop + 8, fields)
        x = jnp.transpose(ens_ref[:, low:high, where].astype(jnp.float32), (1, 0, 2))
        rate = mix_ref[:, where][None]
        above = jnp.concatenate([x[:1], x[:-1]], axis=0)
        below = jnp.concatenate([x[1:], x[-1:]], axis=0)
        keep = slice(start - low, stop - low)
        x, above, below = x[keep], above[keep], below[keep]
        stepped = x + rate * (above - 2.0 * x + below) - 0.05 * x * x * x
        if start == 0:
            top = stepped[:1] + surf_ref[:, where][None]
            stepped = jnp.concatenate([top, stepped[1:]], axis=0)
        land = jnp.broadcast_to(land_ref[:, where][None], x.shape) > 0
        fc_ref[me, step, start:stop] = jnp.where(land, stepped, x).astype(jnp.bfloat16)

    def enter():
        pl.semaphore_wait(barrier, n_mem - 1)
        pl.semaphore_signal(hello, inc=1, device_id={"mem": GATE}, device_id_type=MESH)

    def send_weights():
        for j in range(near):
            for user in range(CORES):
                if j != REACH:
                    remote(
                        stage_ref.at[j, :, user],
                        near_ref.at[core * near + j],
                        tile_send.at[0],
                        tile_recv.at[0],
                        {"mem": y * CORES + user, **tile_peer(j - REACH)},
                    ).start()
        remote(
            stage_ref.at[REACH, :, 1 - core],
            near_ref.at[core * near + REACH],
            tile_send.at[0],
            tile_recv.at[0],
            {"mem": sibling},
        ).start()

    @pl.when(both(wraps, me >= CORES))
    def _():
        enter()

    head = pieces[0][2]
    ens_copy(0).wait()
    head_bytes = 4 * columns * (members + 2)
    drain(acc_ref.at[pl.ds(0, head_bytes // 512)], in_sem.at[0])
    mix_part(0, 0, head)

    @pl.when(jnp.logical_not(wraps))
    def _():
        pl.semaphore_wait(barrier, n_mem - 1 + 2 * REACH * CORES)

    @pl.when(both(wraps, both(me < CORES, me != GATE)))
    def _():
        enter()

    @pl.when(jnp.logical_not(both(wraps, gate)))
    def _():
        own_fc(0)

    mix_part(0, head, fields)

    @pl.when(jnp.logical_not(both(wraps, gate)))
    def _():
        own_fc(1)

    def mix(step, carry):
        ens_copy(step).wait()
        mix_part(step, 0, fields)
        return carry

    lax.fori_loop(1, n_mem, mix, 0)

    drain(slot_ref.at[pl.ds(0, CORES * (near + 2))], in_sem.at[2])

    @pl.when(jnp.logical_not(wraps))
    def _():
        send_weights()

    @pl.when(both(wraps, gate))
    def _():
        pl.semaphore_wait(hello, n_mem - 1)
        own_fc(0)
        own_fc(1)

    drain(slot_ref.at[pl.ds(0, 2 * CORES)], in_sem.at[1])
    share = slots // CHUNKS
    width = min(share, 512)
    flat = jnp.concatenate(
        [fc_ref[me, b].reshape(fields * members, wide) for b in range(n_mem)], axis=1
    )
    for h in range(CHUNKS):
        for step in range(share // width):
            where = pl.ds(h * share + step * width, width)
            rows = lax.broadcasted_iota(jnp.int32, (columns, width), 0)
            hot = jnp.where(rows == pos_ref[:, where], 1.0, 0.0).astype(jnp.bfloat16)
            found = rounded_dot(flat, hot)
            wanted = jnp.broadcast_to(field_ref[:, where], (members, width))
            total = found[:members]
            for f in range(1, fields):
                total = jnp.where(wanted == f, found[f * members : (f + 1) * members], total)
            seen_ref[me, h, :, pl.ds(step * width, width)] = total.astype(jnp.bfloat16)
        if h % CORES == CORES - 1:
            for done in range(h + 1 - CORES, h + 1):
                own_seen(done)

    near_seen()
    n_pieces = len(pieces)
    for piece in range(2, n_pieces - 2):
        own_fc(piece)

    @pl.when(both(wraps, gate))
    def _():
        pl.semaphore_wait(barrier, 2 * REACH * n_mem)
        for step in range(1, n_mem):
            pl.semaphore_signal(
                ready, inc=1, device_id={"mem": lax.rem(me + step, n_mem)}, device_id_type=MESH
            )

    @pl.when(both(wraps, jnp.logical_not(gate)))
    def _():
        pl.semaphore_wait(ready, 1)

    @pl.when(wraps)
    def _():
        send_weights()

    rounds = CHUNKS // CORES
    lanes = 128
    base = [
        valid_ref[i, core].astype(jnp.float32) / error_ref[i, core].astype(jnp.float32)
        for i in range(rounds)
    ]
    for i in range(rounds):
        slot_ref[CORES * near, i] = value_ref[i, core].astype(jnp.float32)
        for spare in range(CORES * near + 1, slot_ref.shape[0]):
            slot_ref[spare, i] = jnp.zeros_like(base[i])
    near_ref[core * near + REACH] = stage_ref[REACH, :, core]

    relay_fc(0)
    relay_fc(1)

    drain(near_ref.at[pl.ds(0, CORES * near - 1)], tile_recv.at[0])
    for r in range(CORES * near):
        for i in range(rounds):
            slot_ref[r, i] = base[i] * near_ref[r, i]
    for i in range(rounds):
        for r in range(share // lanes):
            rinv_ref[i, :, r * lanes : (r + 1) * lanes] = slot_ref[:, i, r, :]

    for i in range(rounds):
        drain(seen_ref.at[pl.ds(0, n_mem - 1), 0], seen_recv.at[i])
        seen = jnp.concatenate(
            [seen_ref[m, i * CORES + core].astype(jnp.float32) for m in range(n_mem)], axis=0
        )
        average = jnp.mean(seen, axis=0, keepdims=True)
        deviation = seen - average
        rinv = rinv_ref[i]
        innovation = rinv[CORES * near : CORES * near + 1] - average
        right = jnp.concatenate(
            [deviation, jnp.broadcast_to(innovation, deviation.shape)], axis=0
        ).astype(jnp.bfloat16)
        rows = [
            (deviation * rinv[r : r + 1]).astype(jnp.bfloat16) for r in range(CORES * near)
        ]
        for user in range(CORES):
            where = slice(user * near * everyone, (user + 1) * near * everyone)
            sums = lax.dot_general(
                jnp.concatenate(rows[user * near : (user + 1) * near], axis=0),
                right,
                (((1,), (1,)), ((), ())),
                preferred_element_type=jnp.float32,
            )
            acc_ref[where] = sums + acc_ref[where] if i else sums

    fold = everyone // 2
    lane = lax.broadcasted_iota(jnp.int32, (fold, 2 * everyone), 1)
    for r in range(CORES * near):
        upper = acc_ref[r * everyone : r * everyone + fold]
        lower = acc_ref[r * everyone + fold : (r + 1) * everyone]
        packed = jnp.where(lane < everyone + fold, pltpu.roll(lower, fold, 1), upper)
        packed = jnp.where(lane < everyone, upper, packed)
        packed = jnp.where(lane < 2 * everyone - fold // 2, packed, lower)
        part_ref[r] = packed.astype(jnp.bfloat16)
        user, j = r // near, r % near
        if j != REACH:
            remote(
                part_ref.at[r],
                got_ref.at[core * near + j],
                tile_send.at[1],
                tile_recv.at[1],
                {"mem": y * CORES + user, **tile_peer(REACH - j)},
            ).start()
    remote(
        part_ref.at[(1 - core) * near + REACH],
        got_ref.at[core * near + REACH],
        tile_send.at[1],
        tile_recv.at[1],
        {"mem": sibling},
    ).start()
    got_ref[core * near + REACH] = part_ref[core * near + REACH]

    relay_fc(2)

    drain(got_ref.at[pl.ds(0, CORES * near - 1)], tile_recv.at[1])

    summed = got_ref[0].astype(jnp.float32)
    for r in range(1, CORES * near):
        summed = summed + got_ref[r].astype(jnp.float32)
    summed = summed / (everyone - 1.0)
    flipped = jnp.transpose(summed)
    spread = jnp.concatenate(
        [
            summed[:, :everyone],
            jnp.concatenate(
                [flipped[fold:everyone], summed[:, everyone : everyone + fold]], axis=1
            ),
        ],
        axis=0,
    )
    first, second = everyone + fold, 2 * everyone - fold // 2
    pulled = jnp.concatenate([flipped[first : first + 8], flipped[second : second + 8]], axis=1)
    rows = lax.broadcasted_iota(jnp.int32, (everyone, everyone), 0)
    identity = jnp.where(
        rows == lax.broadcasted_iota(jnp.int32, (everyone, everyone), 1), 1.0, 0.0
    )
    system = identity + spread
    square = jnp.sum(system * system, keepdims=True)
    scale = jnp.sqrt(square)
    parts = halves(system)
    second = fine_dot(parts, parts) / square
    current = system / scale
    parts, second_parts = halves(current), halves(second)
    third = fine_dot(second_parts, parts)
    fourth = fine_dot(second_parts, second_parts)
    root = 2.25 * identity - 2.4375 * current + 1.6875 * second - 0.5625 * third + 0.0625 * fourth
    root_parts = halves(root)
    inner_parts = halves(fine_dot(parts, root_parts))
    outer_parts = halves(fine_dot(root_parts, root_parts))
    root = 1.5 * root - 0.5 * fine_dot(inner_parts, outer_parts)
    root_parts = halves(root)
    ones = jnp.ones((everyone, everyone), jnp.bfloat16)
    sums = rounded_dot(root_parts[0], ones) + rounded_dot(root_parts[1], ones)
    drawn = halves(fine_dot(halves(pulled), root_parts))
    mean_weight = fine_dot(drawn, root_parts)[:1] / scale
    weight_sum = fine_dot(drawn, halves(sums))[:1] / scale
    turned = root / jnp.sqrt(scale) + mean_weight
    turned = turned + (1.0 - sums / jnp.sqrt(scale) - weight_sum) / everyone
    for m in range(n_mem):
        tsend_ref[m, :, :everyone] = turned[m * members : (m + 1) * members]
        tsend_ref[m, :, everyone:] = jnp.zeros((members, everyone), jnp.float32)

    for step in range(1, n_mem):
        target = lax.rem(me + step, n_mem)
        remote(
            tsend_ref.at[target],
            trecv_ref.at[me],
            t_send.at[0],
            t_recv.at[0],
            {"mem": target},
        ).start()
    own_fc(n_pieces - 2)
    finish_fc(n_pieces - 1)
    trecv_ref[me] = tsend_ref[me]

    group = 8

    def apply(block, start, stop):
        where = pl.ds(block * wide, wide)
        left = jnp.concatenate(halves(trecv_ref[block][:, :everyone]), axis=0)
        land = jnp.broadcast_to(land_ref[:, where], (members, wide)) > 0
        for first in range(start, stop, group):
            states = jnp.concatenate(
                [
                    jnp.concatenate([fc_ref[m, block, f] for m in range(n_mem)], axis=0)
                    for f in range(first, first + group)
                ],
                axis=1,
            )
            pair = rounded_dot(left, states)
            total = pair[:members] + pair[members:]
            for f in range(group):
                moved_ref[first + f, :, :] = jnp.where(
                    land,
                    total[:, f * wide : (f + 1) * wide],
                    fc_ref[me, block, first + f].astype(jnp.float32),
                )
        moved = jnp.transpose(moved_ref[start:stop], (1, 0, 2)).astype(jnp.bfloat16)
        out_ref[:, start:stop, where] = moved

    for piece in range(3, n_pieces - 2):
        relay_fc(piece)

    drain(trecv_ref.at[pl.ds(0, n_mem - 1)], t_recv.at[0])

    for unit, (block, start, stop) in enumerate(units):
        if unit == 1:
            relay_fc(n_pieces - 2)
        count = n_y if unit < len(units) - 1 else n_mem - 1
        drain(fc_ref.at[pl.ds(0, count), block, pl.ds(start, stop - start)], fc_unit.at[unit])
        apply(block, start, stop)

    drain(fc_ref.at[pl.ds(0, n_mem - 1)], fc_send.at[0])
    drain(seen_ref.at[pl.ds(0, n_y - 1)], seen_send.at[0])
    drain(seen_ref.at[0, pl.ds(0, CHUNKS // CORES)], seen_send.at[1])
    drain(near_ref.at[pl.ds(0, CORES * near - 1)], tile_send.at[0])
    drain(part_ref.at[pl.ds(0, CORES * near - 1)], tile_send.at[1])
    drain(tsend_ref.at[pl.ds(0, n_mem - 1)], t_send.at[0])


def on_device(
    n_mem,
    n_tile,
    ensemble_profiles_before,
    mixing_coefficient,
    surface_driver,
    terrain_indicator,
    measured_profile_position,
    measured_field_index,
    obs_valid,
    obs_value,
    obs_error,
    local_weight,
):
    members, fields, columns = ensemble_profiles_before.shape
    slots = measured_field_index.shape[0]
    everyone = members * n_mem
    near = 2 * REACH + 1
    n_y = n_mem // CORES
    wide = columns // n_mem
    half = fields // 2
    units = [(block, 0, fields) for block in range(n_mem - 1)]
    cuts = (0, fields - 16, fields - 8, fields)
    units += [(n_mem - 1, *ends) for ends in zip(cuts[:-1], cuts[1:])]
    pieces = [(0, 0, 16, 0), (0, 16, half + 8, 0), (0, half + 8, fields, 0)]
    pieces += [(*unit, index) for index, unit in enumerate(units) if index]
    row = lambda a: a.reshape(1, -1)
    table = (CHUNKS // CORES, CORES, slots // CHUNKS // 128, 128)
    far = pl.BlockSpec(memory_space=pltpu.HBM)
    dma = pltpu.SemaphoreType.DMA
    return pl.pallas_call(
        functools.partial(kernel, n_mem, n_tile, pieces, units),
        out_shape=pltpu.VMEM(ensemble_profiles_before.shape, jnp.bfloat16),
        in_specs=[far] * 10,
        out_specs=pl.BlockSpec(memory_space=pltpu.VMEM),
        scratch_shapes=[
            pltpu.VMEM((members, fields, columns), jnp.bfloat16),
            pltpu.VMEM((1, columns), jnp.float32),
            pltpu.VMEM((members, columns), jnp.float32),
            pltpu.VMEM((1, columns), jnp.int32),
            pltpu.VMEM((1, slots), jnp.int32),
            pltpu.VMEM((1, slots), jnp.int32),
            pltpu.VMEM(table, jnp.int32),
            pltpu.VMEM(table, jnp.bfloat16),
            pltpu.VMEM(table, jnp.bfloat16),
            pltpu.VMEM((n_mem, n_mem, fields, members, wide), jnp.bfloat16),
            pltpu.VMEM((n_mem, CHUNKS, members, slots // CHUNKS), jnp.bfloat16),
            pltpu.VMEM((near, *table), jnp.float32),
            pltpu.VMEM((CORES * near, table[0], *table[2:]), jnp.float32),
            pltpu.VMEM((16, table[0], *table[2:]), jnp.float32),
            pltpu.VMEM((table[0], 16, slots // CHUNKS), jnp.float32),
            pltpu.VMEM((CORES * near * everyone, 2 * everyone), jnp.float32),
            pltpu.VMEM((CORES * near, everyone // 2, 2 * everyone), jnp.bfloat16),
            pltpu.VMEM((CORES * near, everyone // 2, 2 * everyone), jnp.bfloat16),
            pltpu.VMEM((n_mem, members, 2 * everyone), jnp.float32),
            pltpu.VMEM((n_mem, members, 2 * everyone), jnp.float32),
            pltpu.VMEM((fields, members, wide), jnp.float32),
            dma((n_mem,)),
            dma((3,)),
            dma((2,)),
            dma((CHUNKS // CORES,)),
            dma((1,)),
            dma((len(pieces) - 1, n_y - 1)),
            dma((len(units),)),
            dma((2,)),
            dma((2,)),
            dma((1,)),
            dma((1,)),
            pltpu.SemaphoreType.REGULAR,
            pltpu.SemaphoreType.REGULAR,
        ],
        compiler_params=pltpu.CompilerParams(
            collective_id=0, has_side_effects=True, vmem_limit_bytes=66_000_000
        ),
    )(
        ensemble_profiles_before,
        row(mixing_coefficient),
        surface_driver,
        row(terrain_indicator),
        row(measured_profile_position),
        row(measured_field_index),
        obs_valid.reshape(table),
        obs_value.reshape(table),
        obs_error.reshape(table),
        local_weight.reshape(near, *table),
    )


def fits(n_mem, n_tile, ensemble, slots):
    members, fields, columns = ensemble[0] // n_mem, ensemble[1], ensemble[2] // n_tile
    return (
        n_mem % CORES == 0
        and n_mem > CORES
        and 2 * members * n_mem == 128
        and n_tile > 2 * REACH
        and members % 16 == 0
        and fields % 8 == 0
        and fields > 32
        and columns % (128 * n_mem) == 0
        and slots // n_tile % (1024 * CHUNKS) == 0
    )


def solution(mesh):
    in_specs = (
        P("mem", None, "tile"),
        P("tile"),
        P("mem", "tile"),
        P("tile"),
        P("tile"),
        P("tile"),
        P("tile"),
        P("tile"),
        P("tile"),
        P("mem", "tile", None),
    )
    out_specs = P("mem", None, "tile")

    def run(*args):
        sizes = mesh.shape["mem"], mesh.shape["tile"]
        body = plain_on_device
        if fits(*sizes, args[0].shape, args[5].shape[0]):
            body = functools.partial(on_device, *sizes)
        return jax.shard_map(
            body, mesh=mesh, in_specs=in_specs, out_specs=out_specs, check_vma=False
        )(*args)

    return run
```

```python
import functools
import math

import jax
import jax.numpy as jnp
from jax import lax
from jax.experimental import pallas as pl
from jax.experimental.pallas import tpu as pltpu
from jax.sharding import PartitionSpec as P

REACH = 2
NS_ITERS = 3


EXACT = lax.Precision.HIGHEST


def from_behind(value, axis, steps):
    count = lax.axis_size(axis)
    pairs = [(source, (source + steps) % count) for source in range(count)]
    return lax.ppermute(value, axis, pairs)


def vertical_mixing_step(
    ensemble_profiles_before, mixing_coefficient, surface_driver, terrain_indicator
):
    values = ensemble_profiles_before.astype(jnp.float32)
    above_layer = jnp.concatenate([values[:, :1], values[:, :-1]], axis=1)
    below_layer = jnp.concatenate([values[:, 1:], values[:, -1:]], axis=1)
    diffused = values + mixing_coefficient[None, None, :] * (
        above_layer - 2.0 * values + below_layer
    )
    stepped = diffused - 0.05 * values * values * values
    surface = jnp.concatenate([stepped[:, :1] + surface_driver[:, None, :], stepped[:, 1:]], axis=1)
    result = jnp.where(terrain_indicator[None, None, :] > 0, surface, values)
    return result.astype(jnp.bfloat16)


def measurement_operator(background_ensemble, measured_profile_position, measured_field_index):
    profile_sequence = background_ensemble.shape[2]
    unrolled_ensemble = background_ensemble.reshape(background_ensemble.shape[0], -1)
    slot_index = measured_field_index * profile_sequence + measured_profile_position
    return jnp.take(unrolled_ensemble, slot_index, axis=1)


def prepare(window):
    ensemble_profiles = window.shape[0] - 3
    measured_quantities = window[:ensemble_profiles].astype(jnp.float32)
    average = jnp.mean(measured_quantities, axis=0)
    deviation = measured_quantities - average
    innovation = window[ensemble_profiles].astype(jnp.float32) - average
    obs_precision = window[ensemble_profiles + 2].astype(jnp.float32) / window[
        ensemble_profiles + 1
    ].astype(jnp.float32)
    return (deviation, innovation, obs_precision)


def weights_for(deviation, innovation, precision, portions):
    ensemble_profiles = deviation.shape[0]
    portion_width = deviation.shape[1] // portions
    spread = jnp.zeros((ensemble_profiles, ensemble_profiles), jnp.float32)
    for portion_index in range(portions):
        portion = deviation[:, portion_index * portion_width : (portion_index + 1) * portion_width]
        scaled = (
            portion
            * precision[None, portion_index * portion_width : (portion_index + 1) * portion_width]
        )
        spread = spread + jnp.dot(
            scaled, portion.T, precision=EXACT, preferred_element_type=jnp.float32
        )
    spread = spread / (ensemble_profiles - 1.0)
    pulled = jnp.dot(
        deviation, precision * innovation, precision=EXACT, preferred_element_type=jnp.float32
    ) / (ensemble_profiles - 1.0)
    identity = jnp.eye(ensemble_profiles, dtype=jnp.float32)
    system = identity + spread
    norm_scale = jnp.sqrt(jnp.sum(system * system))

    def newton(sweep, carry):
        current, inv_root = carry
        middle = 1.5 * identity - 0.5 * jnp.dot(inv_root, current, precision=EXACT)
        return (
            jnp.dot(current, middle, precision=EXACT),
            jnp.dot(middle, inv_root, precision=EXACT),
        )

    current, inv_root = lax.fori_loop(0, NS_ITERS, newton, (system / norm_scale, identity))
    inv_root = inv_root / jnp.sqrt(norm_scale)
    inverse = jnp.dot(inv_root, inv_root, precision=EXACT)
    mean_weight = jnp.dot(inverse, pulled, precision=EXACT)
    return inv_root + mean_weight[:, None]


def update(states, transform, land_block):
    values = states.astype(jnp.float32)
    average = jnp.mean(values, axis=0)
    deviation = values - average[None]
    moved = jnp.einsum("isc,ij->jsc", deviation, transform, precision=EXACT)
    result = jnp.where(land_block[None, None, :] > 0, average[None] + moved, values)
    return result.astype(jnp.bfloat16)


def plain_on_device(
    ensemble_profiles_before,
    mixing_coefficient,
    surface_driver,
    terrain_indicator,
    measured_profile_position,
    measured_field_index,
    obs_valid,
    obs_value,
    obs_error,
    local_weight,
):
    background_ensemble = vertical_mixing_step(
        ensemble_profiles_before, mixing_coefficient, surface_driver, terrain_indicator
    )
    measured_quantities = measurement_operator(
        background_ensemble, measured_profile_position, measured_field_index
    )
    metadata = jnp.stack([obs_value, obs_error, obs_valid.astype(jnp.bfloat16)])
    own_rows = jnp.concatenate([measured_quantities, metadata], axis=0)
    pieces = []
    for offset in range(-REACH, REACH + 1):
        if offset == 0:
            pieces.append(own_rows)
        else:
            pieces.append(from_behind(own_rows, "tile", -offset))
    nearby = jnp.concatenate(pieces, axis=1)
    members_here = measured_quantities.shape[0]
    everyone = lax.all_gather(nearby[:members_here], "mem", axis=0, tiled=True)
    window = jnp.concatenate([everyone, nearby[members_here:]], axis=0)
    regrouped_states = lax.all_to_all(
        background_ensemble, "mem", split_axis=2, concat_axis=0, tiled=True
    )
    deviation, innovation, obs_precision = prepare(window)
    columns_here = regrouped_states.shape[2]
    local_land = lax.dynamic_slice_in_dim(
        terrain_indicator, lax.axis_index("mem") * columns_here, columns_here
    )
    transform = weights_for(
        deviation, innovation, obs_precision * local_weight[0, 0], 2 * REACH + 1
    )
    outputs = update(regrouped_states, transform, local_land)
    return lax.all_to_all(outputs, "mem", split_axis=0, concat_axis=2, tiled=True)


MESH = pl.DeviceIdType.MESH
CHUNKS = 4
CORES = 2
GATE = 0


def rounded_dot(a, b):
    return jnp.dot(a, b, preferred_element_type=jnp.float32)


def halves(a):
    high = a.astype(jnp.bfloat16)
    return high, (a - high.astype(jnp.float32)).astype(jnp.bfloat16)


def fine_dot(a, b):
    (a_high, a_low), (b_high, b_low) = a, b
    return rounded_dot(a_high, b_high) + (rounded_dot(a_high, b_low) + rounded_dot(a_low, b_high))


def drain(ref, sem):
    pltpu.make_async_copy(ref, ref, sem).wait()


def counter(bytes_ref):
    def count(size, sem):
        drain(bytes_ref.at[pl.ds(0, size // 512)], sem)

    return count


def kernel(
    n_mem,
    n_tile,
    pieces,
    units,
    ens_hbm,
    mix_hbm,
    surf_hbm,
    land_hbm,
    pos_hbm,
    field_hbm,
    valid_hbm,
    value_hbm,
    error_hbm,
    weight_hbm,
    out_ref,
    ens_ref,
    mix_ref,
    surf_ref,
    land_ref,
    pos_ref,
    field_ref,
    valid_ref,
    value_ref,
    error_ref,
    fc_ref,
    seen_ref,
    stage_ref,
    near_ref,
    slot_ref,
    rinv_ref,
    acc_ref,
    part_ref,
    got_ref,
    tsend_ref,
    trecv_ref,
    moved_ref,
    bytes_ref,
    ens_sem,
    in_sem,
    out_sem,
    seen_recv,
    fc_across,
    fc_unit,
    tile_recv,
    t_recv,
    hello,
    ready,
):
    members, fields, columns = ens_ref.shape
    everyone = members * n_mem
    slots = pos_ref.shape[1]
    near = 2 * REACH + 1
    wide = columns // n_mem
    count = counter(bytes_ref)
    me, tile = lax.axis_index("mem"), lax.axis_index("tile")
    n_y = n_mem // CORES
    y, core = me // CORES, lax.rem(me, CORES)
    sibling = y * CORES + (1 - core)
    across = [lax.rem(y + step, n_y) * CORES + core for step in range(1, n_y)]
    gate = me == GATE
    wraps = tile < REACH

    def both(first, second):
        return jnp.logical_and(first, second)

    barrier = pltpu.get_barrier_semaphore()
    for step in range(1, n_mem):
        peer = lax.rem(me + step, n_mem)

        @pl.when(peer != GATE)
        def _(peer=peer):
            pl.semaphore_signal(barrier, inc=1, device_id={"mem": peer}, device_id_type=MESH)

    for offset in range(-REACH, REACH + 1):
        if offset:
            there = lax.rem(tile + offset + n_tile, n_tile)
            pl.semaphore_signal(
                barrier, inc=1, device_id={"mem": GATE, "tile": there}, device_id_type=MESH
            )

    def ens_copy(step):
        where = pl.ds(pl.multiple_of(step * wide, wide), wide)
        return pltpu.make_async_copy(
            ens_hbm.at[:, :, where], ens_ref.at[:, :, where], ens_sem.at[min(step, 1)]
        )

    groups = [
        [(mix_hbm, mix_ref), (surf_hbm, surf_ref), (land_hbm, land_ref)],
        [(pos_hbm, pos_ref), (field_hbm, field_ref)],
        [
            (valid_hbm, valid_ref),
            (value_hbm, value_ref),
            (error_hbm, error_ref),
            (weight_hbm, stage_ref),
        ],
    ]
    loads = [
        [pltpu.make_async_copy(src, dst, in_sem.at[min(g, 1)]) for src, dst in group]
        for g, group in enumerate(groups)
    ]
    ens_copy(0).start()
    for copy in loads[0]:
        copy.start()
    for step in range(1, n_mem):
        ens_copy(step).start()
    for group in loads[1:]:
        for copy in group:
            copy.start()

    def remote(src, dst, send, recv, where):
        return pltpu.make_async_remote_copy(
            src_ref=src,
            dst_ref=dst,
            send_sem=send,
            recv_sem=recv,
            device_id=where,
            device_id_type=MESH,
        )

    def fc_copy(piece, owner, recv, target):
        block, first, stop = pieces[piece][:3]
        ref = fc_ref.at[owner, block, pl.ds(first, stop - first)]
        return remote(ref, ref, out_sem.at[0], recv, {"mem": target})

    def fc_over(piece, owner, index, target):
        return fc_copy(piece, owner, fc_across.at[max(piece - 2, piece // 2), index], target)

    def fc_near(piece, owner):
        return fc_copy(piece, owner, fc_unit.at[max(pieces[piece][3] + 3 - len(units), 0)], sibling)

    def finish_fc(piece):
        for step in range(1, n_mem):
            fc_copy(piece, me, fc_unit.at[2], lax.rem(me + step, n_mem)).start()

    def own_fc(piece):
        for index, peer in enumerate(across):
            fc_over(piece, me, n_y - 2 - index, peer).start()
        fc_near(piece, me).start()

    def relay_fc(piece):
        for index, peer in enumerate(across):
            fc_over(piece, peer, index, peer).wait_recv()
            fc_near(piece, peer).start()

    def seen_copy(h, target):
        ref = seen_ref.at[me, h]
        return remote(ref, ref, out_sem.at[0], seen_recv.at[h // CORES], {"mem": target})

    def own_seen(h):
        user = h % CORES
        for step in range(1, n_y):
            seen_copy(h, lax.rem(y + step, n_y) * CORES + user).start()

    def near_seen():
        for i in range(CHUNKS // CORES):
            h = i * CORES + 1 - core
            ref = seen_ref.at[me, h]
            remote(ref, ref, out_sem.at[0], seen_recv.at[i], {"mem": sibling}).start()

    def tile_peer(offset):
        return {"tile": lax.rem(tile + offset + n_tile, n_tile)}

    def mix_part(step, start, stop):
        where = pl.ds(pl.multiple_of(step * wide, wide), wide)
        low, high = max(start - 8, 0), min(stop + 8, fields)
        x = jnp.transpose(ens_ref[:, low:high, where].astype(jnp.float32), (1, 0, 2))
        rate = mix_ref[:, where][None]
        above = jnp.concatenate([x[:1], x[:-1]], axis=0)
        below = jnp.concatenate([x[1:], x[-1:]], axis=0)
        keep = slice(start - low, stop - low)
        x, above, below = x[keep], above[keep], below[keep]
        stepped = x + rate * (above - 2.0 * x + below) - 0.05 * x * x * x
        if start == 0:
            top = stepped[:1] + surf_ref[:, where][None]
            stepped = jnp.concatenate([top, stepped[1:]], axis=0)
        land = jnp.broadcast_to(land_ref[:, where][None], x.shape) > 0
        fc_ref[me, step, start:stop] = jnp.where(land, stepped, x).astype(jnp.bfloat16)

    def enter():
        pl.semaphore_wait(barrier, n_mem - 1)
        pl.semaphore_signal(hello, inc=1, device_id={"mem": GATE}, device_id_type=MESH)

    def send_weights():
        for j in range(near):
            for user in range(CORES):
                if j != REACH:
                    remote(
                        stage_ref.at[j, :, user],
                        near_ref.at[core * near + j],
                        out_sem.at[0],
                        tile_recv.at[0],
                        {"mem": y * CORES + user, **tile_peer(j - REACH)},
                    ).start()
        remote(
            stage_ref.at[REACH, :, 1 - core],
            near_ref.at[core * near + REACH],
            out_sem.at[0],
            tile_recv.at[0],
            {"mem": sibling},
        ).start()

    def admit():
        pl.semaphore_wait(barrier, 2 * REACH * n_mem)
        for step in range(1, n_mem):
            peer = lax.rem(me + step, n_mem)
            pl.semaphore_signal(ready, inc=1, device_id={"mem": peer}, device_id_type=MESH)

    def meet_tiles():
        @pl.when(both(wraps, gate))
        def _():
            admit()

        @pl.when(jnp.logical_not(gate))
        def _():
            pl.semaphore_wait(ready, 1)

        send_weights()

    @pl.when(me >= CORES)
    def _():
        enter()

    head = pieces[0][2]
    ens_copy(0).wait()
    count(4 * columns * (members + 2), in_sem.at[0])
    mix_part(0, 0, head)

    @pl.when(both(me < CORES, me != GATE))
    def _():
        enter()

    @pl.when(me != GATE)
    def _():
        own_fc(0)

    mix_part(0, head, fields)

    @pl.when(me != GATE)
    def _():
        own_fc(1)

    count(2 * members * fields * wide * (n_mem - 1), ens_sem.at[1])

    def mix(step, carry):
        mix_part(step, 0, fields)
        return carry

    lax.fori_loop(1, n_mem, mix, 0)

    count(4 * slots * (near + 4), in_sem.at[1])

    @pl.when(gate)
    def _():
        pl.semaphore_wait(hello, n_mem - 1)
        own_fc(0)
        own_fc(1)

    @pl.when(both(gate, jnp.logical_not(wraps)))
    def _():
        admit()

    share = slots // CHUNKS
    width = min(share, 512)
    flat = jnp.concatenate(
        [fc_ref[me, b].reshape(fields * members, wide) for b in range(n_mem)], axis=1
    )
    for h in range(CHUNKS):
        for step in range(share // width):
            where = pl.ds(h * share + step * width, width)
            rows = lax.broadcasted_iota(jnp.int32, (columns, width), 0)
            hot = jnp.where(rows == pos_ref[:, where], 1.0, 0.0).astype(jnp.bfloat16)
            found = rounded_dot(flat, hot)
            wanted = jnp.broadcast_to(field_ref[:, where], (members, width))
            total = found[:members]
            for f in range(1, fields):
                total = jnp.where(wanted == f, found[f * members : (f + 1) * members], total)
            seen_ref[me, h, :, pl.ds(step * width, width)] = total.astype(jnp.bfloat16)
        if h % CORES == CORES - 1:
            for done in range(h + 1 - CORES, h + 1):
                own_seen(done)
            if h < CORES:
                own_fc(2)
        if h == 0:

            @pl.when(jnp.logical_not(wraps))
            def _():
                meet_tiles()

    near_seen()
    n_pieces = len(pieces)
    for piece in range(3, n_pieces - 1):
        own_fc(piece)

    @pl.when(wraps)
    def _():
        meet_tiles()

    rounds = CHUNKS // CORES
    lanes = 128
    base = [
        valid_ref[i, core].astype(jnp.float32) / error_ref[i, core].astype(jnp.float32)
        for i in range(rounds)
    ]
    for i in range(rounds):
        slot_ref[CORES * near, i] = value_ref[i, core].astype(jnp.float32)
        for spare in range(CORES * near + 1, slot_ref.shape[0]):
            slot_ref[spare, i] = jnp.zeros_like(base[i])
    near_ref[core * near + REACH] = stage_ref[REACH, :, core]

    for index, peer in enumerate(across):
        drain(fc_ref.at[peer, 0, pl.ds(0, pieces[1][2])], fc_across.at[0, index])
        fc_near(0, peer).start()
        fc_near(1, peer).start()

    drain(near_ref.at[pl.ds(0, CORES * near - 1)], tile_recv.at[0])
    for r in range(CORES * near):
        for i in range(rounds):
            slot_ref[r, i] = base[i] * near_ref[r, i]
    for i in range(rounds):
        for r in range(share // lanes):
            rinv_ref[i, :, r * lanes : (r + 1) * lanes] = slot_ref[:, i, r, :]

    for i in range(rounds):
        drain(seen_ref.at[pl.ds(0, n_mem - 1), 0], seen_recv.at[i])
        seen = jnp.concatenate(
            [seen_ref[m, i * CORES + core].astype(jnp.float32) for m in range(n_mem)], axis=0
        )
        average = jnp.mean(seen, axis=0, keepdims=True)
        deviation = seen - average
        rinv = rinv_ref[i]
        innovation = rinv[CORES * near : CORES * near + 1] - average
        right = jnp.concatenate(
            [deviation, jnp.broadcast_to(innovation, deviation.shape)], axis=0
        ).astype(jnp.bfloat16)
        rows = [
            (deviation * rinv[r : r + 1]).astype(jnp.bfloat16) for r in range(CORES * near)
        ]
        for user in range(CORES):
            where = slice(user * near * everyone, (user + 1) * near * everyone)
            sums = lax.dot_general(
                jnp.concatenate(rows[user * near : (user + 1) * near], axis=0),
                right,
                (((1,), (1,)), ((), ())),
                preferred_element_type=jnp.float32,
            )
            acc_ref[where] = sums + acc_ref[where] if i else sums

    fold = everyone // 2
    lane = lax.broadcasted_iota(jnp.int32, (fold, 2 * everyone), 1)
    for r in range(CORES * near):
        upper = acc_ref[r * everyone : r * everyone + fold]
        lower = acc_ref[r * everyone + fold : (r + 1) * everyone]
        packed = jnp.where(lane < everyone + fold, pltpu.roll(lower, fold, 1), upper)
        packed = jnp.where(lane < everyone, upper, packed)
        packed = jnp.where(lane < 2 * everyone - fold // 2, packed, lower)
        part_ref[r] = packed.astype(jnp.bfloat16)
        user, j = r // near, r % near
        if j != REACH:
            remote(
                part_ref.at[r],
                got_ref.at[core * near + j],
                out_sem.at[0],
                tile_recv.at[1],
                {"mem": y * CORES + user, **tile_peer(REACH - j)},
            ).start()
    remote(
        part_ref.at[(1 - core) * near + REACH],
        got_ref.at[core * near + REACH],
        out_sem.at[0],
        tile_recv.at[1],
        {"mem": sibling},
    ).start()
    got_ref[core * near + REACH] = part_ref[core * near + REACH]

    for index, peer in enumerate(across):
        first, stop = pieces[2][1], pieces[3][2]
        drain(fc_ref.at[peer, 0, pl.ds(first, stop - first)], fc_across.at[1, index])
        fc_near(2, peer).start()
        fc_near(3, peer).start()

    drain(got_ref.at[pl.ds(0, CORES * near - 1)], tile_recv.at[1])

    summed = got_ref[0].astype(jnp.float32)
    for r in range(1, CORES * near):
        summed = summed + got_ref[r].astype(jnp.float32)
    summed = summed / (everyone - 1.0)
    flipped = jnp.transpose(summed)
    spread = jnp.concatenate(
        [
            summed[:, :everyone],
            jnp.concatenate(
                [flipped[fold:everyone], summed[:, everyone : everyone + fold]], axis=1
            ),
        ],
        axis=0,
    )
    first, second = everyone + fold, 2 * everyone - fold // 2
    pulled = jnp.concatenate([flipped[first : first + 8], flipped[second : second + 8]], axis=1)
    rows = lax.broadcasted_iota(jnp.int32, (everyone, everyone), 0)
    identity = jnp.where(
        rows == lax.broadcasted_iota(jnp.int32, (everyone, everyone), 1), 1.0, 0.0
    )
    system = identity + spread
    square = jnp.sum(system * system, keepdims=True)
    scale = jnp.sqrt(square)
    rows = jnp.concatenate([pulled, jnp.ones_like(pulled)], axis=0)
    powers = [rows]
    parts = halves(system)
    second = fine_dot(parts, parts) / square
    powers.append(fine_dot(halves(rows), parts) / scale)
    current = system / scale
    parts, second_parts = halves(current), halves(second)
    third = fine_dot(second_parts, parts)
    fourth = fine_dot(second_parts, second_parts)
    for power in range(2, 6):
        powers.append(fine_dot(halves(powers[power - 2]), second_parts))
    weights = (2.25, -2.4375, 1.6875, -0.5625, 0.0625)

    def combine(terms):
        return sum(weight * term for weight, term in zip(weights, terms))

    root = combine([identity, current, second, third, fourth])
    root_parts = halves(root)
    inner_parts = halves(fine_dot(parts, root_parts))
    outer_parts = halves(fine_dot(root_parts, root_parts))
    root = 1.5 * root - 0.5 * fine_dot(inner_parts, outer_parts)
    drawn = 1.5 * combine(powers[:5]) - 0.5 * fine_dot(halves(combine(powers[1:])), outer_parts)
    root_parts = halves(root)
    ones = jnp.ones((everyone, everyone), jnp.bfloat16)
    sums = rounded_dot(root_parts[0], ones) + rounded_dot(root_parts[1], ones)
    mean_weight = fine_dot(halves(drawn[:8]), root_parts)[:1] / scale
    weight_sum = jnp.sum(drawn[:1] * drawn[8:9], axis=1, keepdims=True) / scale
    turned = root / jnp.sqrt(scale) + mean_weight
    turned = turned + (1.0 - sums / jnp.sqrt(scale) - weight_sum) / everyone
    for m in range(n_mem):
        tsend_ref[m, :, :everyone] = turned[m * members : (m + 1) * members]
        tsend_ref[m, :, everyone:] = jnp.zeros((members, everyone), jnp.float32)

    for step in range(1, n_mem):
        target = lax.rem(me + step, n_mem)
        remote(
            tsend_ref.at[target],
            trecv_ref.at[me],
            out_sem.at[0],
            t_recv.at[0],
            {"mem": target},
        ).start()
    finish_fc(n_pieces - 1)
    trecv_ref[me] = tsend_ref[me]

    group = 8

    def apply(block, start, stop):
        where = pl.ds(block * wide, wide)
        left = jnp.concatenate(halves(trecv_ref[block][:, :everyone]), axis=0)
        land = jnp.broadcast_to(land_ref[:, where], (members, wide)) > 0
        for first in range(start, stop, group):
            end = min(first + group, stop)
            states = jnp.concatenate(
                [
                    jnp.concatenate([fc_ref[m, block, f] for m in range(n_mem)], axis=0)
                    for f in range(first, end)
                ],
                axis=1,
            )
            pair = rounded_dot(left, states)
            total = pair[:members] + pair[members:]
            for f in range(end - first):
                moved_ref[block, first + f] = jnp.where(
                    land,
                    total[:, f * wide : (f + 1) * wide],
                    fc_ref[me, block, first + f].astype(jnp.float32),
                )
        moved = jnp.transpose(moved_ref[block, start:stop], (1, 0, 2)).astype(jnp.bfloat16)
        out_ref[:, start:stop, where] = moved

    for piece in range(4, n_pieces - 1):
        relay_fc(piece)

    drain(trecv_ref.at[pl.ds(0, n_mem - 1)], t_recv.at[0])

    n_units = len(units)
    for chosen in (range(n_units - 2), range(n_units - 2, n_units - 1), range(n_units - 1, n_units)):
        rows = sum(units[unit][2] - units[unit][1] for unit in chosen)
        owners = n_y if chosen[-1] < n_units - 1 else n_mem - 1
        count(2 * owners * rows * members * wide, fc_unit.at[chosen[-1] + 3 - n_units])
        for unit in chosen:
            apply(*units[unit])

    kinds = [fc_ref.at[0], seen_ref.at[0], part_ref, stage_ref.at[:, :, 0], tsend_ref.at[0]]
    sizes = [ref.dtype.itemsize * math.prod(ref.shape) for ref in kinds]
    counts = [n_mem - 1, n_y - 1, 0, 0, n_mem - 1]
    total = sum(size * count for size, count in zip(sizes, counts))
    total += sizes[1] // CORES
    total += (sizes[2] + sizes[3] * CORES) * (CORES * near - 1) // (CORES * near)
    count(total, out_sem.at[0])


def on_device(
    n_mem,
    n_tile,
    ensemble_profiles_before,
    mixing_coefficient,
    surface_driver,
    terrain_indicator,
    measured_profile_position,
    measured_field_index,
    obs_valid,
    obs_value,
    obs_error,
    local_weight,
):
    members, fields, columns = ensemble_profiles_before.shape
    slots = measured_field_index.shape[0]
    everyone = members * n_mem
    near = 2 * REACH + 1
    n_y = n_mem // CORES
    wide = columns // n_mem
    units = [(block, 0, fields) for block in range(n_mem - 1)]
    cuts = (0, fields - 16, fields - 4, fields)
    units += [(n_mem - 1, *ends) for ends in zip(cuts[:-1], cuts[1:])]
    pieces = [(0, 0, 16, 0), (0, 16, 28, 0), (0, 28, 32, 0), (0, 32, fields, 0)]
    pieces += [(*unit, index) for index, unit in enumerate(units) if index]
    spare = 8 * everyone * fields * columns
    row = lambda a: a.reshape(1, -1)
    table = (CHUNKS // CORES, CORES, slots // CHUNKS // 128, 128)
    far = pl.BlockSpec(memory_space=pltpu.HBM)
    dma = pltpu.SemaphoreType.DMA
    return pl.pallas_call(
        functools.partial(kernel, n_mem, n_tile, pieces, units),
        out_shape=pltpu.VMEM(ensemble_profiles_before.shape, jnp.bfloat16),
        in_specs=[far] * 10,
        out_specs=pl.BlockSpec(memory_space=pltpu.VMEM),
        scratch_shapes=[
            pltpu.VMEM((members, fields, columns), jnp.bfloat16),
            pltpu.VMEM((1, columns), jnp.float32),
            pltpu.VMEM((members, columns), jnp.float32),
            pltpu.VMEM((1, columns), jnp.int32),
            pltpu.VMEM((1, slots), jnp.int32),
            pltpu.VMEM((1, slots), jnp.int32),
            pltpu.VMEM(table, jnp.int32),
            pltpu.VMEM(table, jnp.bfloat16),
            pltpu.VMEM(table, jnp.bfloat16),
            pltpu.VMEM((n_mem, n_mem, fields, members, wide), jnp.bfloat16),
            pltpu.VMEM((n_mem, CHUNKS, members, slots // CHUNKS), jnp.bfloat16),
            pltpu.VMEM((near, *table), jnp.float32),
            pltpu.VMEM((CORES * near, table[0], *table[2:]), jnp.float32),
            pltpu.VMEM((16, table[0], *table[2:]), jnp.float32),
            pltpu.VMEM((table[0], 16, slots // CHUNKS), jnp.float32),
            pltpu.VMEM((CORES * near * everyone, 2 * everyone), jnp.float32),
            pltpu.VMEM((CORES * near, everyone // 2, 2 * everyone), jnp.bfloat16),
            pltpu.VMEM((CORES * near, everyone // 2, 2 * everyone), jnp.bfloat16),
            pltpu.VMEM((n_mem, members, 2 * everyone), jnp.float32),
            pltpu.VMEM((n_mem, members, 2 * everyone), jnp.float32),
            pltpu.VMEM((n_mem, fields, members, wide), jnp.float32),
            pltpu.VMEM((spare // 512, 128), jnp.float32),
            dma((2,)),
            dma((2,)),
            dma((1,)),
            dma((CHUNKS // CORES,)),
            dma((len(pieces) - 3, n_y - 1)),
            dma((3,)),
            dma((2,)),
            dma((1,)),
            pltpu.SemaphoreType.REGULAR,
            pltpu.SemaphoreType.REGULAR,
        ],
        compiler_params=pltpu.CompilerParams(
            collective_id=0, has_side_effects=True, vmem_limit_bytes=66_000_000
        ),
    )(
        ensemble_profiles_before,
        row(mixing_coefficient),
        surface_driver,
        row(terrain_indicator),
        row(measured_profile_position),
        row(measured_field_index),
        obs_valid.reshape(table),
        obs_value.reshape(table),
        obs_error.reshape(table),
        local_weight.reshape(near, *table),
    )


def fits(n_mem, n_tile, ensemble, slots):
    members, fields, columns = ensemble[0] // n_mem, ensemble[1], ensemble[2] // n_tile
    return (
        n_mem % CORES == 0
        and n_mem > CORES
        and 2 * members * n_mem == 128
        and n_tile > 2 * REACH
        and members % 16 == 0
        and fields % 8 == 0
        and fields > 32
        and columns % (128 * n_mem) == 0
        and slots // n_tile % (1024 * CHUNKS) == 0
    )


def solution(mesh):
    in_specs = (
        P("mem", None, "tile"),
        P("tile"),
        P("mem", "tile"),
        P("tile"),
        P("tile"),
        P("tile"),
        P("tile"),
        P("tile"),
        P("tile"),
        P("mem", "tile", None),
    )
    out_specs = P("mem", None, "tile")

    def run(*args):
        sizes = mesh.shape["mem"], mesh.shape["tile"]
        body = plain_on_device
        if fits(*sizes, args[0].shape, args[5].shape[0]):
            body = functools.partial(on_device, *sizes)
        return jax.shard_map(
            body, mesh=mesh, in_specs=in_specs, out_specs=out_specs, check_vma=False
        )(*args)

    return run
```

```python
import functools
import math

import jax
import jax.numpy as jnp
from jax import lax
from jax.experimental import pallas as pl
from jax.experimental.pallas import tpu as pltpu
from jax.sharding import PartitionSpec as P

REACH = 2
NS_ITERS = 3


EXACT = lax.Precision.HIGHEST


def from_behind(value, axis, steps):
    count = lax.axis_size(axis)
    pairs = [(source, (source + steps) % count) for source in range(count)]
    return lax.ppermute(value, axis, pairs)


def vertical_mixing_step(
    ensemble_profiles_before, mixing_coefficient, surface_driver, terrain_indicator
):
    values = ensemble_profiles_before.astype(jnp.float32)
    above_layer = jnp.concatenate([values[:, :1], values[:, :-1]], axis=1)
    below_layer = jnp.concatenate([values[:, 1:], values[:, -1:]], axis=1)
    diffused = values + mixing_coefficient[None, None, :] * (
        above_layer - 2.0 * values + below_layer
    )
    stepped = diffused - 0.05 * values * values * values
    surface = jnp.concatenate([stepped[:, :1] + surface_driver[:, None, :], stepped[:, 1:]], axis=1)
    result = jnp.where(terrain_indicator[None, None, :] > 0, surface, values)
    return result.astype(jnp.bfloat16)


def measurement_operator(background_ensemble, measured_profile_position, measured_field_index):
    profile_sequence = background_ensemble.shape[2]
    unrolled_ensemble = background_ensemble.reshape(background_ensemble.shape[0], -1)
    slot_index = measured_field_index * profile_sequence + measured_profile_position
    return jnp.take(unrolled_ensemble, slot_index, axis=1)


def prepare(window):
    ensemble_profiles = window.shape[0] - 3
    measured_quantities = window[:ensemble_profiles].astype(jnp.float32)
    average = jnp.mean(measured_quantities, axis=0)
    deviation = measured_quantities - average
    innovation = window[ensemble_profiles].astype(jnp.float32) - average
    obs_precision = window[ensemble_profiles + 2].astype(jnp.float32) / window[
        ensemble_profiles + 1
    ].astype(jnp.float32)
    return (deviation, innovation, obs_precision)


def weights_for(deviation, innovation, precision, portions):
    ensemble_profiles = deviation.shape[0]
    portion_width = deviation.shape[1] // portions
    spread = jnp.zeros((ensemble_profiles, ensemble_profiles), jnp.float32)
    for portion_index in range(portions):
        portion = deviation[:, portion_index * portion_width : (portion_index + 1) * portion_width]
        scaled = (
            portion
            * precision[None, portion_index * portion_width : (portion_index + 1) * portion_width]
        )
        spread = spread + jnp.dot(
            scaled, portion.T, precision=EXACT, preferred_element_type=jnp.float32
        )
    spread = spread / (ensemble_profiles - 1.0)
    pulled = jnp.dot(
        deviation, precision * innovation, precision=EXACT, preferred_element_type=jnp.float32
    ) / (ensemble_profiles - 1.0)
    identity = jnp.eye(ensemble_profiles, dtype=jnp.float32)
    system = identity + spread
    norm_scale = jnp.sqrt(jnp.sum(system * system))

    def newton(sweep, carry):
        current, inv_root = carry
        middle = 1.5 * identity - 0.5 * jnp.dot(inv_root, current, precision=EXACT)
        return (
            jnp.dot(current, middle, precision=EXACT),
            jnp.dot(middle, inv_root, precision=EXACT),
        )

    current, inv_root = lax.fori_loop(0, NS_ITERS, newton, (system / norm_scale, identity))
    inv_root = inv_root / jnp.sqrt(norm_scale)
    inverse = jnp.dot(inv_root, inv_root, precision=EXACT)
    mean_weight = jnp.dot(inverse, pulled, precision=EXACT)
    return inv_root + mean_weight[:, None]


def update(states, transform, land_block):
    values = states.astype(jnp.float32)
    average = jnp.mean(values, axis=0)
    deviation = values - average[None]
    moved = jnp.einsum("isc,ij->jsc", deviation, transform, precision=EXACT)
    result = jnp.where(land_block[None, None, :] > 0, average[None] + moved, values)
    return result.astype(jnp.bfloat16)


def plain_on_device(
    ensemble_profiles_before,
    mixing_coefficient,
    surface_driver,
    terrain_indicator,
    measured_profile_position,
    measured_field_index,
    obs_valid,
    obs_value,
    obs_error,
    local_weight,
):
    background_ensemble = vertical_mixing_step(
        ensemble_profiles_before, mixing_coefficient, surface_driver, terrain_indicator
    )
    measured_quantities = measurement_operator(
        background_ensemble, measured_profile_position, measured_field_index
    )
    metadata = jnp.stack([obs_value, obs_error, obs_valid.astype(jnp.bfloat16)])
    own_rows = jnp.concatenate([measured_quantities, metadata], axis=0)
    pieces = []
    for offset in range(-REACH, REACH + 1):
        if offset == 0:
            pieces.append(own_rows)
        else:
            pieces.append(from_behind(own_rows, "tile", -offset))
    nearby = jnp.concatenate(pieces, axis=1)
    members_here = measured_quantities.shape[0]
    everyone = lax.all_gather(nearby[:members_here], "mem", axis=0, tiled=True)
    window = jnp.concatenate([everyone, nearby[members_here:]], axis=0)
    regrouped_states = lax.all_to_all(
        background_ensemble, "mem", split_axis=2, concat_axis=0, tiled=True
    )
    deviation, innovation, obs_precision = prepare(window)
    columns_here = regrouped_states.shape[2]
    local_land = lax.dynamic_slice_in_dim(
        terrain_indicator, lax.axis_index("mem") * columns_here, columns_here
    )
    transform = weights_for(
        deviation, innovation, obs_precision * local_weight[0, 0], 2 * REACH + 1
    )
    outputs = update(regrouped_states, transform, local_land)
    return lax.all_to_all(outputs, "mem", split_axis=0, concat_axis=2, tiled=True)


MESH = pl.DeviceIdType.MESH
CHUNKS = 4
CORES = 2
GATE = 0


def rounded_dot(a, b):
    return jnp.dot(a, b, preferred_element_type=jnp.float32)


def halves(a):
    high = a.astype(jnp.bfloat16)
    return high, (a - high.astype(jnp.float32)).astype(jnp.bfloat16)


def fine_dot(a, b):
    (a_high, a_low), (b_high, b_low) = a, b
    return rounded_dot(a_high, b_high) + (rounded_dot(a_high, b_low) + rounded_dot(a_low, b_high))


def drain(ref, sem):
    pltpu.make_async_copy(ref, ref, sem).wait()


def counter(bytes_ref):
    def count(size, sem):
        drain(bytes_ref.at[pl.ds(0, size // 512)], sem)

    return count


def kernel(
    n_mem,
    n_tile,
    pieces,
    units,
    ens_hbm,
    mix_hbm,
    surf_hbm,
    land_hbm,
    pos_hbm,
    field_hbm,
    valid_hbm,
    value_hbm,
    error_hbm,
    weight_hbm,
    out_ref,
    ens_ref,
    mix_ref,
    surf_ref,
    land_ref,
    pos_ref,
    field_ref,
    valid_ref,
    value_ref,
    error_ref,
    fc_ref,
    seen_ref,
    stage_ref,
    near_ref,
    slot_ref,
    rinv_ref,
    acc_ref,
    part_ref,
    got_ref,
    tsend_ref,
    trecv_ref,
    moved_ref,
    bytes_ref,
    ens_sem,
    in_sem,
    out_sem,
    seen_recv,
    fc_across,
    fc_unit,
    lift_sem,
    tile_recv,
    t_recv,
    hello,
    ready,
):
    members, fields, columns = ens_ref.shape
    everyone = members * n_mem
    slots = pos_ref.shape[1]
    near = 2 * REACH + 1
    wide = columns // n_mem
    count = counter(bytes_ref)
    me, tile = lax.axis_index("mem"), lax.axis_index("tile")
    n_y = n_mem // CORES
    y, core = me // CORES, lax.rem(me, CORES)
    sibling = y * CORES + (1 - core)
    across = [lax.rem(y + step, n_y) * CORES + core for step in range(1, n_y)]
    gate = me == GATE
    wraps = tile < REACH

    def both(first, second):
        return jnp.logical_and(first, second)

    barrier = pltpu.get_barrier_semaphore()
    for step in range(1, n_mem):
        peer = lax.rem(me + step, n_mem)

        @pl.when(peer != GATE)
        def _(peer=peer):
            pl.semaphore_signal(barrier, inc=1, device_id={"mem": peer}, device_id_type=MESH)

    for offset in range(-REACH, REACH + 1):
        if offset:
            there = lax.rem(tile + offset + n_tile, n_tile)
            pl.semaphore_signal(
                barrier, inc=1, device_id={"mem": GATE, "tile": there}, device_id_type=MESH
            )

    def ens_copy(step):
        where = pl.ds(pl.multiple_of(step * wide, wide), wide)
        return pltpu.make_async_copy(
            ens_hbm.at[:, :, where], ens_ref.at[:, :, where], ens_sem.at[min(step, 1)]
        )

    groups = [
        [(mix_hbm, mix_ref), (surf_hbm, surf_ref), (land_hbm, land_ref)],
        [(pos_hbm, pos_ref), (field_hbm, field_ref)],
        [
            (valid_hbm, valid_ref),
            (value_hbm, value_ref),
            (error_hbm, error_ref),
            (weight_hbm, stage_ref),
        ],
    ]
    loads = [
        [pltpu.make_async_copy(src, dst, in_sem.at[min(g, 1)]) for src, dst in group]
        for g, group in enumerate(groups)
    ]
    ens_copy(0).start()
    for copy in loads[0]:
        copy.start()
    for step in range(1, n_mem):
        ens_copy(step).start()
    for group in loads[1:]:
        for copy in group:
            copy.start()

    def remote(src, dst, send, recv, where):
        return pltpu.make_async_remote_copy(
            src_ref=src,
            dst_ref=dst,
            send_sem=send,
            recv_sem=recv,
            device_id=where,
            device_id_type=MESH,
        )

    n_pieces = len(pieces)
    lifted = n_pieces - 2

    def unit_sem(unit):
        return {len(units) - 1: 1, len(units) - 2: 2}.get(unit, 0)

    def piece_ref(piece, owner):
        block, first, stop = pieces[piece][:3]
        return fc_ref.at[owner, block, pl.ds(first, stop - first)]

    def fc_copy(piece, owner, recv, target):
        ref = piece_ref(piece, owner)
        return remote(ref, ref, out_sem.at[0], recv, {"mem": target})

    def fc_over(piece, owner, index, target):
        return fc_copy(piece, owner, fc_across.at[min(max(piece - 2, piece // 2), lifted - 2), index], target)

    def fc_near(piece, owner):
        return fc_copy(piece, owner, fc_unit.at[unit_sem(pieces[piece][3])], sibling)

    def own_fc(piece):
        for index, peer in enumerate(across):
            fc_over(piece, me, n_y - 2 - index, peer).start()
        fc_near(piece, me).start()

    def relay_fc(piece):
        for index, peer in enumerate(across):
            fc_over(piece, peer, index, peer).wait_recv()
            fc_near(piece, peer).start()

    def tail_ref(owner):
        first, stop = pieces[lifted][1], pieces[lifted + 1][2]
        return fc_ref.at[owner, n_mem - 1, pl.ds(first, stop - first)]

    def lift_out():
        fc_copy(lifted, me, lift_sem.at[0], sibling).start()
        fc_copy(lifted + 1, me, lift_sem.at[0], sibling).start()

    def tail_over():
        own_fc(lifted)
        own_fc(lifted + 1)

    def tail_relay():
        for index, peer in enumerate(across):
            drain(tail_ref(peer), fc_across.at[lifted - 2, index])
            fc_near(lifted, peer).start()
            fc_near(lifted + 1, peer).start()

    def lift_over():
        drain(tail_ref(sibling), lift_sem.at[0])
        for index, peer in enumerate(across):
            where = n_y - 2 - index
            fc_copy(lifted, sibling, fc_across.at[lifted - 1, where], peer).start()
            fc_copy(lifted + 1, sibling, fc_across.at[lifted, where], peer).start()
            partner = peer + (1 - 2 * core)
            fc_copy(lifted + 1, sibling, fc_unit.at[1], partner).start()

    def lift_relay():
        for index, peer in enumerate(across):
            partner = peer + (1 - 2 * core)
            drain(piece_ref(lifted, partner), fc_across.at[lifted - 1, index])
            fc_near(lifted, partner).start()

    def lift_end():
        for index, peer in enumerate(across):
            partner = peer + (1 - 2 * core)
            drain(piece_ref(lifted + 1, partner), fc_across.at[lifted, index])

    def seen_copy(h, target):
        ref = seen_ref.at[me, h]
        return remote(ref, ref, out_sem.at[0], seen_recv.at[h // CORES], {"mem": target})

    def own_seen(h):
        user = h % CORES
        for step in range(1, n_y):
            seen_copy(h, lax.rem(y + step, n_y) * CORES + user).start()

    def near_seen():
        for i in range(CHUNKS // CORES):
            h = i * CORES + 1 - core
            ref = seen_ref.at[me, h]
            remote(ref, ref, out_sem.at[0], seen_recv.at[i], {"mem": sibling}).start()

    def tile_peer(offset):
        return {"tile": lax.rem(tile + offset + n_tile, n_tile)}

    def mix_part(step, start, stop):
        where = pl.ds(pl.multiple_of(step * wide, wide), wide)
        low, high = max(start - 8, 0), min(stop + 8, fields)
        x = jnp.transpose(ens_ref[:, low:high, where].astype(jnp.float32), (1, 0, 2))
        rate = mix_ref[:, where][None]
        above = jnp.concatenate([x[:1], x[:-1]], axis=0)
        below = jnp.concatenate([x[1:], x[-1:]], axis=0)
        keep = slice(start - low, stop - low)
        x, above, below = x[keep], above[keep], below[keep]
        stepped = x + rate * (above - 2.0 * x + below) - 0.05 * x * x * x
        if start == 0:
            top = stepped[:1] + surf_ref[:, where][None]
            stepped = jnp.concatenate([top, stepped[1:]], axis=0)
        land = jnp.broadcast_to(land_ref[:, where][None], x.shape) > 0
        fc_ref[me, step, start:stop] = jnp.where(land, stepped, x).astype(jnp.bfloat16)

    def enter():
        pl.semaphore_wait(barrier, n_mem - 1)
        pl.semaphore_signal(hello, inc=1, device_id={"mem": GATE}, device_id_type=MESH)

    def send_weights():
        for j in range(near):
            for user in range(CORES):
                if j != REACH:
                    remote(
                        stage_ref.at[j, :, user],
                        near_ref.at[core * near + j],
                        out_sem.at[0],
                        tile_recv.at[0],
                        {"mem": y * CORES + user, **tile_peer(j - REACH)},
                    ).start()
        remote(
            stage_ref.at[REACH, :, 1 - core],
            near_ref.at[core * near + REACH],
            out_sem.at[0],
            tile_recv.at[0],
            {"mem": sibling},
        ).start()

    def admit():
        pl.semaphore_wait(barrier, 2 * REACH * n_mem)
        for step in range(1, n_mem):
            peer = lax.rem(me + step, n_mem)
            pl.semaphore_signal(ready, inc=1, device_id={"mem": peer}, device_id_type=MESH)

    def meet_tiles():
        @pl.when(both(wraps, gate))
        def _():
            admit()

        @pl.when(jnp.logical_not(gate))
        def _():
            pl.semaphore_wait(ready, 1)

        send_weights()

    @pl.when(me >= CORES)
    def _():
        enter()

    head = pieces[0][2]
    ens_copy(0).wait()
    count(4 * columns * (members + 2), in_sem.at[0])
    mix_part(0, 0, head)

    @pl.when(both(me < CORES, me != GATE))
    def _():
        enter()

    @pl.when(me != GATE)
    def _():
        own_fc(0)

    mix_part(0, head, fields)

    @pl.when(me != GATE)
    def _():
        own_fc(1)

    count(2 * members * fields * wide * (n_mem - 1), ens_sem.at[1])

    def mix(step, carry):
        mix_part(step, 0, fields)
        return carry

    lax.fori_loop(1, n_mem, mix, 0)

    count(4 * slots * (near + 4), in_sem.at[1])

    @pl.when(gate)
    def _():
        pl.semaphore_wait(hello, n_mem - 1)
        own_fc(0)
        own_fc(1)

    @pl.when(both(gate, jnp.logical_not(wraps)))
    def _():
        admit()

    @pl.when(core == 0)
    def _():
        lift_out()

    share = slots // CHUNKS
    width = min(share, 512)
    flat = jnp.concatenate(
        [fc_ref[me, b].reshape(fields * members, wide) for b in range(n_mem)], axis=1
    )
    for h in range(CHUNKS):
        for step in range(share // width):
            where = pl.ds(h * share + step * width, width)
            rows = lax.broadcasted_iota(jnp.int32, (columns, width), 0)
            hot = jnp.where(rows == pos_ref[:, where], 1.0, 0.0).astype(jnp.bfloat16)
            found = rounded_dot(flat, hot)
            wanted = jnp.broadcast_to(field_ref[:, where], (members, width))
            total = found[:members]
            for f in range(1, fields):
                total = jnp.where(wanted == f, found[f * members : (f + 1) * members], total)
            seen_ref[me, h, :, pl.ds(step * width, width)] = total.astype(jnp.bfloat16)
        if h % CORES == CORES - 1:
            for done in range(h + 1 - CORES, h + 1):
                own_seen(done)
            if h < CORES:
                own_fc(2)
        if h == 0:

            @pl.when(jnp.logical_not(wraps))
            def _():
                meet_tiles()

    near_seen()
    for piece in range(3, lifted):
        own_fc(piece)


    @pl.when(wraps)
    def _():
        meet_tiles()

    rounds = CHUNKS // CORES
    lanes = 128
    base = [
        valid_ref[i, core].astype(jnp.float32) / error_ref[i, core].astype(jnp.float32)
        for i in range(rounds)
    ]
    for i in range(rounds):
        slot_ref[CORES * near, i] = value_ref[i, core].astype(jnp.float32)
        for spare in range(CORES * near + 1, slot_ref.shape[0]):
            slot_ref[spare, i] = jnp.zeros_like(base[i])
    near_ref[core * near + REACH] = stage_ref[REACH, :, core]

    for index, peer in enumerate(across):
        drain(fc_ref.at[peer, 0, pl.ds(0, pieces[1][2])], fc_across.at[0, index])
        fc_near(0, peer).start()
        fc_near(1, peer).start()

    drain(near_ref.at[pl.ds(0, CORES * near - 1)], tile_recv.at[0])
    for r in range(CORES * near):
        for i in range(rounds):
            slot_ref[r, i] = base[i] * near_ref[r, i]
    for i in range(rounds):
        for r in range(share // lanes):
            rinv_ref[i, :, r * lanes : (r + 1) * lanes] = slot_ref[:, i, r, :]

    for i in range(rounds):
        drain(seen_ref.at[pl.ds(0, n_mem - 1), 0], seen_recv.at[i])
        seen = jnp.concatenate(
            [seen_ref[m, i * CORES + core].astype(jnp.float32) for m in range(n_mem)], axis=0
        )
        average = jnp.mean(seen, axis=0, keepdims=True)
        deviation = seen - average
        rinv = rinv_ref[i]
        innovation = rinv[CORES * near : CORES * near + 1] - average
        right = jnp.concatenate(
            [deviation, jnp.broadcast_to(innovation, deviation.shape)], axis=0
        ).astype(jnp.bfloat16)
        rows = [
            (deviation * rinv[r : r + 1]).astype(jnp.bfloat16) for r in range(CORES * near)
        ]
        for user in range(CORES):
            where = slice(user * near * everyone, (user + 1) * near * everyone)
            sums = lax.dot_general(
                jnp.concatenate(rows[user * near : (user + 1) * near], axis=0),
                right,
                (((1,), (1,)), ((), ())),
                preferred_element_type=jnp.float32,
            )
            acc_ref[where] = sums + acc_ref[where] if i else sums

    fold = everyone // 2
    lane = lax.broadcasted_iota(jnp.int32, (fold, 2 * everyone), 1)
    for r in range(CORES * near):
        upper = acc_ref[r * everyone : r * everyone + fold]
        lower = acc_ref[r * everyone + fold : (r + 1) * everyone]
        packed = jnp.where(lane < everyone + fold, pltpu.roll(lower, fold, 1), upper)
        packed = jnp.where(lane < everyone, upper, packed)
        packed = jnp.where(lane < 2 * everyone - fold // 2, packed, lower)
        part_ref[r] = packed.astype(jnp.bfloat16)
        user, j = r // near, r % near
        if j != REACH:
            remote(
                part_ref.at[r],
                got_ref.at[core * near + j],
                out_sem.at[0],
                tile_recv.at[1],
                {"mem": y * CORES + user, **tile_peer(REACH - j)},
            ).start()
    remote(
        part_ref.at[(1 - core) * near + REACH],
        got_ref.at[core * near + REACH],
        out_sem.at[0],
        tile_recv.at[1],
        {"mem": sibling},
    ).start()
    got_ref[core * near + REACH] = part_ref[core * near + REACH]

    for index, peer in enumerate(across):
        first, stop = pieces[2][1], pieces[3][2]
        drain(fc_ref.at[peer, 0, pl.ds(first, stop - first)], fc_across.at[1, index])
        fc_near(2, peer).start()
        fc_near(3, peer).start()

    drain(got_ref.at[pl.ds(0, CORES * near - 1)], tile_recv.at[1])

    summed = got_ref[0].astype(jnp.float32)
    for r in range(1, CORES * near):
        summed = summed + got_ref[r].astype(jnp.float32)
    summed = summed / (everyone - 1.0)
    flipped = jnp.transpose(summed)
    spread = jnp.concatenate(
        [
            summed[:, :everyone],
            jnp.concatenate(
                [flipped[fold:everyone], summed[:, everyone : everyone + fold]], axis=1
            ),
        ],
        axis=0,
    )
    first, second = everyone + fold, 2 * everyone - fold // 2
    pulled = jnp.concatenate([flipped[first : first + 8], flipped[second : second + 8]], axis=1)
    rows = lax.broadcasted_iota(jnp.int32, (everyone, everyone), 0)
    identity = jnp.where(
        rows == lax.broadcasted_iota(jnp.int32, (everyone, everyone), 1), 1.0, 0.0
    )
    system = identity + spread
    square = jnp.sum(system * system, keepdims=True)
    scale = jnp.sqrt(square)
    rows = jnp.concatenate([pulled, jnp.ones_like(pulled)], axis=0)
    powers = [rows]
    parts = halves(system)
    second = fine_dot(parts, parts) / square
    powers.append(fine_dot(halves(rows), parts) / scale)
    current = system / scale
    parts, second_parts = halves(current), halves(second)
    third = fine_dot(second_parts, parts)
    fourth = fine_dot(second_parts, second_parts)
    for power in range(2, 6):
        powers.append(fine_dot(halves(powers[power - 2]), second_parts))
    weights = (2.25, -2.4375, 1.6875, -0.5625, 0.0625)

    def combine(terms):
        return sum(weight * term for weight, term in zip(weights, terms))

    root = combine([identity, current, second, third, fourth])
    root_parts = halves(root)
    inner_parts = halves(fine_dot(parts, root_parts))
    outer_parts = halves(fine_dot(root_parts, root_parts))
    root = 1.5 * root - 0.5 * fine_dot(inner_parts, outer_parts)
    drawn = 1.5 * combine(powers[:5]) - 0.5 * fine_dot(halves(combine(powers[1:])), outer_parts)
    root_parts = halves(root)
    ones = jnp.ones((everyone, everyone), jnp.bfloat16)
    sums = rounded_dot(root_parts[0], ones) + rounded_dot(root_parts[1], ones)
    mean_weight = fine_dot(halves(drawn[:8]), root_parts)[:1] / scale
    weight_sum = jnp.sum(drawn[:1] * drawn[8:9], axis=1, keepdims=True) / scale
    turned = root / jnp.sqrt(scale) + mean_weight
    turned = turned + (1.0 - sums / jnp.sqrt(scale) - weight_sum) / everyone
    for m in range(n_mem):
        tsend_ref[m, :, :everyone] = turned[m * members : (m + 1) * members]
        tsend_ref[m, :, everyone:] = jnp.zeros((members, everyone), jnp.float32)

    for step in range(1, n_mem):
        target = lax.rem(me + step, n_mem)
        remote(
            tsend_ref.at[target],
            trecv_ref.at[me],
            out_sem.at[0],
            t_recv.at[0],
            {"mem": target},
        ).start()
    @pl.when(core != 0)
    def _():
        tail_over()
        lift_over()

    trecv_ref[me] = tsend_ref[me]

    group = 8

    def apply(block, start, stop):
        where = pl.ds(block * wide, wide)
        left = jnp.concatenate(halves(trecv_ref[block][:, :everyone]), axis=0)
        land = jnp.broadcast_to(land_ref[:, where], (members, wide)) > 0
        for first in range(start, stop, group):
            end = min(first + group, stop)
            states = jnp.concatenate(
                [
                    jnp.concatenate([fc_ref[m, block, f] for m in range(n_mem)], axis=0)
                    for f in range(first, end)
                ],
                axis=1,
            )
            pair = rounded_dot(left, states)
            total = pair[:members] + pair[members:]
            for f in range(end - first):
                moved_ref[block, first + f] = jnp.where(
                    land,
                    total[:, f * wide : (f + 1) * wide],
                    fc_ref[me, block, first + f].astype(jnp.float32),
                )
        moved = jnp.transpose(moved_ref[block, start:stop], (1, 0, 2)).astype(jnp.bfloat16)
        out_ref[:, start:stop, where] = moved

    for piece in range(4, lifted):
        relay_fc(piece)

    @pl.when(core != 0)
    def _():
        tail_relay()

    drain(trecv_ref.at[pl.ds(0, n_mem - 1)], t_recv.at[0])

    @pl.when(core != 0)
    def _():
        lift_relay()

    count(2 * n_y * fields * (n_mem - 1) * members * wide, fc_unit.at[0])

    for unit in units[:-2]:
        apply(*unit)

    count(2 * n_y * (units[-2][2] - units[-2][1]) * members * wide, fc_unit.at[2])

    apply(*units[-2])

    @pl.when(core == 0)
    def _():
        last_rows = units[-1][2] - units[-1][1]
        count(2 * (n_mem - 1) * last_rows * members * wide, fc_unit.at[1])

    @pl.when(core != 0)
    def _():
        lift_end()

    apply(*units[-1])

    kinds = [fc_ref.at[0], seen_ref.at[0], part_ref, stage_ref.at[:, :, 0], tsend_ref.at[0]]
    sizes = [ref.dtype.itemsize * math.prod(ref.shape) for ref in kinds]
    counts = [n_mem - 1, n_y - 1, 0, 0, n_mem - 1]
    total = sum(size * count for size, count in zip(sizes, counts))
    total += sizes[1] // CORES
    total += (sizes[2] + sizes[3] * CORES) * (CORES * near - 1) // (CORES * near)
    size = 2 * members * wide * (units[-1][2] - units[-1][1])
    total -= (n_mem - 1) * size

    @pl.when(core == 0)
    def _():
        count(total + size, out_sem.at[0])

    @pl.when(core != 0)
    def _():
        count(total + (1 + 4 * (n_y - 1)) * size, out_sem.at[0])


def on_device(
    n_mem,
    n_tile,
    ensemble_profiles_before,
    mixing_coefficient,
    surface_driver,
    terrain_indicator,
    measured_profile_position,
    measured_field_index,
    obs_valid,
    obs_value,
    obs_error,
    local_weight,
):
    members, fields, columns = ensemble_profiles_before.shape
    slots = measured_field_index.shape[0]
    everyone = members * n_mem
    near = 2 * REACH + 1
    n_y = n_mem // CORES
    wide = columns // n_mem
    units = [(block, 0, fields) for block in range(n_mem - 1)]
    cuts = (0, fields - 12, fields)
    units += [(n_mem - 1, *ends) for ends in zip(cuts[:-1], cuts[1:])]
    pieces = [(0, 0, 8, 0), (0, 8, 28, 0), (0, 28, 32, 0), (0, 32, fields, 0)]
    pieces += [(*unit, index) for index, unit in enumerate(units[:-1]) if index]
    pieces += [(n_mem - 1, fields - 12, fields - 4, n_mem), (n_mem - 1, fields - 4, fields, n_mem)]
    spare = 4 * everyone * fields * columns
    row = lambda a: a.reshape(1, -1)
    table = (CHUNKS // CORES, CORES, slots // CHUNKS // 128, 128)
    far = pl.BlockSpec(memory_space=pltpu.HBM)
    dma = pltpu.SemaphoreType.DMA
    return pl.pallas_call(
        functools.partial(kernel, n_mem, n_tile, pieces, units),
        out_shape=pltpu.VMEM(ensemble_profiles_before.shape, jnp.bfloat16),
        in_specs=[far] * 10,
        out_specs=pl.BlockSpec(memory_space=pltpu.VMEM),
        scratch_shapes=[
            pltpu.VMEM((members, fields, columns), jnp.bfloat16),
            pltpu.VMEM((1, columns), jnp.float32),
            pltpu.VMEM((members, columns), jnp.float32),
            pltpu.VMEM((1, columns), jnp.int32),
            pltpu.VMEM((1, slots), jnp.int32),
            pltpu.VMEM((1, slots), jnp.int32),
            pltpu.VMEM(table, jnp.int32),
            pltpu.VMEM(table, jnp.bfloat16),
            pltpu.VMEM(table, jnp.bfloat16),
            pltpu.VMEM((n_mem, n_mem, fields, members, wide), jnp.bfloat16),
            pltpu.VMEM((n_mem, CHUNKS, members, slots // CHUNKS), jnp.bfloat16),
            pltpu.VMEM((near, *table), jnp.float32),
            pltpu.VMEM((CORES * near, table[0], *table[2:]), jnp.float32),
            pltpu.VMEM((16, table[0], *table[2:]), jnp.float32),
            pltpu.VMEM((table[0], 16, slots // CHUNKS), jnp.float32),
            pltpu.VMEM((CORES * near * everyone, 2 * everyone), jnp.float32),
            pltpu.VMEM((CORES * near, everyone // 2, 2 * everyone), jnp.bfloat16),
            pltpu.VMEM((CORES * near, everyone // 2, 2 * everyone), jnp.bfloat16),
            pltpu.VMEM((n_mem, members, 2 * everyone), jnp.float32),
            pltpu.VMEM((n_mem, members, 2 * everyone), jnp.float32),
            pltpu.VMEM((n_mem, fields, members, wide), jnp.float32),
            pltpu.VMEM((spare // 512, 128), jnp.float32),
            dma((2,)),
            dma((2,)),
            dma((1,)),
            dma((CHUNKS // CORES,)),
            dma((len(pieces) - 1, n_y - 1)),
            dma((3,)),
            dma((1,)),
            dma((2,)),
            dma((1,)),
            pltpu.SemaphoreType.REGULAR,
            pltpu.SemaphoreType.REGULAR,
        ],
        compiler_params=pltpu.CompilerParams(
            collective_id=0, has_side_effects=True, vmem_limit_bytes=66_000_000
        ),
    )(
        ensemble_profiles_before,
        row(mixing_coefficient),
        surface_driver,
        row(terrain_indicator),
        row(measured_profile_position),
        row(measured_field_index),
        obs_valid.reshape(table),
        obs_value.reshape(table),
        obs_error.reshape(table),
        local_weight.reshape(near, *table),
    )


def fits(n_mem, n_tile, ensemble, slots):
    members, fields, columns = ensemble[0] // n_mem, ensemble[1], ensemble[2] // n_tile
    return (
        n_mem % CORES == 0
        and n_mem > CORES
        and 2 * members * n_mem == 128
        and n_tile > 2 * REACH
        and members % 16 == 0
        and fields % 8 == 0
        and fields > 32
        and columns % (128 * n_mem) == 0
        and slots // n_tile % (1024 * CHUNKS) == 0
    )


def solution(mesh):
    in_specs = (
        P("mem", None, "tile"),
        P("tile"),
        P("mem", "tile"),
        P("tile"),
        P("tile"),
        P("tile"),
        P("tile"),
        P("tile"),
        P("tile"),
        P("mem", "tile", None),
    )
    out_specs = P("mem", None, "tile")

    def run(*args):
        sizes = mesh.shape["mem"], mesh.shape["tile"]
        body = plain_on_device
        if fits(*sizes, args[0].shape, args[5].shape[0]):
            body = functools.partial(on_device, *sizes)
        return jax.shard_map(
            body, mesh=mesh, in_specs=in_specs, out_specs=out_specs, check_vma=False
        )(*args)

    return run
```

```python
import functools
import math

import jax
import jax.numpy as jnp
from jax import lax
from jax.experimental import pallas as pl
from jax.experimental.pallas import tpu as pltpu
from jax.sharding import PartitionSpec as P

REACH = 2
NS_ITERS = 3


EXACT = lax.Precision.HIGHEST


def from_behind(value, axis, steps):
    count = lax.axis_size(axis)
    pairs = [(source, (source + steps) % count) for source in range(count)]
    return lax.ppermute(value, axis, pairs)


def vertical_mixing_step(
    ensemble_profiles_before, mixing_coefficient, surface_driver, terrain_indicator
):
    values = ensemble_profiles_before.astype(jnp.float32)
    above_layer = jnp.concatenate([values[:, :1], values[:, :-1]], axis=1)
    below_layer = jnp.concatenate([values[:, 1:], values[:, -1:]], axis=1)
    diffused = values + mixing_coefficient[None, None, :] * (
        above_layer - 2.0 * values + below_layer
    )
    stepped = diffused - 0.05 * values * values * values
    surface = jnp.concatenate([stepped[:, :1] + surface_driver[:, None, :], stepped[:, 1:]], axis=1)
    result = jnp.where(terrain_indicator[None, None, :] > 0, surface, values)
    return result.astype(jnp.bfloat16)


def measurement_operator(background_ensemble, measured_profile_position, measured_field_index):
    profile_sequence = background_ensemble.shape[2]
    unrolled_ensemble = background_ensemble.reshape(background_ensemble.shape[0], -1)
    slot_index = measured_field_index * profile_sequence + measured_profile_position
    return jnp.take(unrolled_ensemble, slot_index, axis=1)


def prepare(window):
    ensemble_profiles = window.shape[0] - 3
    measured_quantities = window[:ensemble_profiles].astype(jnp.float32)
    average = jnp.mean(measured_quantities, axis=0)
    deviation = measured_quantities - average
    innovation = window[ensemble_profiles].astype(jnp.float32) - average
    obs_precision = window[ensemble_profiles + 2].astype(jnp.float32) / window[
        ensemble_profiles + 1
    ].astype(jnp.float32)
    return (deviation, innovation, obs_precision)


def weights_for(deviation, innovation, precision, portions):
    ensemble_profiles = deviation.shape[0]
    portion_width = deviation.shape[1] // portions
    spread = jnp.zeros((ensemble_profiles, ensemble_profiles), jnp.float32)
    for portion_index in range(portions):
        portion = deviation[:, portion_index * portion_width : (portion_index + 1) * portion_width]
        scaled = (
            portion
            * precision[None, portion_index * portion_width : (portion_index + 1) * portion_width]
        )
        spread = spread + jnp.dot(
            scaled, portion.T, precision=EXACT, preferred_element_type=jnp.float32
        )
    spread = spread / (ensemble_profiles - 1.0)
    pulled = jnp.dot(
        deviation, precision * innovation, precision=EXACT, preferred_element_type=jnp.float32
    ) / (ensemble_profiles - 1.0)
    identity = jnp.eye(ensemble_profiles, dtype=jnp.float32)
    system = identity + spread
    norm_scale = jnp.sqrt(jnp.sum(system * system))

    def newton(sweep, carry):
        current, inv_root = carry
        middle = 1.5 * identity - 0.5 * jnp.dot(inv_root, current, precision=EXACT)
        return (
            jnp.dot(current, middle, precision=EXACT),
            jnp.dot(middle, inv_root, precision=EXACT),
        )

    current, inv_root = lax.fori_loop(0, NS_ITERS, newton, (system / norm_scale, identity))
    inv_root = inv_root / jnp.sqrt(norm_scale)
    inverse = jnp.dot(inv_root, inv_root, precision=EXACT)
    mean_weight = jnp.dot(inverse, pulled, precision=EXACT)
    return inv_root + mean_weight[:, None]


def update(states, transform, land_block):
    values = states.astype(jnp.float32)
    average = jnp.mean(values, axis=0)
    deviation = values - average[None]
    moved = jnp.einsum("isc,ij->jsc", deviation, transform, precision=EXACT)
    result = jnp.where(land_block[None, None, :] > 0, average[None] + moved, values)
    return result.astype(jnp.bfloat16)


def plain_on_device(
    ensemble_profiles_before,
    mixing_coefficient,
    surface_driver,
    terrain_indicator,
    measured_profile_position,
    measured_field_index,
    obs_valid,
    obs_value,
    obs_error,
    local_weight,
):
    background_ensemble = vertical_mixing_step(
        ensemble_profiles_before, mixing_coefficient, surface_driver, terrain_indicator
    )
    measured_quantities = measurement_operator(
        background_ensemble, measured_profile_position, measured_field_index
    )
    metadata = jnp.stack([obs_value, obs_error, obs_valid.astype(jnp.bfloat16)])
    own_rows = jnp.concatenate([measured_quantities, metadata], axis=0)
    pieces = []
    for offset in range(-REACH, REACH + 1):
        if offset == 0:
            pieces.append(own_rows)
        else:
            pieces.append(from_behind(own_rows, "tile", -offset))
    nearby = jnp.concatenate(pieces, axis=1)
    members_here = measured_quantities.shape[0]
    everyone = lax.all_gather(nearby[:members_here], "mem", axis=0, tiled=True)
    window = jnp.concatenate([everyone, nearby[members_here:]], axis=0)
    regrouped_states = lax.all_to_all(
        background_ensemble, "mem", split_axis=2, concat_axis=0, tiled=True
    )
    deviation, innovation, obs_precision = prepare(window)
    columns_here = regrouped_states.shape[2]
    local_land = lax.dynamic_slice_in_dim(
        terrain_indicator, lax.axis_index("mem") * columns_here, columns_here
    )
    transform = weights_for(
        deviation, innovation, obs_precision * local_weight[0, 0], 2 * REACH + 1
    )
    outputs = update(regrouped_states, transform, local_land)
    return lax.all_to_all(outputs, "mem", split_axis=0, concat_axis=2, tiled=True)


MESH = pl.DeviceIdType.MESH
CHUNKS = 4
CORES = 2
GATE = 0


def rounded_dot(a, b):
    return jnp.dot(a, b, preferred_element_type=jnp.float32)


def halves(a):
    high = a.astype(jnp.bfloat16)
    return high, (a - high.astype(jnp.float32)).astype(jnp.bfloat16)


def fine_dot(a, b):
    (a_high, a_low), (b_high, b_low) = a, b
    return rounded_dot(a_high, b_high) + (rounded_dot(a_high, b_low) + rounded_dot(a_low, b_high))


def drain(ref, sem):
    pltpu.make_async_copy(ref, ref, sem).wait()


def counter(bytes_ref):
    def count(size, sem):
        drain(bytes_ref.at[pl.ds(0, size // 512)], sem)

    return count


def kernel(
    n_mem,
    n_tile,
    pieces,
    units,
    ens_hbm,
    mix_hbm,
    surf_hbm,
    land_hbm,
    pos_hbm,
    field_hbm,
    valid_hbm,
    value_hbm,
    error_hbm,
    weight_hbm,
    out_ref,
    ens_ref,
    mix_ref,
    surf_ref,
    land_ref,
    pos_ref,
    field_ref,
    valid_ref,
    value_ref,
    error_ref,
    fc_ref,
    seen_ref,
    stage_ref,
    near_ref,
    slot_ref,
    rinv_ref,
    acc_ref,
    part_ref,
    got_ref,
    tsend_ref,
    trecv_ref,
    left_ref,
    moved_ref,
    bytes_ref,
    ens_sem,
    in_sem,
    out_sem,
    seen_recv,
    fc_across,
    fc_unit,
    lift_sem,
    tile_recv,
    t_recv,
    hello,
    ready,
):
    members, fields, columns = ens_ref.shape
    everyone = members * n_mem
    slots = pos_ref.shape[1]
    near = 2 * REACH + 1
    wide = columns // n_mem
    count = counter(bytes_ref)
    me, tile = lax.axis_index("mem"), lax.axis_index("tile")
    n_y = n_mem // CORES
    y, core = me // CORES, lax.rem(me, CORES)
    sibling = y * CORES + (1 - core)
    across = [lax.rem(y + step, n_y) * CORES + core for step in range(1, n_y)]
    gate = me == GATE
    wraps = tile < REACH

    def both(first, second):
        return jnp.logical_and(first, second)

    barrier = pltpu.get_barrier_semaphore()
    for step in range(1, n_mem):
        peer = lax.rem(me + step, n_mem)

        @pl.when(peer != GATE)
        def _(peer=peer):
            pl.semaphore_signal(barrier, inc=1, device_id={"mem": peer}, device_id_type=MESH)

    for offset in range(-REACH, REACH + 1):
        if offset:
            there = lax.rem(tile + offset + n_tile, n_tile)
            pl.semaphore_signal(
                barrier, inc=1, device_id={"mem": GATE, "tile": there}, device_id_type=MESH
            )

    opening = pieces[0][2] + 8

    def ens_copy(step, rows, sem):
        where = (slice(None), pl.ds(*rows), pl.ds(step * wide, wide))
        return pltpu.make_async_copy(ens_hbm.at[where], ens_ref.at[where], ens_sem.at[sem])

    groups = [
        [(mix_hbm, mix_ref), (surf_hbm, surf_ref), (land_hbm, land_ref)],
        [(pos_hbm, pos_ref), (field_hbm, field_ref)],
        [
            (valid_hbm, valid_ref),
            (value_hbm, value_ref),
            (error_hbm, error_ref),
            (weight_hbm, stage_ref),
        ],
    ]
    loads = [
        [pltpu.make_async_copy(src, dst, in_sem.at[min(g, 1)]) for src, dst in group]
        for g, group in enumerate(groups)
    ]
    first_load = ens_copy(0, (0, opening), 0)
    first_load.start()
    for copy in loads[0]:
        copy.start()
    ens_copy(0, (opening, fields - opening), 1).start()
    for step in range(1, n_mem):
        ens_copy(step, (0, fields), 2).start()
    for group in loads[1:]:
        for copy in group:
            copy.start()

    def remote(src, dst, send, recv, where):
        return pltpu.make_async_remote_copy(
            src_ref=src,
            dst_ref=dst,
            send_sem=send,
            recv_sem=recv,
            device_id=where,
            device_id_type=MESH,
        )

    n_pieces = len(pieces)
    lifted = n_pieces - 2

    def unit_sem(unit):
        return {len(units) - 1: 1, len(units) - 2: 2}.get(unit, 0)

    def piece_ref(piece, owner):
        block, first, stop = pieces[piece][:3]
        return fc_ref.at[owner, block, pl.ds(first, stop - first)]

    def fc_copy(piece, owner, recv, target):
        ref = piece_ref(piece, owner)
        return remote(ref, ref, out_sem.at[0], recv, {"mem": target})

    def fc_over(piece, owner, index, target):
        return fc_copy(piece, owner, fc_across.at[min(max(piece - 2, piece // 2), lifted - 2), index], target)

    def fc_near(piece, owner):
        return fc_copy(piece, owner, fc_unit.at[unit_sem(pieces[piece][3])], sibling)

    def own_fc(piece):
        for index, peer in enumerate(across):
            fc_over(piece, me, n_y - 2 - index, peer).start()
        fc_near(piece, me).start()

    def relay_fc(piece):
        for index, peer in enumerate(across):
            fc_over(piece, peer, index, peer).wait_recv()
            fc_near(piece, peer).start()

    def tail_ref(owner):
        first, stop = pieces[lifted][1], pieces[lifted + 1][2]
        return fc_ref.at[owner, n_mem - 1, pl.ds(first, stop - first)]

    def lift_out():
        fc_copy(lifted, me, lift_sem.at[0], sibling).start()
        fc_copy(lifted + 1, me, lift_sem.at[0], sibling).start()

    def tail_over():
        own_fc(lifted)
        own_fc(lifted + 1)

    def tail_relay():
        for index, peer in enumerate(across):
            drain(tail_ref(peer), fc_across.at[lifted - 2, index])
            fc_near(lifted, peer).start()
            fc_near(lifted + 1, peer).start()

    def lift_over():
        drain(tail_ref(sibling), lift_sem.at[0])
        for index, peer in enumerate(across):
            where = n_y - 2 - index
            fc_copy(lifted, sibling, fc_across.at[lifted - 1, where], peer).start()
            fc_copy(lifted + 1, sibling, fc_across.at[lifted, where], peer).start()
            partner = peer + (1 - 2 * core)
            fc_copy(lifted + 1, sibling, fc_unit.at[1], partner).start()

    def lift_relay():
        for index, peer in enumerate(across):
            partner = peer + (1 - 2 * core)
            drain(piece_ref(lifted, partner), fc_across.at[lifted - 1, index])
            fc_near(lifted, partner).start()

    def lift_end():
        for index, peer in enumerate(across):
            partner = peer + (1 - 2 * core)
            drain(piece_ref(lifted + 1, partner), fc_across.at[lifted, index])

    def seen_copy(h, target):
        ref = seen_ref.at[me, h]
        return remote(ref, ref, out_sem.at[0], seen_recv.at[h // CORES], {"mem": target})

    def own_seen(h):
        user = h % CORES
        for step in range(1, n_y):
            seen_copy(h, lax.rem(y + step, n_y) * CORES + user).start()

    def near_seen():
        for i in range(CHUNKS // CORES):
            h = i * CORES + 1 - core
            ref = seen_ref.at[me, h]
            remote(ref, ref, out_sem.at[0], seen_recv.at[i], {"mem": sibling}).start()

    def tile_peer(offset):
        return {"tile": lax.rem(tile + offset + n_tile, n_tile)}

    def mix_part(step, start, stop):
        where = pl.ds(pl.multiple_of(step * wide, wide), wide)
        low, high = max(start - 8, 0), min(stop + 8, fields)
        x = jnp.transpose(ens_ref[:, low:high, where].astype(jnp.float32), (1, 0, 2))
        rate = mix_ref[:, where][None]
        above = jnp.concatenate([x[:1], x[:-1]], axis=0)
        below = jnp.concatenate([x[1:], x[-1:]], axis=0)
        keep = slice(start - low, stop - low)
        x, above, below = x[keep], above[keep], below[keep]
        stepped = x + rate * (above - 2.0 * x + below) - 0.05 * x * x * x
        if start == 0:
            top = stepped[:1] + surf_ref[:, where][None]
            stepped = jnp.concatenate([top, stepped[1:]], axis=0)
        land = jnp.broadcast_to(land_ref[:, where][None], x.shape) > 0
        fc_ref[me, step, start:stop] = jnp.where(land, stepped, x).astype(jnp.bfloat16)

    def enter():
        pl.semaphore_wait(barrier, n_mem - 1)
        pl.semaphore_signal(hello, inc=1, device_id={"mem": GATE}, device_id_type=MESH)

    def send_weights():
        for j in range(near):
            for user in range(CORES):
                if j != REACH:
                    remote(
                        stage_ref.at[j, :, user],
                        near_ref.at[core * near + j],
                        out_sem.at[0],
                        tile_recv.at[0],
                        {"mem": y * CORES + user, **tile_peer(j - REACH)},
                    ).start()
        remote(
            stage_ref.at[REACH, :, 1 - core],
            near_ref.at[core * near + REACH],
            out_sem.at[0],
            tile_recv.at[0],
            {"mem": sibling},
        ).start()

    def admit():
        pl.semaphore_wait(barrier, 2 * REACH * n_mem)
        for step in range(1, n_mem):
            peer = lax.rem(me + step, n_mem)
            pl.semaphore_signal(ready, inc=1, device_id={"mem": peer}, device_id_type=MESH)

    def meet_tiles():
        @pl.when(both(wraps, gate))
        def _():
            admit()

        @pl.when(jnp.logical_not(gate))
        def _():
            pl.semaphore_wait(ready, 1)

        send_weights()

    @pl.when(me >= CORES)
    def _():
        enter()

    head = pieces[0][2]
    first_load.wait()
    count(4 * columns * (members + 2), in_sem.at[0])
    mix_part(0, 0, head)

    @pl.when(both(me < CORES, me != GATE))
    def _():
        enter()

    @pl.when(me != GATE)
    def _():
        own_fc(0)

    count(2 * members * wide * (fields - opening), ens_sem.at[1])
    mix_part(0, head, fields)

    @pl.when(me != GATE)
    def _():
        own_fc(1)

    count(2 * members * wide * fields * (n_mem - 1), ens_sem.at[2])

    def mix(step, carry):
        mix_part(step, 0, fields)
        return carry

    lax.fori_loop(1, n_mem, mix, 0)

    count(4 * slots * (near + 4), in_sem.at[1])

    @pl.when(gate)
    def _():
        pl.semaphore_wait(hello, n_mem - 1)
        own_fc(0)
        own_fc(1)

    @pl.when(both(gate, jnp.logical_not(wraps)))
    def _():
        admit()

    @pl.when(core == 0)
    def _():
        lift_out()

    share = slots // CHUNKS
    width = min(share, 512)
    flat = jnp.concatenate(
        [fc_ref[me, b].reshape(fields * members, wide) for b in range(n_mem)], axis=1
    )
    for h in range(CHUNKS):
        for step in range(share // width):
            where = pl.ds(h * share + step * width, width)
            rows = lax.broadcasted_iota(jnp.int32, (columns, width), 0)
            hot = jnp.where(rows == pos_ref[:, where], 1.0, 0.0).astype(jnp.bfloat16)
            found = rounded_dot(flat, hot)
            wanted = jnp.broadcast_to(field_ref[:, where], (members, width))
            total = found[:members]
            for f in range(1, fields):
                total = jnp.where(wanted == f, found[f * members : (f + 1) * members], total)
            seen_ref[me, h, :, pl.ds(step * width, width)] = total.astype(jnp.bfloat16)
        if h % CORES == CORES - 1:
            for done in range(h + 1 - CORES, h + 1):
                own_seen(done)
            if h < CORES:
                own_fc(2)
        if h == 0:

            @pl.when(jnp.logical_not(wraps))
            def _():
                meet_tiles()

    near_seen()
    for piece in range(3, lifted):
        own_fc(piece)


    @pl.when(wraps)
    def _():
        meet_tiles()

    rounds = CHUNKS // CORES
    lanes = 128
    base = [
        valid_ref[i, core].astype(jnp.float32) / error_ref[i, core].astype(jnp.float32)
        for i in range(rounds)
    ]
    for i in range(rounds):
        slot_ref[CORES * near, i] = value_ref[i, core].astype(jnp.float32)
        for spare in range(CORES * near + 1, slot_ref.shape[0]):
            slot_ref[spare, i] = jnp.zeros_like(base[i])
    near_ref[core * near + REACH] = stage_ref[REACH, :, core]

    for index, peer in enumerate(across):
        drain(fc_ref.at[peer, 0, pl.ds(0, pieces[1][2])], fc_across.at[0, index])
        fc_near(0, peer).start()
        fc_near(1, peer).start()

    drain(near_ref.at[pl.ds(0, CORES * near - 1)], tile_recv.at[0])
    for r in range(CORES * near):
        for i in range(rounds):
            slot_ref[r, i] = base[i] * near_ref[r, i]
    for i in range(rounds):
        for r in range(share // lanes):
            rinv_ref[i, :, r * lanes : (r + 1) * lanes] = slot_ref[:, i, r, :]

    for i in range(rounds):
        drain(seen_ref.at[pl.ds(0, n_mem - 1), 0], seen_recv.at[i])
        seen = jnp.concatenate(
            [seen_ref[m, i * CORES + core].astype(jnp.float32) for m in range(n_mem)], axis=0
        )
        average = jnp.mean(seen, axis=0, keepdims=True)
        deviation = seen - average
        rinv = rinv_ref[i]
        innovation = rinv[CORES * near : CORES * near + 1] - average
        right = jnp.concatenate(
            [deviation, jnp.broadcast_to(innovation, deviation.shape)], axis=0
        ).astype(jnp.bfloat16)
        rows = [
            (deviation * rinv[r : r + 1]).astype(jnp.bfloat16) for r in range(CORES * near)
        ]
        for user in range(CORES):
            where = slice(user * near * everyone, (user + 1) * near * everyone)
            sums = lax.dot_general(
                jnp.concatenate(rows[user * near : (user + 1) * near], axis=0),
                right,
                (((1,), (1,)), ((), ())),
                preferred_element_type=jnp.float32,
            )
            acc_ref[where] = sums + acc_ref[where] if i else sums

    fold = everyone // 2
    lane = lax.broadcasted_iota(jnp.int32, (fold, 2 * everyone), 1)
    for r in range(CORES * near):
        upper = acc_ref[r * everyone : r * everyone + fold]
        lower = acc_ref[r * everyone + fold : (r + 1) * everyone]
        packed = jnp.where(lane < everyone + fold, pltpu.roll(lower, fold, 1), upper)
        packed = jnp.where(lane < everyone, upper, packed)
        packed = jnp.where(lane < 2 * everyone - fold // 2, packed, lower)
        part_ref[r] = packed.astype(jnp.bfloat16)
        user, j = r // near, r % near
        if j != REACH:
            remote(
                part_ref.at[r],
                got_ref.at[core * near + j],
                out_sem.at[0],
                tile_recv.at[1],
                {"mem": y * CORES + user, **tile_peer(REACH - j)},
            ).start()
    remote(
        part_ref.at[(1 - core) * near + REACH],
        got_ref.at[core * near + REACH],
        out_sem.at[0],
        tile_recv.at[1],
        {"mem": sibling},
    ).start()
    got_ref[core * near + REACH] = part_ref[core * near + REACH]

    for index, peer in enumerate(across):
        first, stop = pieces[2][1], pieces[3][2]
        drain(fc_ref.at[peer, 0, pl.ds(first, stop - first)], fc_across.at[1, index])
        fc_near(2, peer).start()
        fc_near(3, peer).start()

    drain(got_ref.at[pl.ds(0, CORES * near - 1)], tile_recv.at[1])

    summed = got_ref[0].astype(jnp.float32)
    for r in range(1, CORES * near):
        summed = summed + got_ref[r].astype(jnp.float32)
    summed = summed / (everyone - 1.0)
    flipped = jnp.transpose(summed)
    spread = jnp.concatenate(
        [
            summed[:, :everyone],
            jnp.concatenate(
                [flipped[fold:everyone], summed[:, everyone : everyone + fold]], axis=1
            ),
        ],
        axis=0,
    )
    first, second = everyone + fold, 2 * everyone - fold // 2
    pulled = jnp.concatenate([flipped[first : first + 8], flipped[second : second + 8]], axis=1)
    rows = lax.broadcasted_iota(jnp.int32, (everyone, everyone), 0)
    identity = jnp.where(
        rows == lax.broadcasted_iota(jnp.int32, (everyone, everyone), 1), 1.0, 0.0
    )
    system = identity + spread
    square = jnp.sum(system * system, keepdims=True)
    scale = jnp.sqrt(square)
    rows = jnp.concatenate([pulled, jnp.ones_like(pulled)], axis=0)
    powers = [rows]
    parts = halves(system)
    second = fine_dot(parts, parts) / square
    powers.append(fine_dot(halves(rows), parts) / scale)
    current = system / scale
    parts, second_parts = halves(current), halves(second)
    third = fine_dot(second_parts, parts)
    fourth = fine_dot(second_parts, second_parts)
    for power in range(2, 6):
        powers.append(fine_dot(halves(powers[power - 2]), second_parts))
    weights = (2.25, -2.4375, 1.6875, -0.5625, 0.0625)

    def combine(terms):
        return sum(weight * term for weight, term in zip(weights, terms))

    root = combine([identity, current, second, third, fourth])
    root_parts = halves(root)
    inner_parts = halves(fine_dot(parts, root_parts))
    outer_parts = halves(fine_dot(root_parts, root_parts))
    root = 1.5 * root - 0.5 * fine_dot(inner_parts, outer_parts)
    drawn = 1.5 * combine(powers[:5]) - 0.5 * fine_dot(halves(combine(powers[1:])), outer_parts)
    root_parts = halves(root)
    ones = jnp.ones((everyone, everyone), jnp.bfloat16)
    sums = rounded_dot(root_parts[0], ones) + rounded_dot(root_parts[1], ones)
    mean_weight = fine_dot(halves(drawn[:8]), root_parts)[:1] / scale
    weight_sum = jnp.sum(drawn[:1] * drawn[8:9], axis=1, keepdims=True) / scale
    turned = root / jnp.sqrt(scale) + mean_weight
    turned = turned + (1.0 - sums / jnp.sqrt(scale) - weight_sum) / everyone
    rounded = turned.astype(jnp.bfloat16).astype(jnp.float32)
    turned = jnp.concatenate([rounded, turned - rounded], axis=1).astype(jnp.bfloat16)
    for m in range(n_mem):
        tsend_ref[m] = turned[m * members : (m + 1) * members]

    for step in range(1, n_mem):
        target = lax.rem(me + step, n_mem)
        remote(
            tsend_ref.at[target],
            trecv_ref.at[me],
            out_sem.at[0],
            t_recv.at[0],
            {"mem": target},
        ).start()
    @pl.when(core != 0)
    def _():
        tail_over()
        lift_over()

    trecv_ref[me] = tsend_ref[me]

    group = 8

    def apply(block, start, stop):
        where = pl.ds(block * wide, wide)
        left = left_ref[block]
        land = jnp.broadcast_to(land_ref[:, where], (members, wide)) > 0
        for first in range(start, stop, group):
            end = min(first + group, stop)
            states = jnp.concatenate(
                [
                    jnp.concatenate([fc_ref[m, block, f] for m in range(n_mem)], axis=0)
                    for f in range(first, end)
                ],
                axis=1,
            )
            pair = rounded_dot(left, states)
            total = pair[:members] + pair[members:]
            for f in range(end - first):
                moved_ref[block, first + f] = jnp.where(
                    land,
                    total[:, f * wide : (f + 1) * wide],
                    fc_ref[me, block, first + f].astype(jnp.float32),
                )
        moved = jnp.transpose(moved_ref[block, start:stop], (1, 0, 2)).astype(jnp.bfloat16)
        out_ref[:, start:stop, where] = moved

    for piece in range(4, lifted):
        relay_fc(piece)

    @pl.when(core != 0)
    def _():
        tail_relay()

    drain(trecv_ref.at[pl.ds(0, n_mem - 1)], t_recv.at[0])
    for block in range(n_mem):
        left = trecv_ref[block].astype(jnp.float32)
        left = jnp.concatenate([left[:, :everyone], left[:, everyone:]], axis=0)
        left_ref[block] = left.astype(jnp.bfloat16)

    @pl.when(core != 0)
    def _():
        lift_relay()

    count(2 * n_y * fields * (n_mem - 1) * members * wide, fc_unit.at[0])

    for unit in units[:-2]:
        apply(*unit)

    count(2 * n_y * (units[-2][2] - units[-2][1]) * members * wide, fc_unit.at[2])

    apply(*units[-2])

    @pl.when(core == 0)
    def _():
        last_rows = units[-1][2] - units[-1][1]
        count(2 * (n_mem - 1) * last_rows * members * wide, fc_unit.at[1])

    @pl.when(core != 0)
    def _():
        lift_end()

    apply(*units[-1])

    kinds = [fc_ref.at[0], seen_ref.at[0], part_ref, stage_ref.at[:, :, 0], tsend_ref.at[0]]
    sizes = [ref.dtype.itemsize * math.prod(ref.shape) for ref in kinds]
    counts = [n_mem - 1, n_y - 1, 0, 0, n_mem - 1]
    total = sum(size * count for size, count in zip(sizes, counts))
    total += sizes[1] // CORES
    total += (sizes[2] + sizes[3] * CORES) * (CORES * near - 1) // (CORES * near)
    size = 2 * members * wide * (units[-1][2] - units[-1][1])
    total -= (n_mem - 1) * size

    @pl.when(core == 0)
    def _():
        count(total + size, out_sem.at[0])

    @pl.when(core != 0)
    def _():
        count(total + (1 + 4 * (n_y - 1)) * size, out_sem.at[0])


def store(held_ref, out_ref, sem):
    parts = 4
    rows = held_ref.shape[0] // parts
    for part in range(parts):
        where = pl.ds(part * rows, rows)
        pltpu.make_async_copy(held_ref.at[where], out_ref.at[where], sem.at[0]).start()
    pltpu.make_async_copy(held_ref, out_ref, sem.at[0]).wait()


def on_device(
    n_mem,
    n_tile,
    ensemble_profiles_before,
    mixing_coefficient,
    surface_driver,
    terrain_indicator,
    measured_profile_position,
    measured_field_index,
    obs_valid,
    obs_value,
    obs_error,
    local_weight,
):
    members, fields, columns = ensemble_profiles_before.shape
    slots = measured_field_index.shape[0]
    everyone = members * n_mem
    near = 2 * REACH + 1
    n_y = n_mem // CORES
    wide = columns // n_mem
    units = [(block, 0, fields) for block in range(n_mem - 1)]
    cuts = (0, fields - 12, fields)
    units += [(n_mem - 1, *ends) for ends in zip(cuts[:-1], cuts[1:])]
    pieces = [(0, 0, 16, 0), (0, 16, 28, 0), (0, 28, 32, 0), (0, 32, fields, 0)]
    pieces += [(*unit, index) for index, unit in enumerate(units[:-1]) if index]
    pieces += [(n_mem - 1, fields - 12, fields - 4, n_mem), (n_mem - 1, fields - 4, fields, n_mem)]
    spare = 4 * everyone * fields * columns
    row = lambda a: a.reshape(1, -1)
    table = (CHUNKS // CORES, CORES, slots // CHUNKS // 128, 128)
    far = pl.BlockSpec(memory_space=pltpu.HBM)
    dma = pltpu.SemaphoreType.DMA
    held = pl.pallas_call(
        functools.partial(kernel, n_mem, n_tile, pieces, units),
        out_shape=pltpu.VMEM(ensemble_profiles_before.shape, jnp.bfloat16),
        in_specs=[far] * 10,
        out_specs=pl.BlockSpec(memory_space=pltpu.VMEM),
        scratch_shapes=[
            pltpu.VMEM((members, fields, columns), jnp.bfloat16),
            pltpu.VMEM((1, columns), jnp.float32),
            pltpu.VMEM((members, columns), jnp.float32),
            pltpu.VMEM((1, columns), jnp.int32),
            pltpu.VMEM((1, slots), jnp.int32),
            pltpu.VMEM((1, slots), jnp.int32),
            pltpu.VMEM(table, jnp.int32),
            pltpu.VMEM(table, jnp.bfloat16),
            pltpu.VMEM(table, jnp.bfloat16),
            pltpu.VMEM((n_mem, n_mem, fields, members, wide), jnp.bfloat16),
            pltpu.VMEM((n_mem, CHUNKS, members, slots // CHUNKS), jnp.bfloat16),
            pltpu.VMEM((near, *table), jnp.float32),
            pltpu.VMEM((CORES * near, table[0], *table[2:]), jnp.float32),
            pltpu.VMEM((16, table[0], *table[2:]), jnp.float32),
            pltpu.VMEM((table[0], 16, slots // CHUNKS), jnp.float32),
            pltpu.VMEM((CORES * near * everyone, 2 * everyone), jnp.float32),
            pltpu.VMEM((CORES * near, everyone // 2, 2 * everyone), jnp.bfloat16),
            pltpu.VMEM((CORES * near, everyone // 2, 2 * everyone), jnp.bfloat16),
            pltpu.VMEM((n_mem, members, 2 * everyone), jnp.bfloat16),
            pltpu.VMEM((n_mem, members, 2 * everyone), jnp.bfloat16),
            pltpu.VMEM((n_mem, 2 * members, everyone), jnp.bfloat16),
            pltpu.VMEM((n_mem, fields, members, wide), jnp.float32),
            pltpu.VMEM((spare // 512, 128), jnp.float32),
            dma((3,)),
            dma((2,)),
            dma((1,)),
            dma((CHUNKS // CORES,)),
            dma((len(pieces) - 1, n_y - 1)),
            dma((3,)),
            dma((1,)),
            dma((2,)),
            dma((1,)),
            pltpu.SemaphoreType.REGULAR,
            pltpu.SemaphoreType.REGULAR,
        ],
        compiler_params=pltpu.CompilerParams(
            collective_id=0, has_side_effects=True, vmem_limit_bytes=66_000_000
        ),
    )(
        ensemble_profiles_before,
        row(mixing_coefficient),
        surface_driver,
        row(terrain_indicator),
        row(measured_profile_position),
        row(measured_field_index),
        obs_valid.reshape(table),
        obs_value.reshape(table),
        obs_error.reshape(table),
        local_weight.reshape(near, *table),
    )
    return pl.pallas_call(
        store,
        out_shape=jax.ShapeDtypeStruct(held.shape, held.dtype),
        in_specs=[pl.BlockSpec(memory_space=pltpu.VMEM)],
        out_specs=pl.BlockSpec(memory_space=pltpu.HBM),
        scratch_shapes=[dma((1,))],
        compiler_params=pltpu.CompilerParams(vmem_limit_bytes=2_000_000),
    )(held)


def fits(n_mem, n_tile, ensemble, slots):
    members, fields, columns = ensemble[0] // n_mem, ensemble[1], ensemble[2] // n_tile
    return (
        n_mem % CORES == 0
        and n_mem > CORES
        and 2 * members * n_mem == 128
        and n_tile > 2 * REACH
        and members % 16 == 0
        and fields % 8 == 0
        and fields > 32
        and columns % (128 * n_mem) == 0
        and slots // n_tile % (1024 * CHUNKS) == 0
    )


def solution(mesh):
    in_specs = (
        P("mem", None, "tile"),
        P("tile"),
        P("mem", "tile"),
        P("tile"),
        P("tile"),
        P("tile"),
        P("tile"),
        P("tile"),
        P("tile"),
        P("mem", "tile", None),
    )
    out_specs = P("mem", None, "tile")

    def run(*args):
        sizes = mesh.shape["mem"], mesh.shape["tile"]
        body = plain_on_device
        if fits(*sizes, args[0].shape, args[5].shape[0]):
            body = functools.partial(on_device, *sizes)
        return jax.shard_map(
            body, mesh=mesh, in_specs=in_specs, out_specs=out_specs, check_vma=False
        )(*args)

    return run
```

```python
import functools
import math

import jax
import jax.numpy as jnp
from jax import lax
from jax.experimental import pallas as pl
from jax.experimental.pallas import tpu as pltpu
from jax.sharding import PartitionSpec as P

REACH = 2
NS_ITERS = 3


EXACT = lax.Precision.HIGHEST


def from_behind(value, axis, steps):
    count = lax.axis_size(axis)
    pairs = [(source, (source + steps) % count) for source in range(count)]
    return lax.ppermute(value, axis, pairs)


def vertical_mixing_step(
    ensemble_profiles_before, mixing_coefficient, surface_driver, terrain_indicator
):
    values = ensemble_profiles_before.astype(jnp.float32)
    above_layer = jnp.concatenate([values[:, :1], values[:, :-1]], axis=1)
    below_layer = jnp.concatenate([values[:, 1:], values[:, -1:]], axis=1)
    diffused = values + mixing_coefficient[None, None, :] * (
        above_layer - 2.0 * values + below_layer
    )
    stepped = diffused - 0.05 * values * values * values
    surface = jnp.concatenate([stepped[:, :1] + surface_driver[:, None, :], stepped[:, 1:]], axis=1)
    result = jnp.where(terrain_indicator[None, None, :] > 0, surface, values)
    return result.astype(jnp.bfloat16)


def measurement_operator(background_ensemble, measured_profile_position, measured_field_index):
    profile_sequence = background_ensemble.shape[2]
    unrolled_ensemble = background_ensemble.reshape(background_ensemble.shape[0], -1)
    slot_index = measured_field_index * profile_sequence + measured_profile_position
    return jnp.take(unrolled_ensemble, slot_index, axis=1)


def prepare(window):
    ensemble_profiles = window.shape[0] - 3
    measured_quantities = window[:ensemble_profiles].astype(jnp.float32)
    average = jnp.mean(measured_quantities, axis=0)
    deviation = measured_quantities - average
    innovation = window[ensemble_profiles].astype(jnp.float32) - average
    obs_precision = window[ensemble_profiles + 2].astype(jnp.float32) / window[
        ensemble_profiles + 1
    ].astype(jnp.float32)
    return (deviation, innovation, obs_precision)


def weights_for(deviation, innovation, precision, portions):
    ensemble_profiles = deviation.shape[0]
    portion_width = deviation.shape[1] // portions
    spread = jnp.zeros((ensemble_profiles, ensemble_profiles), jnp.float32)
    for portion_index in range(portions):
        portion = deviation[:, portion_index * portion_width : (portion_index + 1) * portion_width]
        scaled = (
            portion
            * precision[None, portion_index * portion_width : (portion_index + 1) * portion_width]
        )
        spread = spread + jnp.dot(
            scaled, portion.T, precision=EXACT, preferred_element_type=jnp.float32
        )
    spread = spread / (ensemble_profiles - 1.0)
    pulled = jnp.dot(
        deviation, precision * innovation, precision=EXACT, preferred_element_type=jnp.float32
    ) / (ensemble_profiles - 1.0)
    identity = jnp.eye(ensemble_profiles, dtype=jnp.float32)
    system = identity + spread
    norm_scale = jnp.sqrt(jnp.sum(system * system))

    def newton(sweep, carry):
        current, inv_root = carry
        middle = 1.5 * identity - 0.5 * jnp.dot(inv_root, current, precision=EXACT)
        return (
            jnp.dot(current, middle, precision=EXACT),
            jnp.dot(middle, inv_root, precision=EXACT),
        )

    current, inv_root = lax.fori_loop(0, NS_ITERS, newton, (system / norm_scale, identity))
    inv_root = inv_root / jnp.sqrt(norm_scale)
    inverse = jnp.dot(inv_root, inv_root, precision=EXACT)
    mean_weight = jnp.dot(inverse, pulled, precision=EXACT)
    return inv_root + mean_weight[:, None]


def update(states, transform, land_block):
    values = states.astype(jnp.float32)
    average = jnp.mean(values, axis=0)
    deviation = values - average[None]
    moved = jnp.einsum("isc,ij->jsc", deviation, transform, precision=EXACT)
    result = jnp.where(land_block[None, None, :] > 0, average[None] + moved, values)
    return result.astype(jnp.bfloat16)


def plain_on_device(
    ensemble_profiles_before,
    mixing_coefficient,
    surface_driver,
    terrain_indicator,
    measured_profile_position,
    measured_field_index,
    obs_valid,
    obs_value,
    obs_error,
    local_weight,
):
    background_ensemble = vertical_mixing_step(
        ensemble_profiles_before, mixing_coefficient, surface_driver, terrain_indicator
    )
    measured_quantities = measurement_operator(
        background_ensemble, measured_profile_position, measured_field_index
    )
    metadata = jnp.stack([obs_value, obs_error, obs_valid.astype(jnp.bfloat16)])
    own_rows = jnp.concatenate([measured_quantities, metadata], axis=0)
    pieces = []
    for offset in range(-REACH, REACH + 1):
        if offset == 0:
            pieces.append(own_rows)
        else:
            pieces.append(from_behind(own_rows, "tile", -offset))
    nearby = jnp.concatenate(pieces, axis=1)
    members_here = measured_quantities.shape[0]
    everyone = lax.all_gather(nearby[:members_here], "mem", axis=0, tiled=True)
    window = jnp.concatenate([everyone, nearby[members_here:]], axis=0)
    regrouped_states = lax.all_to_all(
        background_ensemble, "mem", split_axis=2, concat_axis=0, tiled=True
    )
    deviation, innovation, obs_precision = prepare(window)
    columns_here = regrouped_states.shape[2]
    local_land = lax.dynamic_slice_in_dim(
        terrain_indicator, lax.axis_index("mem") * columns_here, columns_here
    )
    transform = weights_for(
        deviation, innovation, obs_precision * local_weight[0, 0], 2 * REACH + 1
    )
    outputs = update(regrouped_states, transform, local_land)
    return lax.all_to_all(outputs, "mem", split_axis=0, concat_axis=2, tiled=True)


MESH = pl.DeviceIdType.MESH
CHUNKS = 4
CORES = 2
GATE = 0


def rounded_dot(a, b):
    return jnp.dot(a, b, preferred_element_type=jnp.float32)


def halves(a):
    high = a.astype(jnp.bfloat16)
    return high, (a - high.astype(jnp.float32)).astype(jnp.bfloat16)


def fine_dot(a, b):
    (a_high, a_low), (b_high, b_low) = a, b
    return rounded_dot(a_high, b_high) + (rounded_dot(a_high, b_low) + rounded_dot(a_low, b_high))


def drain(ref, sem):
    pltpu.make_async_copy(ref, ref, sem).wait()


def counter(bytes_ref):
    def count(size, sem):
        drain(bytes_ref.at[pl.ds(0, size // 512)], sem)

    return count


def kernel(
    n_mem,
    n_tile,
    pieces,
    units,
    ens_hbm,
    mix_hbm,
    surf_hbm,
    land_hbm,
    pos_hbm,
    field_hbm,
    valid_hbm,
    value_hbm,
    error_hbm,
    weight_hbm,
    out_ref,
    ens_ref,
    mix_ref,
    surf_ref,
    land_ref,
    pos_ref,
    field_ref,
    valid_ref,
    value_ref,
    error_ref,
    fc_ref,
    seen_ref,
    stage_ref,
    near_ref,
    slot_ref,
    rinv_ref,
    acc_ref,
    part_ref,
    got_ref,
    tsend_ref,
    trecv_ref,
    left_ref,
    moved_ref,
    bytes_ref,
    ens_sem,
    in_sem,
    out_sem,
    seen_recv,
    fc_across,
    fc_unit,
    lift_sem,
    tile_recv,
    t_recv,
    hello,
    ready,
):
    members, fields, columns = ens_ref.shape
    everyone = members * n_mem
    slots = pos_ref.shape[1]
    near = 2 * REACH + 1
    wide = columns // n_mem
    count = counter(bytes_ref)
    me, tile = lax.axis_index("mem"), lax.axis_index("tile")
    n_y = n_mem // CORES
    y, core = me // CORES, lax.rem(me, CORES)
    sibling = y * CORES + (1 - core)
    across = [lax.rem(y + step, n_y) * CORES + core for step in range(1, n_y)]
    gate = me == GATE
    wraps = tile < REACH

    def both(first, second):
        return jnp.logical_and(first, second)

    barrier = pltpu.get_barrier_semaphore()
    for step in range(1, n_mem):
        peer = lax.rem(me + step, n_mem)

        @pl.when(peer != GATE)
        def _(peer=peer):
            pl.semaphore_signal(barrier, inc=1, device_id={"mem": peer}, device_id_type=MESH)

    for offset in range(-REACH, REACH + 1):
        if offset:
            there = lax.rem(tile + offset + n_tile, n_tile)
            pl.semaphore_signal(
                barrier, inc=1, device_id={"mem": GATE, "tile": there}, device_id_type=MESH
            )

    opening = pieces[0][2] + 8

    def ens_copy(step, rows, sem):
        where = (slice(None), pl.ds(*rows), pl.ds(step * wide, wide))
        return pltpu.make_async_copy(ens_hbm.at[where], ens_ref.at[where], ens_sem.at[sem])

    groups = [
        [(mix_hbm, mix_ref), (surf_hbm, surf_ref), (land_hbm, land_ref)],
        [(pos_hbm, pos_ref), (field_hbm, field_ref)],
        [
            (valid_hbm, valid_ref),
            (value_hbm, value_ref),
            (error_hbm, error_ref),
            (weight_hbm, stage_ref),
        ],
    ]
    loads = [
        [pltpu.make_async_copy(src, dst, in_sem.at[min(g, 1)]) for src, dst in group]
        for g, group in enumerate(groups)
    ]
    first_load = ens_copy(0, (0, opening), 0)
    first_load.start()
    for copy in loads[0]:
        copy.start()
    ens_copy(0, (opening, fields - opening), 1).start()
    for step in range(1, n_mem):
        ens_copy(step, (0, fields), 2).start()
    for group in loads[1:]:
        for copy in group:
            copy.start()

    def remote(src, dst, send, recv, where):
        return pltpu.make_async_remote_copy(
            src_ref=src,
            dst_ref=dst,
            send_sem=send,
            recv_sem=recv,
            device_id=where,
            device_id_type=MESH,
        )

    n_pieces = len(pieces)
    lifted = n_pieces - 2

    def unit_sem(unit):
        return {len(units) - 1: 1, len(units) - 2: 2}.get(unit, 0)

    def piece_ref(piece, owner):
        block, first, stop = pieces[piece][:3]
        return fc_ref.at[owner, block, pl.ds(first, stop - first)]

    def fc_copy(piece, owner, recv, target):
        ref = piece_ref(piece, owner)
        return remote(ref, ref, out_sem.at[0], recv, {"mem": target})

    def fc_over(piece, owner, index, target):
        return fc_copy(piece, owner, fc_across.at[min(max(piece - 2, piece // 2), lifted - 2), index], target)

    def fc_near(piece, owner):
        return fc_copy(piece, owner, fc_unit.at[unit_sem(pieces[piece][3])], sibling)

    def own_fc(piece):
        for index, peer in enumerate(across):
            fc_over(piece, me, n_y - 2 - index, peer).start()
        fc_near(piece, me).start()

    def relay_fc(piece):
        for index, peer in enumerate(across):
            fc_over(piece, peer, index, peer).wait_recv()
            fc_near(piece, peer).start()

    def tail_ref(owner):
        first, stop = pieces[lifted][1], pieces[lifted + 1][2]
        return fc_ref.at[owner, n_mem - 1, pl.ds(first, stop - first)]

    def lift_out():
        fc_copy(lifted, me, lift_sem.at[0], sibling).start()
        fc_copy(lifted + 1, me, lift_sem.at[0], sibling).start()

    def tail_over():
        own_fc(lifted)
        own_fc(lifted + 1)

    def tail_relay():
        for index, peer in enumerate(across):
            drain(tail_ref(peer), fc_across.at[lifted - 2, index])
            fc_near(lifted, peer).start()
            fc_near(lifted + 1, peer).start()

    def lift_over():
        drain(tail_ref(sibling), lift_sem.at[0])
        for index, peer in enumerate(across):
            where = n_y - 2 - index
            fc_copy(lifted, sibling, fc_across.at[lifted - 1, where], peer).start()
            fc_copy(lifted + 1, sibling, fc_across.at[lifted, where], peer).start()
            partner = peer + (1 - 2 * core)
            fc_copy(lifted + 1, sibling, fc_unit.at[1], partner).start()

    def lift_relay():
        for index, peer in enumerate(across):
            partner = peer + (1 - 2 * core)
            drain(piece_ref(lifted, partner), fc_across.at[lifted - 1, index])
            fc_near(lifted, partner).start()

    def lift_end():
        for index, peer in enumerate(across):
            partner = peer + (1 - 2 * core)
            drain(piece_ref(lifted + 1, partner), fc_across.at[lifted, index])

    def seen_copy(h, target):
        ref = seen_ref.at[me, h]
        return remote(ref, ref, out_sem.at[0], seen_recv.at[h // CORES], {"mem": target})

    def own_seen(h):
        user = h % CORES
        for step in range(1, n_y):
            seen_copy(h, lax.rem(y + step, n_y) * CORES + user).start()

    def near_seen():
        for i in range(CHUNKS // CORES):
            h = i * CORES + 1 - core
            ref = seen_ref.at[me, h]
            remote(ref, ref, out_sem.at[0], seen_recv.at[i], {"mem": sibling}).start()

    def tile_peer(offset):
        return {"tile": lax.rem(tile + offset + n_tile, n_tile)}

    def mix_part(step, start, stop):
        where = pl.ds(pl.multiple_of(step * wide, wide), wide)
        low, high = max(start - 8, 0), min(stop + 8, fields)
        x = jnp.transpose(ens_ref[:, low:high, where].astype(jnp.float32), (1, 0, 2))
        rate = mix_ref[:, where][None]
        above = jnp.concatenate([x[:1], x[:-1]], axis=0)
        below = jnp.concatenate([x[1:], x[-1:]], axis=0)
        keep = slice(start - low, stop - low)
        x, above, below = x[keep], above[keep], below[keep]
        stepped = x + rate * (above - 2.0 * x + below) - 0.05 * x * x * x
        if start == 0:
            top = stepped[:1] + surf_ref[:, where][None]
            stepped = jnp.concatenate([top, stepped[1:]], axis=0)
        land = jnp.broadcast_to(land_ref[:, where][None], x.shape) > 0
        fc_ref[me, step, start:stop] = jnp.where(land, stepped, x).astype(jnp.bfloat16)

    def enter():
        pl.semaphore_wait(barrier, n_mem - 1)
        pl.semaphore_signal(hello, inc=1, device_id={"mem": GATE}, device_id_type=MESH)

    def send_weights():
        for j in range(near):
            for user in range(CORES):
                if j != REACH:
                    remote(
                        stage_ref.at[j, :, user],
                        near_ref.at[core * near + j],
                        out_sem.at[0],
                        tile_recv.at[0],
                        {"mem": y * CORES + user, **tile_peer(j - REACH)},
                    ).start()
        remote(
            stage_ref.at[REACH, :, 1 - core],
            near_ref.at[core * near + REACH],
            out_sem.at[0],
            tile_recv.at[0],
            {"mem": sibling},
        ).start()

    def admit():
        pl.semaphore_wait(barrier, 2 * REACH * n_mem)
        for step in range(1, n_mem):
            peer = lax.rem(me + step, n_mem)
            pl.semaphore_signal(ready, inc=1, device_id={"mem": peer}, device_id_type=MESH)

    def meet_tiles():
        @pl.when(both(wraps, gate))
        def _():
            admit()

        @pl.when(jnp.logical_not(gate))
        def _():
            pl.semaphore_wait(ready, 1)

        send_weights()

    @pl.when(me >= CORES)
    def _():
        enter()

    head = pieces[0][2]
    first_load.wait()
    count(4 * columns * (members + 2), in_sem.at[0])
    mix_part(0, 0, head)

    @pl.when(both(me < CORES, me != GATE))
    def _():
        enter()

    @pl.when(me != GATE)
    def _():
        own_fc(0)

    count(2 * members * wide * (fields - opening), ens_sem.at[1])
    mix_part(0, head, fields)

    @pl.when(me != GATE)
    def _():
        own_fc(1)

    count(2 * members * wide * fields * (n_mem - 1), ens_sem.at[2])

    def mix(step, carry):
        mix_part(step, 0, fields)
        return carry

    lax.fori_loop(1, n_mem, mix, 0)

    count(4 * slots * (near + 4), in_sem.at[1])

    @pl.when(gate)
    def _():
        pl.semaphore_wait(hello, n_mem - 1)
        own_fc(0)
        own_fc(1)

    @pl.when(both(gate, jnp.logical_not(wraps)))
    def _():
        admit()

    @pl.when(core == 0)
    def _():
        lift_out()

    share = slots // CHUNKS
    width = min(share, 512)
    flat = jnp.concatenate(
        [fc_ref[me, b].reshape(fields * members, wide) for b in range(n_mem)], axis=1
    )
    for h in range(CHUNKS):
        for step in range(share // width):
            where = pl.ds(h * share + step * width, width)
            rows = lax.broadcasted_iota(jnp.int32, (columns, width), 0)
            hot = jnp.where(rows == pos_ref[:, where], 1.0, 0.0).astype(jnp.bfloat16)
            found = rounded_dot(flat, hot)
            wanted = jnp.broadcast_to(field_ref[:, where], (members, width))
            total = found[:members]
            for f in range(1, fields):
                total = jnp.where(wanted == f, found[f * members : (f + 1) * members], total)
            seen_ref[me, h, :, pl.ds(step * width, width)] = total.astype(jnp.bfloat16)
        if h % CORES == CORES - 1:
            for done in range(h + 1 - CORES, h + 1):
                own_seen(done)
            if h < CORES:
                own_fc(2)
        if h == 0:

            @pl.when(jnp.logical_not(wraps))
            def _():
                meet_tiles()

    near_seen()
    for piece in range(3, lifted):
        own_fc(piece)


    @pl.when(wraps)
    def _():
        meet_tiles()

    rounds = CHUNKS // CORES
    lanes = 128
    base = [
        valid_ref[i, core].astype(jnp.float32) / error_ref[i, core].astype(jnp.float32)
        for i in range(rounds)
    ]
    for i in range(rounds):
        slot_ref[CORES * near, i] = value_ref[i, core].astype(jnp.float32)
        for spare in range(CORES * near + 1, slot_ref.shape[0]):
            slot_ref[spare, i] = jnp.zeros_like(base[i])
    near_ref[core * near + REACH] = stage_ref[REACH, :, core]

    for index, peer in enumerate(across):
        drain(fc_ref.at[peer, 0, pl.ds(0, pieces[1][2])], fc_across.at[0, index])
        fc_near(0, peer).start()
        fc_near(1, peer).start()

    drain(near_ref.at[pl.ds(0, CORES * near - 1)], tile_recv.at[0])
    for r in range(CORES * near):
        for i in range(rounds):
            slot_ref[r, i] = base[i] * near_ref[r, i]
    for i in range(rounds):
        for r in range(share // lanes):
            rinv_ref[i, :, r * lanes : (r + 1) * lanes] = slot_ref[:, i, r, :]

    for i in range(rounds):
        drain(seen_ref.at[pl.ds(0, n_mem - 1), 0], seen_recv.at[i])
        seen = jnp.concatenate(
            [seen_ref[m, i * CORES + core].astype(jnp.float32) for m in range(n_mem)], axis=0
        )
        average = jnp.mean(seen, axis=0, keepdims=True)
        deviation = seen - average
        rinv = rinv_ref[i]
        innovation = rinv[CORES * near : CORES * near + 1] - average
        right = jnp.concatenate(
            [deviation, jnp.broadcast_to(innovation, deviation.shape)], axis=0
        ).astype(jnp.bfloat16)
        rows = [
            (deviation * rinv[r : r + 1]).astype(jnp.bfloat16) for r in range(CORES * near)
        ]
        for user in range(CORES):
            where = slice(user * near * everyone, (user + 1) * near * everyone)
            sums = lax.dot_general(
                jnp.concatenate(rows[user * near : (user + 1) * near], axis=0),
                right,
                (((1,), (1,)), ((), ())),
                preferred_element_type=jnp.float32,
            )
            acc_ref[where] = sums + acc_ref[where] if i else sums

    fold = everyone // 2
    lane = lax.broadcasted_iota(jnp.int32, (fold, 2 * everyone), 1)
    for r in range(CORES * near):
        upper = acc_ref[r * everyone : r * everyone + fold]
        lower = acc_ref[r * everyone + fold : (r + 1) * everyone]
        packed = jnp.where(lane < everyone + fold, pltpu.roll(lower, fold, 1), upper)
        packed = jnp.where(lane < everyone, upper, packed)
        packed = jnp.where(lane < 2 * everyone - fold // 2, packed, lower)
        part_ref[r] = packed.astype(jnp.bfloat16)
        user, j = r // near, r % near
        if j != REACH:
            remote(
                part_ref.at[r],
                got_ref.at[core * near + j],
                out_sem.at[0],
                tile_recv.at[1],
                {"mem": y * CORES + user, **tile_peer(REACH - j)},
            ).start()
    remote(
        part_ref.at[(1 - core) * near + REACH],
        got_ref.at[core * near + REACH],
        out_sem.at[0],
        tile_recv.at[1],
        {"mem": sibling},
    ).start()
    got_ref[core * near + REACH] = part_ref[core * near + REACH]

    for index, peer in enumerate(across):
        first, stop = pieces[2][1], pieces[3][2]
        drain(fc_ref.at[peer, 0, pl.ds(first, stop - first)], fc_across.at[1, index])
        fc_near(2, peer).start()
        fc_near(3, peer).start()

    drain(got_ref.at[pl.ds(0, CORES * near - 1)], tile_recv.at[1])

    summed = got_ref[0].astype(jnp.float32)
    for r in range(1, CORES * near):
        summed = summed + got_ref[r].astype(jnp.float32)
    summed = summed / (everyone - 1.0)
    flipped = jnp.transpose(summed)
    spread = jnp.concatenate(
        [
            summed[:, :everyone],
            jnp.concatenate(
                [flipped[fold:everyone], summed[:, everyone : everyone + fold]], axis=1
            ),
        ],
        axis=0,
    )
    first, second = everyone + fold, 2 * everyone - fold // 2
    pulled = jnp.concatenate([flipped[first : first + 8], flipped[second : second + 8]], axis=1)
    rows = lax.broadcasted_iota(jnp.int32, (everyone, everyone), 0)
    identity = jnp.where(
        rows == lax.broadcasted_iota(jnp.int32, (everyone, everyone), 1), 1.0, 0.0
    )
    system = identity + spread
    square = jnp.sum(system * system, keepdims=True)
    scale = jnp.sqrt(square)
    rows = jnp.concatenate([pulled, jnp.ones_like(pulled)], axis=0)
    powers = [rows]
    parts = halves(system)
    second = fine_dot(parts, parts) / square
    powers.append(fine_dot(halves(rows), parts) / scale)
    current = system / scale
    parts, second_parts = halves(current), halves(second)
    third = fine_dot(second_parts, parts)
    fourth = fine_dot(second_parts, second_parts)
    for power in range(2, 6):
        powers.append(fine_dot(halves(powers[power - 2]), second_parts))
    weights = (2.25, -2.4375, 1.6875, -0.5625, 0.0625)

    def combine(terms):
        return sum(weight * term for weight, term in zip(weights, terms))

    root = combine([identity, current, second, third, fourth])
    root_parts = halves(root)
    inner_parts = halves(fine_dot(parts, root_parts))
    outer_parts = halves(fine_dot(root_parts, root_parts))
    root = 1.5 * root - 0.5 * fine_dot(inner_parts, outer_parts)
    drawn = 1.5 * combine(powers[:5]) - 0.5 * fine_dot(halves(combine(powers[1:])), outer_parts)
    root_parts = halves(root)
    ones = jnp.ones((everyone, everyone), jnp.bfloat16)
    sums = rounded_dot(root_parts[0], ones) + rounded_dot(root_parts[1], ones)
    mean_weight = fine_dot(halves(drawn[:8]), root_parts)[:1] / scale
    weight_sum = jnp.sum(drawn[:1] * drawn[8:9], axis=1, keepdims=True) / scale
    turned = root / jnp.sqrt(scale) + mean_weight
    turned = turned + (1.0 - sums / jnp.sqrt(scale) - weight_sum) / everyone
    rounded = turned.astype(jnp.bfloat16).astype(jnp.float32)
    turned = jnp.concatenate([rounded, turned - rounded], axis=1).astype(jnp.bfloat16)
    for m in range(n_mem):
        tsend_ref[m] = turned[m * members : (m + 1) * members]

    for step in range(1, n_mem):
        target = lax.rem(me + step, n_mem)
        remote(
            tsend_ref.at[target],
            trecv_ref.at[me],
            out_sem.at[0],
            t_recv.at[0],
            {"mem": target},
        ).start()
    @pl.when(core != 0)
    def _():
        tail_over()
        lift_over()

    trecv_ref[me] = tsend_ref[me]

    group = 8

    def apply(block, start, stop):
        where = pl.ds(block * wide, wide)
        left = left_ref[block]
        land = jnp.broadcast_to(land_ref[:, where], (members, wide)) > 0
        for first in range(start, stop, group):
            end = min(first + group, stop)
            states = jnp.concatenate(
                [
                    jnp.concatenate([fc_ref[m, block, f] for m in range(n_mem)], axis=0)
                    for f in range(first, end)
                ],
                axis=1,
            )
            pair = rounded_dot(left, states)
            total = pair[:members] + pair[members:]
            for f in range(end - first):
                moved_ref[block, first + f] = jnp.where(
                    land,
                    total[:, f * wide : (f + 1) * wide],
                    fc_ref[me, block, first + f].astype(jnp.float32),
                )
        moved = jnp.transpose(moved_ref[block, start:stop], (1, 0, 2)).astype(jnp.bfloat16)
        out_ref[:, start:stop, where] = moved

    for piece in range(4, lifted):
        relay_fc(piece)

    @pl.when(core != 0)
    def _():
        tail_relay()

    drain(trecv_ref.at[pl.ds(0, n_mem - 1)], t_recv.at[0])
    for block in range(n_mem):
        left = trecv_ref[block].astype(jnp.float32)
        left = jnp.concatenate([left[:, :everyone], left[:, everyone:]], axis=0)
        left_ref[block] = left.astype(jnp.bfloat16)

    @pl.when(core != 0)
    def _():
        lift_relay()

    count(2 * n_y * fields * (n_mem - 1) * members * wide, fc_unit.at[0])

    for unit in units[:-2]:
        apply(*unit)

    count(2 * n_y * (units[-2][2] - units[-2][1]) * members * wide, fc_unit.at[2])

    apply(*units[-2])

    @pl.when(core == 0)
    def _():
        last_rows = units[-1][2] - units[-1][1]
        count(2 * (n_mem - 1) * last_rows * members * wide, fc_unit.at[1])

    @pl.when(core != 0)
    def _():
        lift_end()

    apply(*units[-1])

    kinds = [fc_ref.at[0], seen_ref.at[0], part_ref, stage_ref.at[:, :, 0], tsend_ref.at[0]]
    sizes = [ref.dtype.itemsize * math.prod(ref.shape) for ref in kinds]
    counts = [n_mem - 1, n_y - 1, 0, 0, n_mem - 1]
    total = sum(size * count for size, count in zip(sizes, counts))
    total += sizes[1] // CORES
    total += (sizes[2] + sizes[3] * CORES) * (CORES * near - 1) // (CORES * near)
    size = 2 * members * wide * (units[-1][2] - units[-1][1])
    total -= (n_mem - 1) * size

    @pl.when(core == 0)
    def _():
        count(total + size, out_sem.at[0])

    @pl.when(core != 0)
    def _():
        count(total + (1 + 4 * (n_y - 1)) * size, out_sem.at[0])


def store(held_ref, out_ref, sem):
    parts = 4
    rows = held_ref.shape[0] // parts
    for part in range(parts):
        where = pl.ds(part * rows, rows)
        pltpu.make_async_copy(held_ref.at[where], out_ref.at[where], sem.at[0]).start()
    pltpu.make_async_copy(held_ref, out_ref, sem.at[0]).wait()


def on_device(
    n_mem,
    n_tile,
    ensemble_profiles_before,
    mixing_coefficient,
    surface_driver,
    terrain_indicator,
    measured_profile_position,
    measured_field_index,
    obs_valid,
    obs_value,
    obs_error,
    local_weight,
):
    members, fields, columns = ensemble_profiles_before.shape
    slots = measured_field_index.shape[0]
    everyone = members * n_mem
    near = 2 * REACH + 1
    n_y = n_mem // CORES
    wide = columns // n_mem
    units = [(block, 0, fields) for block in range(n_mem - 1)]
    cuts = (0, fields - 12, fields)
    units += [(n_mem - 1, *ends) for ends in zip(cuts[:-1], cuts[1:])]
    pieces = [(0, 0, 16, 0), (0, 16, 32, 0), (0, 32, 36, 0), (0, 36, fields, 0)]
    pieces += [(*unit, index) for index, unit in enumerate(units[:-1]) if index]
    pieces += [(n_mem - 1, fields - 12, fields - 4, n_mem), (n_mem - 1, fields - 4, fields, n_mem)]
    spare = 4 * everyone * fields * columns
    row = lambda a: a.reshape(1, -1)
    table = (CHUNKS // CORES, CORES, slots // CHUNKS // 128, 128)
    far = pl.BlockSpec(memory_space=pltpu.HBM)
    dma = pltpu.SemaphoreType.DMA
    held = pl.pallas_call(
        functools.partial(kernel, n_mem, n_tile, pieces, units),
        out_shape=pltpu.VMEM(ensemble_profiles_before.shape, jnp.bfloat16),
        in_specs=[far] * 10,
        out_specs=pl.BlockSpec(memory_space=pltpu.VMEM),
        scratch_shapes=[
            pltpu.VMEM((members, fields, columns), jnp.bfloat16),
            pltpu.VMEM((1, columns), jnp.float32),
            pltpu.VMEM((members, columns), jnp.float32),
            pltpu.VMEM((1, columns), jnp.int32),
            pltpu.VMEM((1, slots), jnp.int32),
            pltpu.VMEM((1, slots), jnp.int32),
            pltpu.VMEM(table, jnp.int32),
            pltpu.VMEM(table, jnp.bfloat16),
            pltpu.VMEM(table, jnp.bfloat16),
            pltpu.VMEM((n_mem, n_mem, fields, members, wide), jnp.bfloat16),
            pltpu.VMEM((n_mem, CHUNKS, members, slots // CHUNKS), jnp.bfloat16),
            pltpu.VMEM((near, *table), jnp.float32),
            pltpu.VMEM((CORES * near, table[0], *table[2:]), jnp.float32),
            pltpu.VMEM((16, table[0], *table[2:]), jnp.float32),
            pltpu.VMEM((table[0], 16, slots // CHUNKS), jnp.float32),
            pltpu.VMEM((CORES * near * everyone, 2 * everyone), jnp.float32),
            pltpu.VMEM((CORES * near, everyone // 2, 2 * everyone), jnp.bfloat16),
            pltpu.VMEM((CORES * near, everyone // 2, 2 * everyone), jnp.bfloat16),
            pltpu.VMEM((n_mem, members, 2 * everyone), jnp.bfloat16),
            pltpu.VMEM((n_mem, members, 2 * everyone), jnp.bfloat16),
            pltpu.VMEM((n_mem, 2 * members, everyone), jnp.bfloat16),
            pltpu.VMEM((n_mem, fields, members, wide), jnp.float32),
            pltpu.VMEM((spare // 512, 128), jnp.float32),
            dma((3,)),
            dma((2,)),
            dma((1,)),
            dma((CHUNKS // CORES,)),
            dma((len(pieces) - 1, n_y - 1)),
            dma((3,)),
            dma((1,)),
            dma((2,)),
            dma((1,)),
            pltpu.SemaphoreType.REGULAR,
            pltpu.SemaphoreType.REGULAR,
        ],
        compiler_params=pltpu.CompilerParams(
            collective_id=0, has_side_effects=True, vmem_limit_bytes=66_000_000
        ),
    )(
        ensemble_profiles_before,
        row(mixing_coefficient),
        surface_driver,
        row(terrain_indicator),
        row(measured_profile_position),
        row(measured_field_index),
        obs_valid.reshape(table),
        obs_value.reshape(table),
        obs_error.reshape(table),
        local_weight.reshape(near, *table),
    )
    return pl.pallas_call(
        store,
        out_shape=jax.ShapeDtypeStruct(held.shape, held.dtype),
        in_specs=[pl.BlockSpec(memory_space=pltpu.VMEM)],
        out_specs=pl.BlockSpec(memory_space=pltpu.HBM),
        scratch_shapes=[dma((1,))],
        compiler_params=pltpu.CompilerParams(vmem_limit_bytes=2_000_000),
    )(held)


def fits(n_mem, n_tile, ensemble, slots):
    members, fields, columns = ensemble[0] // n_mem, ensemble[1], ensemble[2] // n_tile
    return (
        n_mem % CORES == 0
        and n_mem > CORES
        and 2 * members * n_mem == 128
        and n_tile > 2 * REACH
        and members % 16 == 0
        and fields % 8 == 0
        and fields > 32
        and columns % (128 * n_mem) == 0
        and slots // n_tile % (1024 * CHUNKS) == 0
    )


def solution(mesh):
    in_specs = (
        P("mem", None, "tile"),
        P("tile"),
        P("mem", "tile"),
        P("tile"),
        P("tile"),
        P("tile"),
        P("tile"),
        P("tile"),
        P("tile"),
        P("mem", "tile", None),
    )
    out_specs = P("mem", None, "tile")

    def run(*args):
        sizes = mesh.shape["mem"], mesh.shape["tile"]
        body = plain_on_device
        if fits(*sizes, args[0].shape, args[5].shape[0]):
            body = functools.partial(on_device, *sizes)
        return jax.shard_map(
            body, mesh=mesh, in_specs=in_specs, out_specs=out_specs, check_vma=False
        )(*args)

    return run
```
